32 devices in a mesh: rows: 8 (over z, y), grp: 4 (over x, core).
Axes of the slice: x: 2, y: 2, z: 4, core: 2. Of those that a mesh axis runs over, the one named last changes fastest.
Arguments:
- embeddings: float32 [4096, 768], P(('rows', 'grp')), may hold values from -100 to 100
- assignments: int32 [4096], P(('rows', 'grp')), may hold values from 0 to 16383, as said below
Outputs:
- whitened: float32 [4096, 768], P(('rows', 'grp'))
- centroid_means: float32 [16384, 768], P(('rows', 'grp'))
The draws below stay inside these ranges and needn't reach their ends.
Inputs may be any that keep to these rules, and one draw needn't show every extreme that they name: `assignments`: owner o holds the 2048 centroids o * 2048 to (o + 1) * 2048 - 1. The 128 rows of one device name centroids of at most 32 rows for any one owner, and exactly 32 for some owner. Some centroids are named by no row.
All inputs are finite; a program needn't handle non-finite values.
Results may differ from the reference program's by a relative error of at most 0.00007.
Values sent between devices are 32-bit elements; how exact they have to be, the bound alone decides.
A program may use at most 64 MiB of HBM per device.

```python
import math
import jax
import jax.numpy as jnp
from jax import lax

D = 768
CENTROIDS = 16384
R_DEV = 128
CAP = 32
TOTAL_ROWS = 4096
N_ROWS = 8


def draw_embeddings(key, part):
    first, second = jax.random.split(jax.random.fold_in(key, 11), 2)
    blocks = TOTAL_ROWS // R_DEV
    block_index = jnp.arange(TOTAL_ROWS, dtype=jnp.int32) // R_DEV
    device_scale = 3.0 ** (0.5 * block_index.astype(jnp.float32) / max(blocks - 1, 1))
    base = jnp.clip(jax.random.normal(first, (TOTAL_ROWS, D), jnp.float32), -5.0, 5.0)
    row_scale = jnp.exp(jax.random.uniform(second, (TOTAL_ROWS,), jnp.float32, 0.0, math.log(10.0)))
    values = base * row_scale[:, None]
    return values * device_scale[:, None]


def draw_assignments(key, part):
    per_owner = CENTROIDS // N_ROWS
    blocks = TOTAL_ROWS // R_DEV
    offsets = jax.random.randint(jax.random.fold_in(key, 7), (N_ROWS,), 0, per_owner)
    block_keys = jax.random.split(jax.random.fold_in(key, 5), blocks)

    def one_block(block_key):
        kfirst, ksecond, kthird, kfourth = jax.random.split(block_key, 4)
        chosen = jax.random.randint(kfirst, (), 0, N_ROWS)
        others = jnp.tile(jnp.arange(1, N_ROWS, dtype=jnp.int32), CAP)
        others = jax.random.permutation(ksecond, others)[:R_DEV - CAP]
        owners = jnp.concatenate([jnp.zeros((CAP,), jnp.int32), others])
        owners = (owners + chosen) % N_ROWS
        owners = jax.random.permutation(kthird, owners)
        tries = jax.random.randint(kfourth, (3, R_DEV), 0, per_owner)
        local = (jnp.min(tries, axis=0) + offsets[owners]) % per_owner
        return owners * per_owner + local
    return jax.vmap(one_block)(block_keys).reshape(TOTAL_ROWS).astype(jnp.int32)


def setup_inputs(seed: int = 0) -> dict:
    streams_of = jax.random.split(jax.random.key(seed), 3)
    return {
        "embeddings": draw_embeddings(jax.random.fold_in(streams_of[2], 71), 0),
        "assignments": draw_assignments(jax.random.fold_in(streams_of[2], 71), 0),
    }


def reference(embeddings, assignments):
    total = embeddings.shape[0]
    width = embeddings.shape[1]
    gram = jnp.dot(embeddings.T.astype(jnp.float32), embeddings.astype(jnp.float32), precision=lax.Precision.HIGHEST, preferred_element_type=jnp.float32)
    gram = gram / total + 1e-05 * jnp.eye(width, dtype=jnp.float32)
    factor = jnp.linalg.cholesky(gram)
    whitened = lax.linalg.triangular_solve(factor, embeddings, left_side=False, lower=True, transpose_a=True)
    list_sums = jax.ops.segment_sum(whitened, assignments, num_segments=CENTROIDS)
    ones = jnp.ones(assignments.shape, dtype=jnp.float32)
    list_counts = jax.ops.segment_sum(ones, assignments, num_segments=CENTROIDS)
    centroid_means = list_sums / jnp.maximum(list_counts, 1.0)[:, None]
    return (whitened, centroid_means)
```

```python
import functools

import jax
import jax.numpy as jnp
from jax import lax
from jax.experimental import pallas as pl
from jax.experimental.pallas import tpu as pltpu
from jax.sharding import PartitionSpec as P

CENTROIDS = 16384
BLOCK = 128
PANEL = 8


def split3(value):
    high = value.astype(jnp.bfloat16).astype(jnp.float32)
    rest = value - high
    mid = rest.astype(jnp.bfloat16).astype(jnp.float32)
    return high, mid, rest - mid


def dot(a, b, dims):
    return lax.dot_general(
        a, b, (dims, ((), ())), precision=lax.Precision.HIGHEST, preferred_element_type=jnp.float32
    )


def solve_into(out_ref, values, x_ref, scale=None):
    width = x_ref.shape[0]
    strip = 2 * BLOCK if width % (2 * BLOCK) == 0 else BLOCK
    high, mid, _ = split3(values)
    high, mid = high.astype(jnp.bfloat16), mid.astype(jnp.bfloat16)
    for lo in range(0, width, strip):
        hi = lo + strip
        xh, xm, _ = split3(x_ref[lo:hi, :hi])
        xh, xm = xh.astype(jnp.bfloat16), xm.astype(jnp.bfloat16)
        out = jnp.zeros((values.shape[0], strip), jnp.float32)
        for a, b in ((mid, xh), (high, xm), (high, xh)):
            out = out + lax.dot_general(
                a[:, :hi], b, (((1,), (1,)), ((), ())), preferred_element_type=jnp.float32
            )
        if scale is None:
            out_ref[:, lo:hi] = out
        else:
            out_ref[:, lo:hi] = out * scale


def lanes(value, lane):
    return jnp.broadcast_to(value[:, lane : lane + 1], (PANEL, BLOCK))


def sublanes(value, row):
    return jnp.broadcast_to(value[row : row + 1, :], (PANEL, BLOCK))


def merge_rows(rows):
    sub = lax.broadcasted_iota(jnp.int32, (PANEL, BLOCK), 0)
    out = rows[0]
    for i in range(1, PANEL):
        out = jnp.where(sub == i, rows[i], out)
    return out


def invert_block(d_ref, v_ref):
    groups = BLOCK // PANEL

    def load(g):
        rows = slice(g * PANEL, (g + 1) * PANEL)
        return d_ref[rows, :BLOCK], d_ref[rows, BLOCK:]

    def store(g, left, right):
        rows = slice(g * PANEL, (g + 1) * PANEL)
        d_ref[rows, :BLOCK] = left
        d_ref[rows, BLOCK:] = right

    left, right = load(0)
    for p in range(groups):
        first = p * PANEL
        near, middle, far = p + 1 < groups, p + 2 < groups, p + 3 < groups
        a = {}
        for j in range(PANEL):
            column = lanes(left, first + j)
            for i in range(j, PANEL):
                a[i, j] = sublanes(column, i)
        u = [sublanes(left, i) for i in range(PANEL)]
        v = [sublanes(right, i) for i in range(PANEL)]
        if near:
            next_left, next_right = load(p + 1)
            b = [lanes(next_left, first + j) for j in range(PANEL)]
        if far:
            gh, gm, gl = split3(left)
            lhs = jnp.concatenate([gh, gh, gm, gh, gm, gl], axis=0).astype(jnp.bfloat16)
        s = [None] * PANEL
        for j in range(PANEL):
            if j % 2 == 0:
                top, side, low = a[j, j], a[j + 1, j], a[j + 1, j + 1]
                s[j] = lax.rsqrt(top)
                s[j + 1] = lax.rsqrt(top * low - side * side) * (top * s[j])
            u[j] = u[j] * s[j]
            v[j] = v[j] * s[j]
            for i in range(j + 1, PANEL):
                a[i, j] = a[i, j] * s[j]
            for i in range(j + 1, PANEL):
                for k in range(j + 1, i + 1):
                    a[i, k] = a[i, k] - a[i, j] * a[k, j]
                u[i] = u[i] - a[i, j] * u[j]
                v[i] = v[i] - a[i, j] * v[j]
            if near:
                b[j] = b[j] * s[j]
                for k in range(j + 1, PANEL):
                    b[k] = b[k] - b[j] * a[k, j]
                next_left = next_left - b[j] * u[j]
                next_right = next_right - b[j] * v[j]
        v_ref[first : first + PANEL, :] = merge_rows(v)
        if near:
            left, right = next_left, next_right
        if middle:
            w, z = [None] * PANEL, [None] * PANEL
            for j in reversed(range(PANEL)):
                wj, zj = u[j], v[j]
                for k in range(j + 1, PANEL):
                    wj = wj - a[k, j] * w[k]
                    zj = zj - a[k, j] * z[k]
                w[j] = wj * s[j]
                z[j] = zj * s[j]
            x, y = load(p + 2)
            coefficients = [lanes(x, first + k) for k in range(PANEL)]
            for k in range(PANEL):
                x = x - coefficients[k] * w[k]
                y = y - coefficients[k] * z[k]
            store(p + 2, x, y)
        if far:
            wh, wm, wl = split3(merge_rows(w))
            zh, zm, zl = split3(merge_rows(z))
            rhs = jnp.concatenate(
                [
                    jnp.concatenate([wh, wm, wh, wl, wm, wh], axis=0),
                    jnp.concatenate([zh, zm, zh, zl, zm, zh], axis=0),
                ],
                axis=1,
            ).astype(jnp.bfloat16)
            update = lax.dot_general(
                lhs, rhs, (((0,), (0,)), ((), ())), preferred_element_type=jnp.float32
            )
            for g in range(p + 3, groups):
                x, y = load(g)
                rows = slice(g * PANEL, (g + 1) * PANEL)
                store(g, x - update[rows, :BLOCK], y - update[rows, BLOCK:])


def block_pairs(width):
    blocks = width // BLOCK
    return [(i, j) for i in range(blocks) for j in range(i, blocks)]


def gram_kernel(e_ref, g_ref):
    width = e_ref.shape[1]
    used = 0
    for i in range(width // BLOCK):
        lo = i * BLOCK
        strip = dot(e_ref[:, lo : lo + BLOCK], e_ref[:, lo:], ((0,), (0,)))
        for j in range(strip.shape[1] // BLOCK):
            g_ref[used : used + BLOCK, :] = strip[:, j * BLOCK : (j + 1) * BLOCK]
            used += BLOCK
    if used < g_ref.shape[0]:
        g_ref[used:, :] = jnp.zeros((g_ref.shape[0] - used, BLOCK), jnp.float32)


def local_gram(embeddings, devices):
    width = embeddings.shape[1]
    unit = devices * 8
    rows = len(block_pairs(width)) * BLOCK
    rows = (rows + unit - 1) // unit * unit
    vmem = pl.BlockSpec(memory_space=pltpu.VMEM)
    return pl.pallas_call(
        gram_kernel,
        out_shape=jax.ShapeDtypeStruct((rows, BLOCK), jnp.float32),
        in_specs=[vmem],
        out_specs=vmem,
        compiler_params=pltpu.CompilerParams(vmem_limit_bytes=32 * 1024 * 1024),
    )(embeddings)


def reduce_kernel(links, g_ref, out_ref, acc_ref, in_ref, send_sem, recv_sem):
    partners, bits = [], []
    for axis, bit in links:
        me = lax.axis_index(axis)
        one = lax.rem(me // bit, 2)
        bits.append(one)
        partners.append({axis: me + bit - 2 * bit * one})
    barrier = pltpu.get_barrier_semaphore()
    for partner in partners:
        pl.semaphore_signal(
            barrier, inc=1, device_id=partner, device_id_type=pl.DeviceIdType.MESH
        )
    pl.semaphore_wait(barrier, len(partners))
    steps = len(links)
    unit = 8
    for axis in ("grp", "rows"):
        unit *= lax.axis_size(axis)
    units = g_ref.shape[0] // unit
    streams = max(1, min(3, units, steps - 1))
    orders, sizes, starts = [], [], []
    first = 0
    for n in range(streams):
        size = (units // streams + (1 if n < units % streams else 0)) * unit
        orders.append([0] + [1 + (n + k) % (steps - 1) for k in range(steps - 1)])
        sizes.append(size)
        starts.append([first])
        first += size
    landed = [s[0] for s in starts]

    def send(source, source_start, target, target_start, rows, link, slot):
        copy = pltpu.make_async_remote_copy(
            src_ref=source.at[pl.ds(source_start, rows)],
            dst_ref=target.at[pl.ds(target_start, rows)],
            send_sem=send_sem.at[slot],
            recv_sem=recv_sem.at[slot],
            device_id=partners[link],
            device_id_type=pl.DeviceIdType.MESH,
        )
        copy.start()
        return copy

    for k in range(steps):
        source = g_ref if k == 0 else acc_ref
        target = out_ref if k == steps - 1 else acc_ref
        copies = []
        for n in range(streams):
            link, start, half = orders[n][k], starts[n][-1], sizes[n] // 2
            keep = pl.multiple_of(start + bits[link] * half, 8)
            give = pl.multiple_of(start + (1 - bits[link]) * half, 8)
            slot = k * streams + n
            copies.append(send(source, give, in_ref, landed[n], half, link, slot))
            starts[n].append(keep)
        for n in range(streams):
            half, keep = sizes[n] // 2, starts[n][-1]
            copies[n].wait()
            target[pl.ds(keep, half), :] = (
                source[pl.ds(keep, half), :] + in_ref[pl.ds(landed[n], half), :]
            )
            landed[n] += half
            sizes[n] = half
    for k in reversed(range(steps)):
        copies = []
        for n in range(streams):
            start = starts[n][k + 1]
            slot = (steps + k) * streams + n
            copies.append(send(out_ref, start, out_ref, start, sizes[n], orders[n][k], slot))
        for n in range(streams):
            copies[n].wait()
            sizes[n] *= 2


def reduce_everywhere(packed):
    links = []
    for axis in ("grp", "rows"):
        bit = 1
        while bit < lax.axis_size(axis):
            links.append((axis, bit))
            bit *= 2
    vmem = pl.BlockSpec(memory_space=pltpu.VMEM)
    return pl.pallas_call(
        functools.partial(reduce_kernel, links),
        out_shape=jax.ShapeDtypeStruct(packed.shape, jnp.float32),
        in_specs=[vmem],
        out_specs=vmem,
        scratch_shapes=[
            pltpu.VMEM(packed.shape, jnp.float32),
            pltpu.VMEM(packed.shape, jnp.float32),
            pltpu.SemaphoreType.DMA((6 * len(links),)),
            pltpu.SemaphoreType.DMA((6 * len(links),)),
        ],
        compiler_params=pltpu.CompilerParams(
            collective_id=0, has_side_effects=True, vmem_limit_bytes=24 * 1024 * 1024
        ),
    )(packed)


def factor_kernel(total, g_ref, e_ref, w_ref, x_ref, a_ref, d_ref, v_ref):
    width = x_ref.shape[0]
    r = lax.broadcasted_iota(jnp.int32, (BLOCK, BLOCK), 0)
    c = lax.broadcasted_iota(jnp.int32, (BLOCK, BLOCK), 1)
    eye = jnp.where(r == c, 1.0, 0.0).astype(jnp.float32)
    for n, (i, j) in enumerate(block_pairs(width)):
        a_ref[i * BLOCK : (i + 1) * BLOCK, j * BLOCK : (j + 1) * BLOCK] = (
            g_ref[n * BLOCK : (n + 1) * BLOCK, :] / total
        )
    x_ref[...] = jnp.zeros_like(x_ref)
    for lo in range(0, width, BLOCK):
        hi = lo + BLOCK
        here = slice(lo, hi)
        d_ref[:, :BLOCK] = a_ref[here, here] + 1e-05 * eye
        d_ref[:, BLOCK:] = eye
        invert_block(d_ref, v_ref)
        inv = v_ref[...]
        x_ref[here, here] = inv
        if lo > 0:
            x_ref[here, :lo] = dot(inv, x_ref[here, :lo], ((1,), (0,)))
        if hi < width:
            upper = dot(inv, a_ref[here, hi:], ((1,), (0,)))
            for row in range(hi, width, BLOCK):
                strip = slice(row, row + BLOCK)
                a_ref[strip, row:] = a_ref[strip, row:] - dot(
                    upper[:, row - hi : row - hi + BLOCK], upper[:, row - hi :], ((0,), (0,))
                )
            x_ref[hi:, :hi] = x_ref[hi:, :hi] - dot(upper, x_ref[here, :hi], ((0,), (0,)))
    solve_into(w_ref, e_ref[...], x_ref)


def factor_and_whiten(packed, embeddings, total):
    width = embeddings.shape[1]
    vmem = pl.BlockSpec(memory_space=pltpu.VMEM)
    return pl.pallas_call(
        functools.partial(factor_kernel, float(total)),
        out_shape=(
            jax.ShapeDtypeStruct(embeddings.shape, jnp.float32),
            jax.ShapeDtypeStruct((width, width), jnp.float32),
        ),
        in_specs=[vmem] * 2,
        out_specs=(vmem, vmem),
        scratch_shapes=[
            pltpu.VMEM((width, width), jnp.float32),
            pltpu.VMEM((BLOCK, 2 * BLOCK), jnp.float32),
            pltpu.VMEM((BLOCK, BLOCK), jnp.float32),
        ],
        cost_estimate=pl.CostEstimate(
            flops=12 * width**3, bytes_accessed=12 * width**2, transcendentals=width
        ),
        compiler_params=pltpu.CompilerParams(vmem_limit_bytes=32 * 1024 * 1024),
    )(packed, embeddings)


def means_kernel(*refs):
    parts, x_ref, m_ref, s_ref, c_ref = refs[:-4], refs[-4], refs[-3], refs[-2], refs[-1]
    lists, width = m_ref.shape
    base = lax.axis_index("grp") * lists + 1
    for n, part in enumerate(parts):
        count = part.shape[0]
        tags = part[:, width:]
        lane = lax.broadcasted_iota(jnp.int32, (count, BLOCK), 1).astype(jnp.float32)
        members = []
        for lo in range(0, lists, BLOCK):
            members.append(jnp.where(tags == lane + (base + lo).astype(jnp.float32), 1.0, 0.0))
        if lists < BLOCK:
            members[0] = members[0][:, :lists]
        member = jnp.concatenate(members, axis=1).astype(jnp.bfloat16)
        dims = (((0,), (0,)), ((), ()))
        sums = jnp.zeros((lists, width), jnp.float32)
        for piece in split3(part[:, :width]):
            sums = sums + lax.dot_general(
                member, piece.astype(jnp.bfloat16), dims, preferred_element_type=jnp.float32
            )
        counts = lax.dot_general(
            member,
            jnp.ones((count, BLOCK), jnp.bfloat16),
            dims,
            preferred_element_type=jnp.float32,
        )
        if n == 0:
            s_ref[...] = sums
            c_ref[...] = counts
        else:
            s_ref[...] = s_ref[...] + sums
            c_ref[...] = c_ref[...] + counts
    solve_into(m_ref, s_ref[...], x_ref, 1.0 / jnp.maximum(c_ref[:, :1], 1.0))


def centroid_means_of(parts, inverse, lists):
    width = inverse.shape[0]
    vmem = pl.BlockSpec(memory_space=pltpu.VMEM)
    return pl.pallas_call(
        means_kernel,
        out_shape=jax.ShapeDtypeStruct((lists, width), jnp.float32),
        in_specs=[vmem] * (len(parts) + 1),
        out_specs=vmem,
        scratch_shapes=[
            pltpu.VMEM((lists, width), jnp.float32),
            pltpu.VMEM((lists, BLOCK), jnp.float32),
        ],
        compiler_params=pltpu.CompilerParams(vmem_limit_bytes=40 * 1024 * 1024),
    )(*parts, inverse)


def exchange(outgoing, owners):
    if owners > 16:
        got = lax.all_to_all(outgoing, "rows", split_axis=0, concat_axis=0, tiled=True)
        return got.reshape(-1, got.shape[-1])
    me = lax.axis_index("rows")
    got = [lax.dynamic_index_in_dim(outgoing, me, 0, keepdims=False)]
    for shift in range(1, owners):
        block = lax.dynamic_index_in_dim(outgoing, (me + shift) % owners, 0, keepdims=False)
        got.append(
            lax.ppermute(block, "rows", [(i, (i + shift) % owners) for i in range(owners)])
        )
    return jnp.concatenate(got, axis=0)


def body(embeddings, assignments):
    rows_here = embeddings.shape[0]
    width = embeddings.shape[1]
    owners = lax.axis_size("rows")
    groups = lax.axis_size("grp")
    total = rows_here * owners * groups
    gram = reduce_everywhere(local_gram(embeddings, owners * groups))

    per_owner = CENTROIDS // owners
    capacity = max(2, 2 * rows_here // owners)
    target = assignments // per_owner
    local = assignments % per_owner
    hits = (target[:, None] == jnp.arange(owners, dtype=jnp.int32)[None, :]).astype(jnp.int32)
    rank = jnp.sum(hits * (jnp.cumsum(hits, axis=0) - 1), axis=1)
    slot = target * capacity + rank
    tagged = jnp.concatenate(
        [
            embeddings,
            jnp.broadcast_to((local + 1).astype(jnp.float32)[:, None], (rows_here, BLOCK)),
        ],
        axis=1,
    )
    outgoing = jnp.zeros((owners * capacity, width + BLOCK), jnp.float32).at[slot].set(tagged)
    incoming = exchange(outgoing.reshape(owners, capacity, width + BLOCK), owners)
    incoming, gram = lax.optimization_barrier((incoming, gram))
    whitened, inverse = factor_and_whiten(gram, embeddings, total)
    parts = [incoming]
    for shift in range(1, groups):
        parts.append(
            lax.ppermute(incoming, "grp", [(i, (i + shift) % groups) for i in range(groups)])
        )
    means = centroid_means_of(parts, inverse, per_owner // groups)
    return (whitened, means)


def solution(mesh):
    return jax.shard_map(
        body,
        mesh=mesh,
        in_specs=(P(("rows", "grp"), None), P(("rows", "grp"))),
        out_specs=(P(("rows", "grp"), None), P(("rows", "grp"), None)),
        check_vma=False,
    )
```

```python
import functools

import jax
import jax.numpy as jnp
from jax import lax
from jax.experimental import pallas as pl
from jax.experimental.pallas import tpu as pltpu
from jax.sharding import PartitionSpec as P

CENTROIDS = 16384
BLOCK = 128
PANEL = 8


def split3(value):
    high = value.astype(jnp.bfloat16).astype(jnp.float32)
    rest = value - high
    mid = rest.astype(jnp.bfloat16).astype(jnp.float32)
    return high, mid, rest - mid


def dot(a, b, dims):
    return lax.dot_general(
        a, b, (dims, ((), ())), precision=lax.Precision.HIGHEST, preferred_element_type=jnp.float32
    )


def solve_into(out_ref, values, x_ref, scale=None):
    width = x_ref.shape[0]
    strip = 2 * BLOCK if width % (2 * BLOCK) == 0 else BLOCK
    high, mid, _ = split3(values)
    high, mid = high.astype(jnp.bfloat16), mid.astype(jnp.bfloat16)
    for lo in range(0, width, strip):
        hi = lo + strip
        xh, xm, _ = split3(x_ref[lo:hi, :hi])
        xh, xm = xh.astype(jnp.bfloat16), xm.astype(jnp.bfloat16)
        out = jnp.zeros((values.shape[0], strip), jnp.float32)
        for a, b in ((mid, xh), (high, xm), (high, xh)):
            out = out + lax.dot_general(
                a[:, :hi], b, (((1,), (1,)), ((), ())), preferred_element_type=jnp.float32
            )
        if scale is None:
            out_ref[:, lo:hi] = out
        else:
            out_ref[:, lo:hi] = out * scale


def lanes(value, lane):
    return jnp.broadcast_to(value[:, lane : lane + 1], (PANEL, BLOCK))


def sublanes(value, row):
    return jnp.broadcast_to(value[row : row + 1, :], (PANEL, BLOCK))


def merge_rows(rows):
    sub = lax.broadcasted_iota(jnp.int32, (PANEL, BLOCK), 0)
    out = rows[0]
    for i in range(1, PANEL):
        out = jnp.where(sub == i, rows[i], out)
    return out


def invert_block(d_ref, v_ref):
    groups = BLOCK // PANEL

    def load(g):
        rows = slice(g * PANEL, (g + 1) * PANEL)
        return d_ref[rows, :BLOCK], d_ref[rows, BLOCK:]

    def store(g, left, right):
        rows = slice(g * PANEL, (g + 1) * PANEL)
        d_ref[rows, :BLOCK] = left
        d_ref[rows, BLOCK:] = right

    left, right = load(0)
    for p in range(groups):
        first = p * PANEL
        near, middle, far = p + 1 < groups, p + 2 < groups, p + 3 < groups
        a = {}
        for j in range(PANEL):
            column = lanes(left, first + j)
            for i in range(j, PANEL):
                a[i, j] = sublanes(column, i)
        u = [sublanes(left, i) for i in range(PANEL)]
        v = [sublanes(right, i) for i in range(PANEL)]
        if near:
            next_left, next_right = load(p + 1)
            b = [lanes(next_left, first + j) for j in range(PANEL)]
        if far:
            gh, gm, gl = split3(left)
            lhs = jnp.concatenate([gh, gh, gm, gh, gm, gl], axis=0).astype(jnp.bfloat16)
        s = [None] * PANEL
        for j in range(PANEL):
            if j % 2 == 0:
                top, side, low = a[j, j], a[j + 1, j], a[j + 1, j + 1]
                s[j] = lax.rsqrt(top)
                s[j + 1] = lax.rsqrt(top * low - side * side) * (top * s[j])
            u[j] = u[j] * s[j]
            v[j] = v[j] * s[j]
            for i in range(j + 1, PANEL):
                a[i, j] = a[i, j] * s[j]
            for i in range(j + 1, PANEL):
                for k in range(j + 1, i + 1):
                    a[i, k] = a[i, k] - a[i, j] * a[k, j]
                u[i] = u[i] - a[i, j] * u[j]
                v[i] = v[i] - a[i, j] * v[j]
            if near:
                b[j] = b[j] * s[j]
                for k in range(j + 1, PANEL):
                    b[k] = b[k] - b[j] * a[k, j]
                next_left = next_left - b[j] * u[j]
                next_right = next_right - b[j] * v[j]
        v_ref[first : first + PANEL, :] = merge_rows(v)
        if near:
            left, right = next_left, next_right
        if middle:
            w, z = [None] * PANEL, [None] * PANEL
            for j in reversed(range(PANEL)):
                wj, zj = u[j], v[j]
                for k in range(j + 1, PANEL):
                    wj = wj - a[k, j] * w[k]
                    zj = zj - a[k, j] * z[k]
                w[j] = wj * s[j]
                z[j] = zj * s[j]
            x, y = load(p + 2)
            coefficients = [lanes(x, first + k) for k in range(PANEL)]
            for k in range(PANEL):
                x = x - coefficients[k] * w[k]
                y = y - coefficients[k] * z[k]
            store(p + 2, x, y)
        if far:
            wh, wm, wl = split3(merge_rows(w))
            zh, zm, zl = split3(merge_rows(z))
            rhs = jnp.concatenate(
                [
                    jnp.concatenate([wh, wm, wh, wl, wm, wh], axis=0),
                    jnp.concatenate([zh, zm, zh, zl, zm, zh], axis=0),
                ],
                axis=1,
            ).astype(jnp.bfloat16)
            update = lax.dot_general(
                lhs, rhs, (((0,), (0,)), ((), ())), preferred_element_type=jnp.float32
            )
            for g in range(p + 3, groups):
                x, y = load(g)
                rows = slice(g * PANEL, (g + 1) * PANEL)
                store(g, x - update[rows, :BLOCK], y - update[rows, BLOCK:])


def block_pairs(width):
    blocks = width // BLOCK
    return [(i, j) for i in range(blocks) for j in range(i, blocks)]


def gram_kernel(e_ref, g_ref):
    width = e_ref.shape[1]
    used = 0
    for i in range(width // BLOCK):
        lo = i * BLOCK
        strip = dot(e_ref[:, lo : lo + BLOCK], e_ref[:, lo:], ((0,), (0,)))
        for j in range(strip.shape[1] // BLOCK):
            g_ref[used : used + BLOCK, :] = strip[:, j * BLOCK : (j + 1) * BLOCK]
            used += BLOCK
    if used < g_ref.shape[0]:
        g_ref[used:, :] = jnp.zeros((g_ref.shape[0] - used, BLOCK), jnp.float32)


def local_gram(embeddings, devices):
    width = embeddings.shape[1]
    unit = devices * 8
    rows = len(block_pairs(width)) * BLOCK
    rows = (rows + unit - 1) // unit * unit
    vmem = pl.BlockSpec(memory_space=pltpu.VMEM)
    return pl.pallas_call(
        gram_kernel,
        out_shape=jax.ShapeDtypeStruct((rows, BLOCK), jnp.float32),
        in_specs=[vmem],
        out_specs=vmem,
        compiler_params=pltpu.CompilerParams(vmem_limit_bytes=32 * 1024 * 1024),
    )(embeddings)


def reduce_kernel(links, g_ref, out_ref, acc_ref, in_ref, send_sem, recv_sem):
    partners, bits = [], []
    for axis, bit in links:
        me = lax.axis_index(axis)
        one = lax.rem(me // bit, 2)
        bits.append(one)
        partners.append({axis: me + bit - 2 * bit * one})
    barrier = pltpu.get_barrier_semaphore()
    for partner in partners:
        pl.semaphore_signal(
            barrier, inc=1, device_id=partner, device_id_type=pl.DeviceIdType.MESH
        )
    pl.semaphore_wait(barrier, len(partners))
    steps = len(links)
    unit = 8
    for axis in ("grp", "rows"):
        unit *= lax.axis_size(axis)
    units = g_ref.shape[0] // unit
    streams = max(1, min(3, units, steps - 1))
    orders, sizes, starts = [], [], []
    first = 0
    for n in range(streams):
        size = (units // streams + (1 if n < units % streams else 0)) * unit
        orders.append([0] + [1 + (n + k) % (steps - 1) for k in range(steps - 1)])
        sizes.append(size)
        starts.append([first])
        first += size
    landed = [s[0] for s in starts]

    def send(source, source_start, target, target_start, rows, link, slot):
        copy = pltpu.make_async_remote_copy(
            src_ref=source.at[pl.ds(source_start, rows)],
            dst_ref=target.at[pl.ds(target_start, rows)],
            send_sem=send_sem.at[slot],
            recv_sem=recv_sem.at[slot],
            device_id=partners[link],
            device_id_type=pl.DeviceIdType.MESH,
        )
        copy.start()
        return copy

    for k in range(steps):
        source = g_ref if k == 0 else acc_ref
        target = out_ref if k == steps - 1 else acc_ref
        copies = []
        for n in range(streams):
            link, start, half = orders[n][k], starts[n][-1], sizes[n] // 2
            keep = pl.multiple_of(start + bits[link] * half, 8)
            give = pl.multiple_of(start + (1 - bits[link]) * half, 8)
            slot = k * streams + n
            copies.append(send(source, give, in_ref, landed[n], half, link, slot))
            starts[n].append(keep)
        for n in range(streams):
            half, keep = sizes[n] // 2, starts[n][-1]
            copies[n].wait()
            target[pl.ds(keep, half), :] = (
                source[pl.ds(keep, half), :] + in_ref[pl.ds(landed[n], half), :]
            )
            landed[n] += half
            sizes[n] = half
    for k in reversed(range(steps)):
        copies = []
        for n in range(streams):
            start = starts[n][k + 1]
            slot = (steps + k) * streams + n
            copies.append(send(out_ref, start, out_ref, start, sizes[n], orders[n][k], slot))
        for n in range(streams):
            copies[n].wait()
            sizes[n] *= 2


def reduce_everywhere(packed):
    links = []
    for axis in ("grp", "rows"):
        bit = 1
        while bit < lax.axis_size(axis):
            links.append((axis, bit))
            bit *= 2
    vmem = pl.BlockSpec(memory_space=pltpu.VMEM)
    return pl.pallas_call(
        functools.partial(reduce_kernel, links),
        out_shape=jax.ShapeDtypeStruct(packed.shape, jnp.float32),
        in_specs=[vmem],
        out_specs=vmem,
        scratch_shapes=[
            pltpu.VMEM(packed.shape, jnp.float32),
            pltpu.VMEM(packed.shape, jnp.float32),
            pltpu.SemaphoreType.DMA((6 * len(links),)),
            pltpu.SemaphoreType.DMA((6 * len(links),)),
        ],
        compiler_params=pltpu.CompilerParams(
            collective_id=0, has_side_effects=True, vmem_limit_bytes=24 * 1024 * 1024
        ),
    )(packed)


def factor_kernel_large(total, g_ref, e_ref, w_ref, x_ref, a_ref, d_ref, v_ref):
    width = x_ref.shape[0]
    r = lax.broadcasted_iota(jnp.int32, (BLOCK, BLOCK), 0)
    c = lax.broadcasted_iota(jnp.int32, (BLOCK, BLOCK), 1)
    eye = jnp.where(r == c, 1.0, 0.0).astype(jnp.float32)
    for n, (i, j) in enumerate(block_pairs(width)):
        a_ref[i * BLOCK : (i + 1) * BLOCK, j * BLOCK : (j + 1) * BLOCK] = (
            g_ref[n * BLOCK : (n + 1) * BLOCK, :] / total
        )
    x_ref[...] = jnp.zeros_like(x_ref)
    for lo in range(0, width, BLOCK):
        hi = lo + BLOCK
        here = slice(lo, hi)
        d_ref[:, :BLOCK] = a_ref[here, here] + 1e-05 * eye
        d_ref[:, BLOCK:] = eye
        invert_block(d_ref, v_ref)
        inv = v_ref[...]
        x_ref[here, here] = inv
        if lo > 0:
            x_ref[here, :lo] = dot(inv, x_ref[here, :lo], ((1,), (0,)))
        if hi < width:
            upper = dot(inv, a_ref[here, hi:], ((1,), (0,)))
            for row in range(hi, width, BLOCK):
                strip = slice(row, row + BLOCK)
                a_ref[strip, row:] = a_ref[strip, row:] - dot(
                    upper[:, row - hi : row - hi + BLOCK], upper[:, row - hi :], ((0,), (0,))
                )
            x_ref[hi:, :hi] = x_ref[hi:, :hi] - dot(upper, x_ref[here, :hi], ((0,), (0,)))
    solve_into(w_ref, e_ref[...], x_ref)


def factor_and_whiten(packed, embeddings, total):
    width = embeddings.shape[1]
    vmem = pl.BlockSpec(memory_space=pltpu.VMEM)
    return pl.pallas_call(
        functools.partial(factor_kernel_large, float(total)),
        out_shape=(
            jax.ShapeDtypeStruct(embeddings.shape, jnp.float32),
            jax.ShapeDtypeStruct((width, width), jnp.float32),
        ),
        in_specs=[vmem] * 2,
        out_specs=(vmem, vmem),
        scratch_shapes=[
            pltpu.VMEM((width, width), jnp.float32),
            pltpu.VMEM((BLOCK, 2 * BLOCK), jnp.float32),
            pltpu.VMEM((BLOCK, BLOCK), jnp.float32),
        ],
        cost_estimate=pl.CostEstimate(
            flops=12 * width**3, bytes_accessed=12 * width**2, transcendentals=width
        ),
        compiler_params=pltpu.CompilerParams(vmem_limit_bytes=32 * 1024 * 1024),
    )(packed, embeddings)


def flip(index, mask):
    bit = 1
    while bit <= mask:
        if mask & bit:
            index = index + bit - 2 * bit * lax.rem(index // bit, 2)
        bit *= 2
    return index


def rows_with(mask):
    return {"rows": flip(lax.axis_index("rows"), mask)}


def grp_with(mask):
    return {"grp": flip(lax.axis_index("grp"), mask)}


class Exchange:
    def __init__(self, out_ref, buf_ref, send_sem, recv_sem):
        self.owners = buf_ref.shape[0]
        self.out_ref, self.buf_ref = out_ref, buf_ref
        self.send_sem, self.recv_sem = send_sem, recv_sem
        self.row = lax.axis_index("rows")
        self.grp = lax.axis_index("grp")

    def copy(self, source, target, kind, mask, device):
        slot = kind * self.owners + mask
        return pltpu.make_async_remote_copy(
            src_ref=source,
            dst_ref=target,
            send_sem=self.send_sem.at[slot],
            recv_sem=self.recv_sem.at[slot],
            device_id=device,
            device_id_type=pl.DeviceIdType.MESH,
        )

    def local(self):
        return pltpu.make_async_copy(
            self.out_ref.at[self.row], self.buf_ref.at[self.row, self.grp], self.send_sem.at[0]
        )

    def first(self, mask):
        return self.copy(
            self.out_ref.at[flip(self.row, mask)],
            self.buf_ref.at[self.row, self.grp],
            0,
            mask,
            rows_with(mask),
        )

    def spread(self, mask, kind, origin, device):
        place = self.buf_ref.at[flip(self.row, mask), flip(self.grp, origin)]
        return self.copy(place, place, kind, mask, device)

    def across(self, mask):
        return self.spread(mask, 1, 0, grp_with(2))

    def beside(self, mask):
        return self.spread(mask, 2, 0, grp_with(1))

    def relay(self, mask):
        return self.spread(mask, 3, 2, grp_with(1))

    def greet(self):
        partners = [rows_with(m) for m in range(1, self.owners)]
        partners += [grp_with(2), grp_with(1)]
        barrier = pltpu.get_barrier_semaphore()
        for partner in partners:
            pl.semaphore_signal(
                barrier, inc=1, device_id=partner, device_id_type=pl.DeviceIdType.MESH
            )
        pl.semaphore_wait(barrier, len(partners))

    def begin(self):
        self.local().start()
        for m in range(1, self.owners):
            self.first(m).start()
        self.local().wait()
        self.across(0).start()
        self.beside(0).start()

    def waves(self):
        waves, low = [[0]], 1
        while low < self.owners:
            size = 1 if low == 1 else 2
            for m in range(low, 2 * low, size):
                waves.append(list(range(m, m + size)))
            low *= 2
        return waves

    def stage(self, c, last):
        waves = self.waves()
        for n, wave in enumerate(waves):
            for m in wave:
                if n > 0 and (n - 1 == c or (c == last and n - 1 > c)):
                    self.first(m).wait_recv()
                    self.across(m).start()
                    self.beside(m).start()
            if n == c or (c == last and n > c):
                for m in wave:
                    self.across(m).wait_recv()
                    self.relay(m).start()
        if c == last:
            for m in range(self.owners):
                self.beside(m).wait_recv()
                self.relay(m).wait_recv()
            for m in range(self.owners):
                if m > 0:
                    self.first(m).wait_send()
                self.across(m).wait_send()
                self.beside(m).wait_send()
                self.relay(m).wait_send()


def factor_kernel(
    total, g_ref, out_ref, x_ref, buf_ref, tag_ref, a_ref, d_ref, v_ref, send_sem, recv_sem
):
    width = x_ref.shape[0]
    blocks = width // BLOCK
    exchange = Exchange(out_ref, buf_ref, send_sem, recv_sem)
    exchange.greet()
    exchange.begin()
    r = lax.broadcasted_iota(jnp.int32, (BLOCK, BLOCK), 0)
    c = lax.broadcasted_iota(jnp.int32, (BLOCK, BLOCK), 1)
    eye = jnp.where(r == c, 1.0, 0.0).astype(jnp.float32)
    pairs = block_pairs(width)
    for n, (i, j) in enumerate(pairs):
        a_ref[i * BLOCK : (i + 1) * BLOCK, j * BLOCK : (j + 1) * BLOCK] = (
            g_ref[n * BLOCK : (n + 1) * BLOCK, :] / total
        )
    tags = tag_ref.shape[0]
    tag_ref[...] = g_ref[
        pl.ds(pl.multiple_of(len(pairs) * BLOCK + lax.axis_index("rows") * tags, tags), tags), :
    ]
    x_ref[...] = jnp.zeros_like(x_ref)

    def finish(k):
        lo = k * BLOCK
        hi = lo + BLOCK
        here = slice(lo, hi)
        inv = v_ref[...]
        x_ref[here, here] = inv
        if lo > 0:
            x_ref[here, :lo] = dot(inv, x_ref[here, :lo], ((1,), (0,)))
        if hi < width:
            upper = dot(inv, a_ref[here, hi:], ((1,), (0,)))
            for row in range(hi, width, BLOCK):
                strip = slice(row, row + BLOCK)
                a_ref[strip, row:] = a_ref[strip, row:] - dot(
                    upper[:, row - hi : row - hi + BLOCK], upper[:, row - hi :], ((0,), (0,))
                )
            x_ref[hi:, :hi] = x_ref[hi:, :hi] - dot(upper, x_ref[here, :hi], ((0,), (0,)))
        exchange.stage(k, blocks - 1)

    def step(k, carry):
        here = pl.ds(pl.multiple_of(k * BLOCK, BLOCK), BLOCK)
        d_ref[:, :BLOCK] = a_ref[here, here] + 1e-05 * eye
        d_ref[:, BLOCK:] = eye
        invert_block(d_ref, v_ref)
        for n in range(blocks):
            pl.when(k == n)(functools.partial(finish, n))
        return carry

    lax.fori_loop(0, blocks, step, 0)


def factor_and_exchange(packed, outgoing, width, total):
    owners, capacity = outgoing.shape[0], outgoing.shape[1]
    groups = lax.axis_size("grp")
    vmem = pl.BlockSpec(memory_space=pltpu.VMEM)
    tags = owners * groups * capacity // BLOCK
    return pl.pallas_call(
        functools.partial(factor_kernel, float(total)),
        out_shape=(
            jax.ShapeDtypeStruct((width, width), jnp.float32),
            jax.ShapeDtypeStruct((owners, groups, capacity, width), jnp.float32),
            jax.ShapeDtypeStruct((tags, BLOCK), jnp.float32),
        ),
        in_specs=[vmem] * 2,
        out_specs=(vmem,) * 3,
        scratch_shapes=[
            pltpu.VMEM((width, width), jnp.float32),
            pltpu.VMEM((BLOCK, 2 * BLOCK), jnp.float32),
            pltpu.VMEM((BLOCK, BLOCK), jnp.float32),
            pltpu.SemaphoreType.DMA((4 * owners,)),
            pltpu.SemaphoreType.DMA((4 * owners,)),
        ],
        compiler_params=pltpu.CompilerParams(
            collective_id=1, has_side_effects=True, vmem_limit_bytes=32 * 1024 * 1024
        ),
    )(packed, outgoing)


def refit_kernel(e_ref, x_ref, part_ref, tag_ref, w_ref, m_ref):
    solve_into(w_ref, e_ref[...], x_ref)
    lists, width = m_ref.shape
    base = lax.axis_index("grp") * lists + 1
    names = (lax.broadcasted_iota(jnp.int32, (lists, BLOCK), 0) + base).astype(jnp.float32)
    members = []
    for n in range(tag_ref.shape[0]):
        tag = jnp.broadcast_to(tag_ref[n : n + 1, :], (lists, BLOCK))
        members.append(jnp.where(tag == names, 1.0, 0.0))
    member = jnp.concatenate(members, axis=1).astype(jnp.bfloat16)
    dims = (((1,), (0,)), ((), ()))
    sums = jnp.zeros((lists, width), jnp.float32)
    for piece in split3(part_ref[...]):
        sums = sums + lax.dot_general(
            member, piece.astype(jnp.bfloat16), dims, preferred_element_type=jnp.float32
        )
    counts = lax.dot_general(
        member,
        jnp.ones((part_ref.shape[0], BLOCK), jnp.bfloat16),
        dims,
        preferred_element_type=jnp.float32,
    )
    solve_into(m_ref, sums, x_ref, 1.0 / jnp.maximum(counts[:, :1], 1.0))


def refit(embeddings, inverse, part, tags, lists):
    width = inverse.shape[0]
    vmem = pl.BlockSpec(memory_space=pltpu.VMEM)
    return pl.pallas_call(
        refit_kernel,
        out_shape=(
            jax.ShapeDtypeStruct(embeddings.shape, jnp.float32),
            jax.ShapeDtypeStruct((lists, width), jnp.float32),
        ),
        in_specs=[vmem] * 4,
        out_specs=(vmem,) * 2,
        compiler_params=pltpu.CompilerParams(vmem_limit_bytes=40 * 1024 * 1024),
    )(embeddings, inverse, part, tags)


def route_kernel(per_owner, e_ref, where_ref, g_ref, out_ref):
    owners, capacity, width = out_ref.shape
    rows = e_ref.shape[0]
    gram_kernel(e_ref, g_ref)
    lists = where_ref[...].astype(jnp.float32)
    target = jnp.floor((lists + 0.5) * (1.0 / per_owner))
    tag = lists - target * per_owner + 1.0
    across = jnp.broadcast_to(target, (rows, rows))
    down = across.T
    earlier = lax.broadcasted_iota(jnp.int32, (rows, rows), 0) < lax.broadcasted_iota(
        jnp.int32, (rows, rows), 1
    )
    same = jnp.where((across == down) & earlier, 1.0, 0.0)
    rank = jnp.sum(same, axis=0, keepdims=True)
    slot = target * capacity + rank
    names = lax.broadcasted_iota(jnp.int32, (owners * capacity, rows), 0).astype(jnp.float32)
    pick = jnp.where(names == jnp.broadcast_to(slot, names.shape), 1.0, 0.0).astype(jnp.bfloat16)
    dims = (((1,), (0,)), ((), ()))
    out = jnp.zeros((owners * capacity, width), jnp.float32)
    for piece in split3(e_ref[...]):
        out = out + lax.dot_general(
            pick, piece.astype(jnp.bfloat16), dims, preferred_element_type=jnp.float32
        )
    out_ref[...] = out.reshape(owners, capacity, width)
    me = lax.axis_index("rows") * lax.axis_size("grp") + lax.axis_index("grp")
    fit = BLOCK // capacity
    lane = lax.rem(me, fit) * capacity
    shown = lax.broadcasted_iota(jnp.int32, (BLOCK, rows), 0) - lane
    place = jnp.where(
        shown.astype(jnp.float32) == jnp.broadcast_to(rank, (BLOCK, rows)), 1.0, 0.0
    ).astype(jnp.bfloat16)
    owner = lax.broadcasted_iota(jnp.int32, (owners, rows), 0).astype(jnp.float32)
    mine = jnp.where(
        owner == jnp.broadcast_to(target, (owners, rows)),
        jnp.broadcast_to(tag, (owners, rows)),
        0.0,
    )
    table = jnp.zeros((owners, BLOCK), jnp.float32)
    for piece in split3(mine):
        table = table + lax.dot_general(
            piece.astype(jnp.bfloat16),
            place,
            (((1,), (1,)), ((), ())),
            preferred_element_type=jnp.float32,
        )
    base = len(block_pairs(width)) * BLOCK
    stride = owners * lax.axis_size("grp") * capacity // BLOCK
    for o in range(owners):
        g_ref[pl.ds(base + o * stride + me // fit, 1), :] = table[o : o + 1, :]


def route_and_gram(embeddings, assignments, owners, groups, capacity, per_owner):
    width = embeddings.shape[1]
    unit = owners * groups * 8
    rows = len(block_pairs(width)) * BLOCK + owners * owners * groups * capacity // BLOCK
    rows = (rows + unit - 1) // unit * unit
    vmem = pl.BlockSpec(memory_space=pltpu.VMEM)
    return pl.pallas_call(
        functools.partial(route_kernel, per_owner),
        out_shape=(
            jax.ShapeDtypeStruct((rows, BLOCK), jnp.float32),
            jax.ShapeDtypeStruct((owners, capacity, width), jnp.float32),
        ),
        in_specs=[vmem] * 2,
        out_specs=(vmem,) * 2,
        compiler_params=pltpu.CompilerParams(vmem_limit_bytes=32 * 1024 * 1024),
    )(embeddings, assignments.reshape(1, -1))


def means_kernel(*refs):
    parts, x_ref, m_ref, s_ref, c_ref = refs[:-4], refs[-4], refs[-3], refs[-2], refs[-1]
    lists, width = m_ref.shape
    base = lax.axis_index("grp") * lists + 1
    for n, part in enumerate(parts):
        count = part.shape[0]
        tags = part[:, width:]
        lane = lax.broadcasted_iota(jnp.int32, (count, BLOCK), 1).astype(jnp.float32)
        members = []
        for lo in range(0, lists, BLOCK):
            members.append(jnp.where(tags == lane + (base + lo).astype(jnp.float32), 1.0, 0.0))
        if lists < BLOCK:
            members[0] = members[0][:, :lists]
        member = jnp.concatenate(members, axis=1).astype(jnp.bfloat16)
        dims = (((0,), (0,)), ((), ()))
        sums = jnp.zeros((lists, width), jnp.float32)
        for piece in split3(part[:, :width]):
            sums = sums + lax.dot_general(
                member, piece.astype(jnp.bfloat16), dims, preferred_element_type=jnp.float32
            )
        counts = lax.dot_general(
            member,
            jnp.ones((count, BLOCK), jnp.bfloat16),
            dims,
            preferred_element_type=jnp.float32,
        )
        if n == 0:
            s_ref[...] = sums
            c_ref[...] = counts
        else:
            s_ref[...] = s_ref[...] + sums
            c_ref[...] = c_ref[...] + counts
    solve_into(m_ref, s_ref[...], x_ref, 1.0 / jnp.maximum(c_ref[:, :1], 1.0))


def centroid_means_of(parts, inverse, lists):
    width = inverse.shape[0]
    vmem = pl.BlockSpec(memory_space=pltpu.VMEM)
    return pl.pallas_call(
        means_kernel,
        out_shape=jax.ShapeDtypeStruct((lists, width), jnp.float32),
        in_specs=[vmem] * (len(parts) + 1),
        out_specs=vmem,
        scratch_shapes=[
            pltpu.VMEM((lists, width), jnp.float32),
            pltpu.VMEM((lists, BLOCK), jnp.float32),
        ],
        compiler_params=pltpu.CompilerParams(vmem_limit_bytes=40 * 1024 * 1024),
    )(*parts, inverse)


def exchange(outgoing, owners):
    if owners > 16:
        got = lax.all_to_all(outgoing, "rows", split_axis=0, concat_axis=0, tiled=True)
        return got.reshape(-1, got.shape[-1])
    me = lax.axis_index("rows")
    got = [lax.dynamic_index_in_dim(outgoing, me, 0, keepdims=False)]
    for shift in range(1, owners):
        block = lax.dynamic_index_in_dim(outgoing, (me + shift) % owners, 0, keepdims=False)
        got.append(
            lax.ppermute(block, "rows", [(i, (i + shift) % owners) for i in range(owners)])
        )
    return jnp.concatenate(got, axis=0)


def body_large(embeddings, assignments):
    rows_here = embeddings.shape[0]
    width = embeddings.shape[1]
    owners = lax.axis_size("rows")
    groups = lax.axis_size("grp")
    total = rows_here * owners * groups
    gram = reduce_everywhere(local_gram(embeddings, owners * groups))

    per_owner = CENTROIDS // owners
    capacity = max(2, 2 * rows_here // owners)
    target = assignments // per_owner
    local = assignments % per_owner
    hits = (target[:, None] == jnp.arange(owners, dtype=jnp.int32)[None, :]).astype(jnp.int32)
    rank = jnp.sum(hits * (jnp.cumsum(hits, axis=0) - 1), axis=1)
    slot = target * capacity + rank
    tagged = jnp.concatenate(
        [
            embeddings,
            jnp.broadcast_to((local + 1).astype(jnp.float32)[:, None], (rows_here, BLOCK)),
        ],
        axis=1,
    )
    outgoing = jnp.zeros((owners * capacity, width + BLOCK), jnp.float32).at[slot].set(tagged)
    incoming = exchange(outgoing.reshape(owners, capacity, width + BLOCK), owners)
    incoming, gram = lax.optimization_barrier((incoming, gram))
    whitened, inverse = factor_and_whiten(gram, embeddings, total)
    parts = [incoming]
    for shift in range(1, groups):
        parts.append(
            lax.ppermute(incoming, "grp", [(i, (i + shift) % groups) for i in range(groups)])
        )
    means = centroid_means_of(parts, inverse, per_owner // groups)
    return (whitened, means)


def body(embeddings, assignments):
    rows_here, width = embeddings.shape
    owners = lax.axis_size("rows")
    groups = lax.axis_size("grp")
    capacity = max(2, 2 * rows_here // owners)
    if owners & (owners - 1) or owners > 16 or groups != 4 or capacity % 8 or BLOCK % capacity:
        return body_large(embeddings, assignments)
    per_owner = CENTROIDS // owners
    packed, outgoing = route_and_gram(
        embeddings, assignments, owners, groups, capacity, per_owner
    )
    packed = reduce_everywhere(packed)
    inverse, part, tags = factor_and_exchange(
        packed, outgoing, width, rows_here * owners * groups
    )
    part = part.reshape(owners * groups * capacity, width)
    return refit(embeddings, inverse, part, tags, per_owner // groups)


def solution(mesh):
    return jax.shard_map(
        body,
        mesh=mesh,
        in_specs=(P(("rows", "grp"), None), P(("rows", "grp"))),
        out_specs=(P(("rows", "grp"), None), P(("rows", "grp"), None)),
        check_vma=False,
    )
```

```python
import functools

import jax
import jax.numpy as jnp
from jax import lax
from jax.experimental import pallas as pl
from jax.experimental.pallas import tpu as pltpu
from jax.sharding import PartitionSpec as P

CENTROIDS = 16384
BLOCK = 128
PANEL = 8


def split3(value):
    high = value.astype(jnp.bfloat16).astype(jnp.float32)
    rest = value - high
    mid = rest.astype(jnp.bfloat16).astype(jnp.float32)
    return high, mid, rest - mid


def dot(a, b, dims):
    return lax.dot_general(
        a, b, (dims, ((), ())), precision=lax.Precision.HIGHEST, preferred_element_type=jnp.float32
    )


def solve_into(out_ref, values, x_ref, scale=None):
    width = x_ref.shape[0]
    strip = 2 * BLOCK if width % (2 * BLOCK) == 0 else BLOCK
    high, mid, _ = split3(values)
    high, mid = high.astype(jnp.bfloat16), mid.astype(jnp.bfloat16)
    for lo in range(0, width, strip):
        hi = lo + strip
        xh, xm, _ = split3(x_ref[lo:hi, :hi])
        xh, xm = xh.astype(jnp.bfloat16), xm.astype(jnp.bfloat16)
        out = jnp.zeros((values.shape[0], strip), jnp.float32)
        for a, b in ((mid, xh), (high, xm), (high, xh)):
            out = out + lax.dot_general(
                a[:, :hi], b, (((1,), (1,)), ((), ())), preferred_element_type=jnp.float32
            )
        if scale is None:
            out_ref[:, lo:hi] = out
        else:
            out_ref[:, lo:hi] = out * scale


def lanes(value, lane):
    return jnp.broadcast_to(value[:, lane : lane + 1], (PANEL, BLOCK))


def sublanes(value, row):
    return jnp.broadcast_to(value[row : row + 1, :], (PANEL, BLOCK))


def merge_rows(rows):
    sub = lax.broadcasted_iota(jnp.int32, (PANEL, BLOCK), 0)
    out = rows[0]
    for i in range(1, PANEL):
        out = jnp.where(sub == i, rows[i], out)
    return out


def invert_block(d_ref, v_ref, hook=None):
    groups = BLOCK // PANEL

    def load(g):
        rows = slice(g * PANEL, (g + 1) * PANEL)
        return d_ref[rows, :BLOCK], d_ref[rows, BLOCK:]

    def store(g, left, right):
        rows = slice(g * PANEL, (g + 1) * PANEL)
        d_ref[rows, :BLOCK] = left
        d_ref[rows, BLOCK:] = right

    left, right = load(0)
    for p in range(groups):
        first = p * PANEL
        near, middle, far = p + 1 < groups, p + 2 < groups, p + 3 < groups
        a = {}
        for j in range(PANEL):
            column = lanes(left, first + j)
            for i in range(j, PANEL):
                a[i, j] = sublanes(column, i)
        u = [sublanes(left, i) for i in range(PANEL)]
        v = [sublanes(right, i) for i in range(PANEL)]
        if near:
            next_left, next_right = load(p + 1)
            b = [lanes(next_left, first + j) for j in range(PANEL)]
        if far:
            gh, gm, gl = split3(left)
            lhs = jnp.concatenate([gh, gh, gm, gh, gm, gl], axis=0).astype(jnp.bfloat16)
        s = [None] * PANEL
        for j in range(PANEL):
            if j % 2 == 0:
                top, side, low = a[j, j], a[j + 1, j], a[j + 1, j + 1]
                s[j] = lax.rsqrt(top)
                s[j + 1] = lax.rsqrt(top * low - side * side) * (top * s[j])
            u[j] = u[j] * s[j]
            v[j] = v[j] * s[j]
            for i in range(j + 1, PANEL):
                a[i, j] = a[i, j] * s[j]
            for i in range(j + 1, PANEL):
                for k in range(j + 1, i + 1):
                    a[i, k] = a[i, k] - a[i, j] * a[k, j]
                u[i] = u[i] - a[i, j] * u[j]
                v[i] = v[i] - a[i, j] * v[j]
            if near:
                b[j] = b[j] * s[j]
                for k in range(j + 1, PANEL):
                    b[k] = b[k] - b[j] * a[k, j]
                next_left = next_left - b[j] * u[j]
                next_right = next_right - b[j] * v[j]
        v_ref[first : first + PANEL, :] = merge_rows(v)
        if near:
            left, right = next_left, next_right
        if middle:
            w, z = [None] * PANEL, [None] * PANEL
            for j in reversed(range(PANEL)):
                wj, zj = u[j], v[j]
                for k in range(j + 1, PANEL):
                    wj = wj - a[k, j] * w[k]
                    zj = zj - a[k, j] * z[k]
                w[j] = wj * s[j]
                z[j] = zj * s[j]
            x, y = load(p + 2)
            coefficients = [lanes(x, first + k) for k in range(PANEL)]
            for k in range(PANEL):
                x = x - coefficients[k] * w[k]
                y = y - coefficients[k] * z[k]
            store(p + 2, x, y)
        if far:
            wh, wm, wl = split3(merge_rows(w))
            zh, zm, zl = split3(merge_rows(z))
            rhs = jnp.concatenate(
                [
                    jnp.concatenate([wh, wm, wh, wl, wm, wh], axis=0),
                    jnp.concatenate([zh, zm, zh, zl, zm, zh], axis=0),
                ],
                axis=1,
            ).astype(jnp.bfloat16)
            update = lax.dot_general(
                lhs, rhs, (((0,), (0,)), ((), ())), preferred_element_type=jnp.float32
            )
            for g in range(p + 3, groups):
                x, y = load(g)
                rows = slice(g * PANEL, (g + 1) * PANEL)
                store(g, x - update[rows, :BLOCK], y - update[rows, BLOCK:])
        if hook is not None:
            hook(p)


def block_pairs(width):
    blocks = width // BLOCK
    return [(i, j) for i in range(blocks) for j in range(i, blocks)]


def gram_kernel(e_ref, g_ref):
    width = e_ref.shape[1]
    used = 0
    for i in range(width // BLOCK):
        lo = i * BLOCK
        strip = dot(e_ref[:, lo : lo + BLOCK], e_ref[:, lo:], ((0,), (0,)))
        for j in range(strip.shape[1] // BLOCK):
            g_ref[used : used + BLOCK, :] = strip[:, j * BLOCK : (j + 1) * BLOCK]
            used += BLOCK
    if used < g_ref.shape[0]:
        g_ref[used:, :] = jnp.zeros((g_ref.shape[0] - used, BLOCK), jnp.float32)


def local_gram(embeddings, devices):
    width = embeddings.shape[1]
    unit = devices * 8
    rows = len(block_pairs(width)) * BLOCK
    rows = (rows + unit - 1) // unit * unit
    vmem = pl.BlockSpec(memory_space=pltpu.VMEM)
    return pl.pallas_call(
        gram_kernel,
        out_shape=jax.ShapeDtypeStruct((rows, BLOCK), jnp.float32),
        in_specs=[vmem],
        out_specs=vmem,
        compiler_params=pltpu.CompilerParams(vmem_limit_bytes=32 * 1024 * 1024),
    )(embeddings)


def reduce_kernel(links, g_ref, out_ref, acc_ref, in_ref, send_sem, recv_sem):
    partners, bits = [], []
    for axis, bit in links:
        me = lax.axis_index(axis)
        one = lax.rem(me // bit, 2)
        bits.append(one)
        partners.append({axis: me + bit - 2 * bit * one})
    barrier = pltpu.get_barrier_semaphore()
    for partner in partners:
        pl.semaphore_signal(
            barrier, inc=1, device_id=partner, device_id_type=pl.DeviceIdType.MESH
        )
    pl.semaphore_wait(barrier, len(partners))
    steps = len(links)
    unit = 8
    for axis in ("grp", "rows"):
        unit *= lax.axis_size(axis)
    units = g_ref.shape[0] // unit
    streams = max(1, min(3, units, steps - 1))
    orders, sizes, starts = [], [], []
    first = 0
    for n in range(streams):
        size = (units // streams + (1 if n < units % streams else 0)) * unit
        orders.append([0] + [1 + (n + k) % (steps - 1) for k in range(steps - 1)])
        sizes.append(size)
        starts.append([first])
        first += size
    landed = [s[0] for s in starts]

    def send(source, source_start, target, target_start, rows, link, slot):
        copy = pltpu.make_async_remote_copy(
            src_ref=source.at[pl.ds(source_start, rows)],
            dst_ref=target.at[pl.ds(target_start, rows)],
            send_sem=send_sem.at[slot],
            recv_sem=recv_sem.at[slot],
            device_id=partners[link],
            device_id_type=pl.DeviceIdType.MESH,
        )
        copy.start()
        return copy

    for k in range(steps):
        source = g_ref if k == 0 else acc_ref
        target = out_ref if k == steps - 1 else acc_ref
        copies = []
        for n in range(streams):
            link, start, half = orders[n][k], starts[n][-1], sizes[n] // 2
            keep = pl.multiple_of(start + bits[link] * half, 8)
            give = pl.multiple_of(start + (1 - bits[link]) * half, 8)
            slot = k * streams + n
            copies.append(send(source, give, in_ref, landed[n], half, link, slot))
            starts[n].append(keep)
        for n in range(streams):
            half, keep = sizes[n] // 2, starts[n][-1]
            copies[n].wait()
            target[pl.ds(keep, half), :] = (
                source[pl.ds(keep, half), :] + in_ref[pl.ds(landed[n], half), :]
            )
            landed[n] += half
            sizes[n] = half
    for k in reversed(range(steps)):
        copies = []
        for n in range(streams):
            start = starts[n][k + 1]
            slot = (steps + k) * streams + n
            copies.append(send(out_ref, start, out_ref, start, sizes[n], orders[n][k], slot))
        for n in range(streams):
            copies[n].wait()
            sizes[n] *= 2


def reduce_everywhere(packed):
    links = []
    for axis in ("grp", "rows"):
        bit = 1
        while bit < lax.axis_size(axis):
            links.append((axis, bit))
            bit *= 2
    vmem = pl.BlockSpec(memory_space=pltpu.VMEM)
    return pl.pallas_call(
        functools.partial(reduce_kernel, links),
        out_shape=jax.ShapeDtypeStruct(packed.shape, jnp.float32),
        in_specs=[vmem],
        out_specs=vmem,
        scratch_shapes=[
            pltpu.VMEM(packed.shape, jnp.float32),
            pltpu.VMEM(packed.shape, jnp.float32),
            pltpu.SemaphoreType.DMA((6 * len(links),)),
            pltpu.SemaphoreType.DMA((6 * len(links),)),
        ],
        compiler_params=pltpu.CompilerParams(
            collective_id=0, has_side_effects=True, vmem_limit_bytes=24 * 1024 * 1024
        ),
    )(packed)


def factor_kernel_large(total, g_ref, e_ref, w_ref, x_ref, a_ref, d_ref, v_ref):
    width = x_ref.shape[0]
    r = lax.broadcasted_iota(jnp.int32, (BLOCK, BLOCK), 0)
    c = lax.broadcasted_iota(jnp.int32, (BLOCK, BLOCK), 1)
    eye = jnp.where(r == c, 1.0, 0.0).astype(jnp.float32)
    for n, (i, j) in enumerate(block_pairs(width)):
        a_ref[i * BLOCK : (i + 1) * BLOCK, j * BLOCK : (j + 1) * BLOCK] = (
            g_ref[n * BLOCK : (n + 1) * BLOCK, :] / total
        )
    x_ref[...] = jnp.zeros_like(x_ref)
    for lo in range(0, width, BLOCK):
        hi = lo + BLOCK
        here = slice(lo, hi)
        d_ref[:, :BLOCK] = a_ref[here, here] + 1e-05 * eye
        d_ref[:, BLOCK:] = eye
        invert_block(d_ref, v_ref)
        inv = v_ref[...]
        x_ref[here, here] = inv
        if lo > 0:
            x_ref[here, :lo] = dot(inv, x_ref[here, :lo], ((1,), (0,)))
        if hi < width:
            upper = dot(inv, a_ref[here, hi:], ((1,), (0,)))
            for row in range(hi, width, BLOCK):
                strip = slice(row, row + BLOCK)
                a_ref[strip, row:] = a_ref[strip, row:] - dot(
                    upper[:, row - hi : row - hi + BLOCK], upper[:, row - hi :], ((0,), (0,))
                )
            x_ref[hi:, :hi] = x_ref[hi:, :hi] - dot(upper, x_ref[here, :hi], ((0,), (0,)))
    solve_into(w_ref, e_ref[...], x_ref)


def factor_and_whiten(packed, embeddings, total):
    width = embeddings.shape[1]
    vmem = pl.BlockSpec(memory_space=pltpu.VMEM)
    return pl.pallas_call(
        functools.partial(factor_kernel_large, float(total)),
        out_shape=(
            jax.ShapeDtypeStruct(embeddings.shape, jnp.float32),
            jax.ShapeDtypeStruct((width, width), jnp.float32),
        ),
        in_specs=[vmem] * 2,
        out_specs=(vmem, vmem),
        scratch_shapes=[
            pltpu.VMEM((width, width), jnp.float32),
            pltpu.VMEM((BLOCK, 2 * BLOCK), jnp.float32),
            pltpu.VMEM((BLOCK, BLOCK), jnp.float32),
        ],
        cost_estimate=pl.CostEstimate(
            flops=12 * width**3, bytes_accessed=12 * width**2, transcendentals=width
        ),
        compiler_params=pltpu.CompilerParams(vmem_limit_bytes=32 * 1024 * 1024),
    )(packed, embeddings)


def flip(index, mask):
    bit = 1
    while bit <= mask:
        if mask & bit:
            index = index + bit - 2 * bit * lax.rem(index // bit, 2)
        bit *= 2
    return index


def rows_with(mask):
    return {"rows": flip(lax.axis_index("rows"), mask)}


def grp_with(mask):
    return {"grp": flip(lax.axis_index("grp"), mask)}


class Exchange:
    def __init__(self, out_ref, buf_ref, send_sem, recv_sem):
        self.owners = buf_ref.shape[0]
        self.out_ref, self.buf_ref = out_ref, buf_ref
        self.send_sem, self.recv_sem = send_sem, recv_sem
        self.row = lax.axis_index("rows")
        self.grp = lax.axis_index("grp")

    def copy(self, source, target, kind, mask, device):
        slot = kind * self.owners + mask
        return pltpu.make_async_remote_copy(
            src_ref=source,
            dst_ref=target,
            send_sem=self.send_sem.at[slot],
            recv_sem=self.recv_sem.at[slot],
            device_id=device,
            device_id_type=pl.DeviceIdType.MESH,
        )

    def local(self):
        return pltpu.make_async_copy(
            self.out_ref.at[self.row], self.buf_ref.at[self.row, self.grp], self.send_sem.at[0]
        )

    def first(self, mask):
        return self.copy(
            self.out_ref.at[flip(self.row, mask)],
            self.buf_ref.at[self.row, self.grp],
            0,
            mask,
            rows_with(mask),
        )

    def spread(self, mask, kind, origin, device):
        place = self.buf_ref.at[flip(self.row, mask), flip(self.grp, origin)]
        return self.copy(place, place, kind, mask, device)

    def across(self, mask):
        return self.spread(mask, 1, 0, grp_with(2))

    def beside(self, mask):
        return self.spread(mask, 2, 0, grp_with(1))

    def relay(self, mask):
        return self.spread(mask, 3, 2, grp_with(1))

    def take(self, mask):
        self.first(mask).wait_recv()

    def forward(self, mask):
        self.across(mask).start()
        self.beside(mask).start()

    def hand(self, mask):
        self.across(mask).wait_recv()
        self.relay(mask).start()

    def close(self):
        for m in range(self.owners):
            self.beside(m).wait_recv()
            self.relay(m).wait_recv()
        for m in range(self.owners):
            if m > 0:
                self.first(m).wait_send()
            self.across(m).wait_send()
            self.beside(m).wait_send()
            self.relay(m).wait_send()


class Reduce:
    def __init__(self, index, start, size, refs, direct):
        self.index, self.start, self.size, self.direct = index, start, size, direct
        self.g, self.acc, self.land, self.far, self.out, self.send_sem, self.recv_sem = refs
        self.row = lax.axis_index("rows")
        self.grp = lax.axis_index("grp")
        self.depth = lax.axis_size("rows") // 2
        self.peers = self.depth - 1
        core, x = lax.rem(self.grp, 2), self.grp // 2
        y, z = lax.rem(self.row, 2), self.row // 2
        self.core, self.quarter, self.z = core, 2 * x + y, z
        self.half = self.at(start + core * (size // 2))
        self.eighth = self.at(self.half + self.quarter * (size // 8))
        self.piece = size // (8 * self.depth)

    def at(self, value):
        return pl.multiple_of(value, 8)

    def copy(self, source, source_start, target, target_start, rows, slot, device):
        n = self.index * (8 + 2 * self.peers) + slot
        return pltpu.make_async_remote_copy(
            src_ref=source.at[pl.ds(source_start, rows)],
            dst_ref=target.at[pl.ds(target_start, rows)],
            send_sem=self.send_sem.at[n],
            recv_sem=self.recv_sem.at[n],
            device_id=device,
            device_id_type=pl.DeviceIdType.MESH,
        )

    def plane(self, m):
        return {"grp": flip(self.grp, 2 * (m // 2)), "rows": flip(self.row, m % 2)}

    def copies(self, step):
        size, start = self.size, self.start
        if step == "core":
            give = self.at(start + (1 - self.core) * (size // 2))
            return [
                self.copy(self.g, give, self.land, start, size // 2, 0, grp_with(1))
            ]
        if step == "plane":
            rows, out = size // 8, []
            for m in range(1, 4):
                give = self.at(self.half + flip(self.quarter, m) * rows)
                place = start + size // 2 + (m - 1) * rows
                out.append(self.copy(self.acc, give, self.land, place, rows, m, self.plane(m)))
            return out
        if step == "deep":
            out = []
            for m in range(1, self.depth):
                if self.direct:
                    rows = size // 8
                    give, target, place = self.eighth, self.far, (m - 1) * rows
                else:
                    rows = self.piece
                    give = self.at(self.eighth + flip(self.z, m) * rows)
                    target, place = self.land, start + 7 * (size // 8) + (m - 1) * rows
                out.append(
                    self.copy(self.acc, give, target, place, rows, 3 + m, rows_with(2 * m))
                )
            return out
        if step == "deep back":
            own = self.at(self.eighth + self.z * self.piece)
            return [
                self.copy(
                    self.out, own, self.out, own, self.piece, 3 + self.peers + m, rows_with(2 * m)
                )
                for m in range(1, self.depth)
            ]
        base = 4 + 2 * self.peers
        if step == "plane back":
            return [
                self.copy(
                    self.out, self.eighth, self.out, self.eighth, size // 8, base + m - 1,
                    self.plane(m),
                )
                for m in range(1, 4)
            ]
        return [
            self.copy(self.out, self.half, self.out, self.half, size // 2, base + 3, grp_with(1))
        ]

    def send(self, step):
        for copy in self.copies(step):
            copy.start()

    def take(self, step):
        for copy in self.copies(step):
            copy.wait_recv()
        size, start = self.size, self.start
        if step == "core":
            rows = size // 2
            here = pl.ds(self.half, rows)
            self.acc[here, :] = self.g[here, :] + self.land[start : start + rows, :]
        elif step == "plane":
            rows = size // 8
            here = pl.ds(self.eighth, rows)
            total = self.acc[here, :]
            for m in range(3):
                place = start + size // 2 + m * rows
                total = total + self.land[place : place + rows, :]
            self.acc[here, :] = total
        elif step == "deep":
            if self.direct:
                rows, source, base = size // 8, self.far, 0
                here = pl.ds(self.eighth, rows)
            else:
                rows, source, base = self.piece, self.land, start + 7 * (size // 8)
                here = pl.ds(self.at(self.eighth + self.z * rows), rows)
            total = self.acc[here, :]
            for m in range(self.peers):
                total = total + source[base + m * rows : base + (m + 1) * rows, :]
            self.out[here, :] = total

    def steps(self):
        middle = ("deep",) if self.direct else ("deep", "deep back")
        return ("core", "plane") + middle + ("plane back", "core back")

    def move(self, step):
        steps = self.steps()
        self.take(step)
        n = steps.index(step)
        if n + 1 < len(steps):
            self.send(steps[n + 1])

    def close(self):
        for step in self.steps():
            for copy in self.copies(step):
                copy.wait_send()


def gram_strip(e_ref, g_ref, i):
    width = e_ref.shape[1]
    blocks = width // BLOCK
    used = sum(blocks - n for n in range(i)) * BLOCK
    lo = i * BLOCK
    strip = dot(e_ref[:, lo : lo + BLOCK], e_ref[:, lo:], ((0,), (0,)))
    for j in range(blocks - i):
        g_ref[used : used + BLOCK, :] = strip[:, j * BLOCK : (j + 1) * BLOCK]
        used += BLOCK
    return used


def whole_kernel(
    total, per_owner, sizes, e_ref, where_ref, x_ref, buf_ref, tag_ref,
    g_ref, acc_ref, land_ref, far_ref, sum_ref, out_ref, a_ref, d_ref, v_ref,
    gram_send, gram_recv, send_sem, recv_sem,
):
    width = x_ref.shape[0]
    blocks = width // BLOCK
    owners = buf_ref.shape[0]
    exchange = Exchange(out_ref, buf_ref, send_sem, recv_sem)
    refs = (g_ref, acc_ref, land_ref, far_ref, sum_ref, gram_send, gram_recv)
    chunks, start = [], 0
    for n, size in enumerate(sizes):
        chunks.append(Reduce(n, start, size, refs, n == 0))
        start += size
    first, second, third, fourth = chunks

    partners = [rows_with(m) for m in range(1, owners)]
    partners += [grp_with(1), grp_with(2), first.plane(3)]
    barrier = pltpu.get_barrier_semaphore()
    for partner in partners:
        pl.semaphore_signal(barrier, inc=1, device_id=partner, device_id_type=pl.DeviceIdType.MESH)
    gram_strip(e_ref, g_ref, 0)
    pl.semaphore_wait(barrier, len(partners))
    first.send("core")
    second.send("core")
    for i in range(1, blocks):
        used = gram_strip(e_ref, g_ref, i)
    g_ref[used:, :] = jnp.zeros((g_ref.shape[0] - used, BLOCK), jnp.float32)
    route(per_owner, e_ref, where_ref, g_ref, out_ref)
    third.send("core")
    fourth.send("core")
    exchange.local().start()
    top = owners // 2
    if top > 1:
        exchange.first(top).start()
    for chunk in chunks:
        chunk.move("core")
    a_ref[...] = jnp.zeros_like(a_ref)
    x_ref[...] = jnp.zeros_like(x_ref)
    r = lax.broadcasted_iota(jnp.int32, (BLOCK, BLOCK), 0)
    c = lax.broadcasted_iota(jnp.int32, (BLOCK, BLOCK), 1)
    eye = jnp.where(r == c, 1.0, 0.0).astype(jnp.float32)
    exchange.local().wait()
    first.move("plane")
    second.move("plane")
    third.move("plane")
    first.move("deep")
    second.move("deep")
    fourth.move("plane")
    first.move("plane back")
    third.move("deep")
    exchange.forward(0)
    near = [m for m in range(2, owners) if m < 4 and m != top]
    for m in near:
        exchange.first(m).start()
    first.move("core back")

    rest = [m for m in range(1, owners) if m != top and m not in near]
    early = [m for m in [top] + near if m > 0]
    tags = tag_ref.shape[0]
    pairs = block_pairs(width)

    def copy_tags():
        tag_ref[...] = sum_ref[
            pl.ds(pl.multiple_of(len(pairs) * BLOCK + exchange.row * tags, tags), tags), :
        ]

    def do(*actions):
        def run():
            for function, *arguments in actions:
                function(*arguments)
        return run

    inside = {
        (0, 3): do((second.move, "deep back")),
        (0, 11): do((fourth.move, "deep")),
    }
    ending = {
        0: do(
            (third.move, "deep back"), (second.move, "plane back"), (second.move, "core back")
        ),
        1: do(
            (fourth.move, "plane back"),
            *[(exchange.take, m) for m in early],
            *[(exchange.forward, m) for m in early],
        ),
        2: do(*[(exchange.take, m) for m in rest], *[(exchange.forward, m) for m in rest]),
        3: do(*[(exchange.hand, m) for m in [0] + early]),
        blocks - 1: do(*[(exchange.hand, m) for m in rest]),
    }
    opening = {
        1: do(
            *[(exchange.first(m).start,) for m in rest],
            (third.move, "plane back"), (fourth.move, "deep back"), (third.move, "core back"),
        ),
        2: do((fourth.move, "core back"), (copy_tags,)),
    }

    def add(i, j):
        n = pairs.index((i, j))
        here = (slice(i * BLOCK, (i + 1) * BLOCK), slice(j * BLOCK, (j + 1) * BLOCK))
        a_ref[here] = a_ref[here] + sum_ref[n * BLOCK : (n + 1) * BLOCK, :] / total

    def open_block(k):
        if k in opening:
            opening[k]()
        add(k, k)

    def finish(k):
        lo = k * BLOCK
        hi = lo + BLOCK
        here = slice(lo, hi)
        if k in ending:
            ending[k]()
        for j in range(k + 1, blocks):
            add(k, j)
        inv = v_ref[...]
        x_ref[here, here] = inv
        if lo > 0:
            x_ref[here, :lo] = dot(inv, x_ref[here, :lo], ((1,), (0,)))
        if hi < width:
            upper = dot(inv, a_ref[here, hi:], ((1,), (0,)))
            for row in range(hi, width, BLOCK):
                strip = slice(row, row + BLOCK)
                a_ref[strip, row:] = a_ref[strip, row:] - dot(
                    upper[:, row - hi : row - hi + BLOCK], upper[:, row - hi :], ((0,), (0,))
                )
            x_ref[hi:, :hi] = x_ref[hi:, :hi] - dot(upper, x_ref[here, :hi], ((0,), (0,)))

    def step(k, carry):
        for n in range(blocks):
            pl.when(k == n)(functools.partial(open_block, n))
        here = pl.ds(pl.multiple_of(k * BLOCK, BLOCK), BLOCK)
        d_ref[:, :BLOCK] = a_ref[here, here] + 1e-05 * eye
        d_ref[:, BLOCK:] = eye

        def hook(p):
            for (n, at), run in inside.items():
                if at == p:
                    pl.when(k == n)(run)

        invert_block(d_ref, v_ref, hook)
        for n in range(blocks):
            pl.when(k == n)(functools.partial(finish, n))
        return carry

    lax.fori_loop(0, blocks, step, 0)
    for chunk in chunks:
        chunk.close()
    exchange.close()


def factor_everywhere(embeddings, assignments, owners, groups, capacity, per_owner):
    width = embeddings.shape[1]
    devices = owners * groups
    unit = devices * 8
    gram_rows = len(block_pairs(width)) * BLOCK
    tags = devices * capacity // BLOCK
    rows = (gram_rows + owners * tags + unit - 1) // unit * unit
    strip = (width // BLOCK) * BLOCK
    sizes = [unit, strip - unit, unit * ((strip + unit - 1) // unit)]
    sizes.append(rows - sum(sizes))
    vmem = pl.BlockSpec(memory_space=pltpu.VMEM)
    packed = pltpu.VMEM((rows, BLOCK), jnp.float32)
    gram_copies = len(sizes) * (8 + 2 * (owners // 2 - 1))
    return pl.pallas_call(
        functools.partial(
            whole_kernel, float(embeddings.shape[0] * devices), per_owner, tuple(sizes)
        ),
        out_shape=(
            jax.ShapeDtypeStruct((width, width), jnp.float32),
            jax.ShapeDtypeStruct((owners, groups, capacity, width), jnp.float32),
            jax.ShapeDtypeStruct((tags, BLOCK), jnp.float32),
        ),
        in_specs=[vmem] * 2,
        out_specs=(vmem,) * 3,
        scratch_shapes=[
            packed,
            packed,
            packed,
            pltpu.VMEM(((owners // 2 - 1) * unit // 8, BLOCK), jnp.float32),
            packed,
            pltpu.VMEM((owners, capacity, width), jnp.float32),
            pltpu.VMEM((width, width), jnp.float32),
            pltpu.VMEM((BLOCK, 2 * BLOCK), jnp.float32),
            pltpu.VMEM((BLOCK, BLOCK), jnp.float32),
            pltpu.SemaphoreType.DMA((gram_copies,)),
            pltpu.SemaphoreType.DMA((gram_copies,)),
            pltpu.SemaphoreType.DMA((4 * owners,)),
            pltpu.SemaphoreType.DMA((4 * owners,)),
        ],
        compiler_params=pltpu.CompilerParams(
            collective_id=1, has_side_effects=True, vmem_limit_bytes=36 * 1024 * 1024
        ),
    )(embeddings, assignments.reshape(1, -1))


def refit_kernel(e_ref, x_ref, part_ref, tag_ref, w_ref, m_ref):
    solve_into(w_ref, e_ref[...], x_ref)
    lists, width = m_ref.shape
    base = lax.axis_index("grp") * lists + 1
    names = (lax.broadcasted_iota(jnp.int32, (lists, BLOCK), 0) + base).astype(jnp.float32)
    members = []
    for n in range(tag_ref.shape[0]):
        tag = jnp.broadcast_to(tag_ref[n : n + 1, :], (lists, BLOCK))
        members.append(jnp.where(tag == names, 1.0, 0.0))
    member = jnp.concatenate(members, axis=1).astype(jnp.bfloat16)
    dims = (((1,), (0,)), ((), ()))
    sums = jnp.zeros((lists, width), jnp.float32)
    for piece in split3(part_ref[...]):
        sums = sums + lax.dot_general(
            member, piece.astype(jnp.bfloat16), dims, preferred_element_type=jnp.float32
        )
    counts = lax.dot_general(
        member,
        jnp.ones((part_ref.shape[0], BLOCK), jnp.bfloat16),
        dims,
        preferred_element_type=jnp.float32,
    )
    solve_into(m_ref, sums, x_ref, 1.0 / jnp.maximum(counts[:, :1], 1.0))


def refit(embeddings, inverse, part, tags, lists):
    width = inverse.shape[0]
    vmem = pl.BlockSpec(memory_space=pltpu.VMEM)
    return pl.pallas_call(
        refit_kernel,
        out_shape=(
            jax.ShapeDtypeStruct(embeddings.shape, jnp.float32),
            jax.ShapeDtypeStruct((lists, width), jnp.float32),
        ),
        in_specs=[vmem] * 4,
        out_specs=(vmem,) * 2,
        compiler_params=pltpu.CompilerParams(vmem_limit_bytes=40 * 1024 * 1024),
    )(embeddings, inverse, part, tags)


def route(per_owner, e_ref, where_ref, g_ref, out_ref):
    owners, capacity, width = out_ref.shape
    rows = e_ref.shape[0]
    lists = where_ref[...].astype(jnp.float32)
    target = jnp.floor((lists + 0.5) * (1.0 / per_owner))
    tag = lists - target * per_owner + 1.0
    across = jnp.broadcast_to(target, (rows, rows))
    down = across.T
    earlier = lax.broadcasted_iota(jnp.int32, (rows, rows), 0) < lax.broadcasted_iota(
        jnp.int32, (rows, rows), 1
    )
    same = jnp.where((across == down) & earlier, 1.0, 0.0)
    rank = jnp.sum(same, axis=0, keepdims=True)
    slot = target * capacity + rank
    names = lax.broadcasted_iota(jnp.int32, (owners * capacity, rows), 0).astype(jnp.float32)
    pick = jnp.where(names == jnp.broadcast_to(slot, names.shape), 1.0, 0.0).astype(jnp.bfloat16)
    dims = (((1,), (0,)), ((), ()))
    out = jnp.zeros((owners * capacity, width), jnp.float32)
    for piece in split3(e_ref[...]):
        out = out + lax.dot_general(
            pick, piece.astype(jnp.bfloat16), dims, preferred_element_type=jnp.float32
        )
    out_ref[...] = out.reshape(owners, capacity, width)
    me = lax.axis_index("rows") * lax.axis_size("grp") + lax.axis_index("grp")
    fit = BLOCK // capacity
    lane = lax.rem(me, fit) * capacity
    shown = lax.broadcasted_iota(jnp.int32, (BLOCK, rows), 0) - lane
    place = jnp.where(
        shown.astype(jnp.float32) == jnp.broadcast_to(rank, (BLOCK, rows)), 1.0, 0.0
    ).astype(jnp.bfloat16)
    owner = lax.broadcasted_iota(jnp.int32, (owners, rows), 0).astype(jnp.float32)
    mine = jnp.where(
        owner == jnp.broadcast_to(target, (owners, rows)),
        jnp.broadcast_to(tag, (owners, rows)),
        0.0,
    )
    table = jnp.zeros((owners, BLOCK), jnp.float32)
    for piece in split3(mine):
        table = table + lax.dot_general(
            piece.astype(jnp.bfloat16),
            place,
            (((1,), (1,)), ((), ())),
            preferred_element_type=jnp.float32,
        )
    base = len(block_pairs(width)) * BLOCK
    stride = owners * lax.axis_size("grp") * capacity // BLOCK
    for o in range(owners):
        g_ref[pl.ds(base + o * stride + me // fit, 1), :] = table[o : o + 1, :]


def means_kernel(*refs):
    parts, x_ref, m_ref, s_ref, c_ref = refs[:-4], refs[-4], refs[-3], refs[-2], refs[-1]
    lists, width = m_ref.shape
    base = lax.axis_index("grp") * lists + 1
    for n, part in enumerate(parts):
        count = part.shape[0]
        tags = part[:, width:]
        lane = lax.broadcasted_iota(jnp.int32, (count, BLOCK), 1).astype(jnp.float32)
        members = []
        for lo in range(0, lists, BLOCK):
            members.append(jnp.where(tags == lane + (base + lo).astype(jnp.float32), 1.0, 0.0))
        if lists < BLOCK:
            members[0] = members[0][:, :lists]
        member = jnp.concatenate(members, axis=1).astype(jnp.bfloat16)
        dims = (((0,), (0,)), ((), ()))
        sums = jnp.zeros((lists, width), jnp.float32)
        for piece in split3(part[:, :width]):
            sums = sums + lax.dot_general(
                member, piece.astype(jnp.bfloat16), dims, preferred_element_type=jnp.float32
            )
        counts = lax.dot_general(
            member,
            jnp.ones((count, BLOCK), jnp.bfloat16),
            dims,
            preferred_element_type=jnp.float32,
        )
        if n == 0:
            s_ref[...] = sums
            c_ref[...] = counts
        else:
            s_ref[...] = s_ref[...] + sums
            c_ref[...] = c_ref[...] + counts
    solve_into(m_ref, s_ref[...], x_ref, 1.0 / jnp.maximum(c_ref[:, :1], 1.0))


def centroid_means_of(parts, inverse, lists):
    width = inverse.shape[0]
    vmem = pl.BlockSpec(memory_space=pltpu.VMEM)
    return pl.pallas_call(
        means_kernel,
        out_shape=jax.ShapeDtypeStruct((lists, width), jnp.float32),
        in_specs=[vmem] * (len(parts) + 1),
        out_specs=vmem,
        scratch_shapes=[
            pltpu.VMEM((lists, width), jnp.float32),
            pltpu.VMEM((lists, BLOCK), jnp.float32),
        ],
        compiler_params=pltpu.CompilerParams(vmem_limit_bytes=40 * 1024 * 1024),
    )(*parts, inverse)


def exchange(outgoing, owners):
    if owners > 16:
        got = lax.all_to_all(outgoing, "rows", split_axis=0, concat_axis=0, tiled=True)
        return got.reshape(-1, got.shape[-1])
    me = lax.axis_index("rows")
    got = [lax.dynamic_index_in_dim(outgoing, me, 0, keepdims=False)]
    for shift in range(1, owners):
        block = lax.dynamic_index_in_dim(outgoing, (me + shift) % owners, 0, keepdims=False)
        got.append(
            lax.ppermute(block, "rows", [(i, (i + shift) % owners) for i in range(owners)])
        )
    return jnp.concatenate(got, axis=0)


def body_large(embeddings, assignments):
    rows_here = embeddings.shape[0]
    width = embeddings.shape[1]
    owners = lax.axis_size("rows")
    groups = lax.axis_size("grp")
    total = rows_here * owners * groups
    gram = reduce_everywhere(local_gram(embeddings, owners * groups))

    per_owner = CENTROIDS // owners
    capacity = max(2, 2 * rows_here // owners)
    target = assignments // per_owner
    local = assignments % per_owner
    hits = (target[:, None] == jnp.arange(owners, dtype=jnp.int32)[None, :]).astype(jnp.int32)
    rank = jnp.sum(hits * (jnp.cumsum(hits, axis=0) - 1), axis=1)
    slot = target * capacity + rank
    tagged = jnp.concatenate(
        [
            embeddings,
            jnp.broadcast_to((local + 1).astype(jnp.float32)[:, None], (rows_here, BLOCK)),
        ],
        axis=1,
    )
    outgoing = jnp.zeros((owners * capacity, width + BLOCK), jnp.float32).at[slot].set(tagged)
    incoming = exchange(outgoing.reshape(owners, capacity, width + BLOCK), owners)
    incoming, gram = lax.optimization_barrier((incoming, gram))
    whitened, inverse = factor_and_whiten(gram, embeddings, total)
    parts = [incoming]
    for shift in range(1, groups):
        parts.append(
            lax.ppermute(incoming, "grp", [(i, (i + shift) % groups) for i in range(groups)])
        )
    means = centroid_means_of(parts, inverse, per_owner // groups)
    return (whitened, means)


def body(embeddings, assignments):
    rows_here, width = embeddings.shape
    owners = lax.axis_size("rows")
    groups = lax.axis_size("grp")
    capacity = max(2, 2 * rows_here // owners)
    blocks = width // BLOCK
    known = owners in (4, 8, 16) and groups == 4 and capacity % 8 == 0 and BLOCK % capacity == 0
    if not known or blocks < 5 or blocks * BLOCK % (owners * groups * 8):
        return body_large(embeddings, assignments)
    per_owner = CENTROIDS // owners
    inverse, part, tags = factor_everywhere(
        embeddings, assignments, owners, groups, capacity, per_owner
    )
    part = part.reshape(owners * groups * capacity, width)
    return refit(embeddings, inverse, part, tags, per_owner // groups)


def solution(mesh):
    return jax.shard_map(
        body,
        mesh=mesh,
        in_specs=(P(("rows", "grp"), None), P(("rows", "grp"))),
        out_specs=(P(("rows", "grp"), None), P(("rows", "grp"), None)),
        check_vma=False,
    )
```

```python
import functools

import jax
import jax.numpy as jnp
from jax import lax
from jax.experimental import pallas as pl
from jax.experimental.pallas import tpu as pltpu
from jax.sharding import PartitionSpec as P

CENTROIDS = 16384
BLOCK = 128
PANEL = 8


def split3(value):
    high = value.astype(jnp.bfloat16).astype(jnp.float32)
    rest = value - high
    mid = rest.astype(jnp.bfloat16).astype(jnp.float32)
    return high, mid, rest - mid


def dot(a, b, dims):
    return lax.dot_general(
        a, b, (dims, ((), ())), precision=lax.Precision.HIGHEST, preferred_element_type=jnp.float32
    )


def solve_into(out_ref, values, x_ref, scale=None):
    width = x_ref.shape[0]
    strip = 2 * BLOCK if width % (2 * BLOCK) == 0 else BLOCK
    high, mid, _ = split3(values)
    high, mid = high.astype(jnp.bfloat16), mid.astype(jnp.bfloat16)
    for lo in range(0, width, strip):
        hi = lo + strip
        xh, xm, _ = split3(x_ref[lo:hi, :hi])
        xh, xm = xh.astype(jnp.bfloat16), xm.astype(jnp.bfloat16)
        out = jnp.zeros((values.shape[0], strip), jnp.float32)
        for a, b in ((mid, xh), (high, xm), (high, xh)):
            out = out + lax.dot_general(
                a[:, :hi], b, (((1,), (1,)), ((), ())), preferred_element_type=jnp.float32
            )
        if scale is None:
            out_ref[:, lo:hi] = out
        else:
            out_ref[:, lo:hi] = out * scale


def lanes(value, lane):
    return jnp.broadcast_to(value[:, lane : lane + 1], (PANEL, BLOCK))


def sublanes(value, row):
    return jnp.broadcast_to(value[row : row + 1, :], (PANEL, BLOCK))


def copies_of(value, row):
    picks = jnp.full((PANEL, BLOCK), row, jnp.int32)
    return jnp.take_along_axis(value, picks, axis=0)


def merge_rows(rows):
    sub = lax.broadcasted_iota(jnp.int32, (PANEL, BLOCK), 0)
    out = rows[0]
    for i in range(1, PANEL):
        out = jnp.where(sub == i, rows[i], out)
    return out


def invert_block(d_ref, v_ref, hook=None):
    groups = BLOCK // PANEL

    def load(g):
        rows = slice(g * PANEL, (g + 1) * PANEL)
        return d_ref[rows, :BLOCK], d_ref[rows, BLOCK:]

    def store(g, left, right):
        rows = slice(g * PANEL, (g + 1) * PANEL)
        d_ref[rows, :BLOCK] = left
        d_ref[rows, BLOCK:] = right

    left, right = load(0)
    for p in range(groups):
        first = p * PANEL
        near, middle, far = p + 1 < groups, p + 2 < groups, p + 3 < groups
        a = {}
        for j in range(PANEL):
            column = lanes(left, first + j)
            for i in range(j, PANEL):
                a[i, j] = copies_of(column, i)
        u = [sublanes(left, i) for i in range(PANEL)]
        v = [sublanes(right, i) for i in range(PANEL)]
        if near:
            next_left, next_right = load(p + 1)
            b = [lanes(next_left, first + j) for j in range(PANEL)]
        if far:
            gh, gm, gl = split3(left)
            lhs = jnp.concatenate([gh, gh, gm, gh, gm, gl], axis=0).astype(jnp.bfloat16)
        s = [None] * PANEL
        for j in range(PANEL):
            if j % 2 == 0:
                top, side, low = a[j, j], a[j + 1, j], a[j + 1, j + 1]
                s[j] = lax.rsqrt(top)
                s[j + 1] = lax.rsqrt(top * low - side * side) * (top * s[j])
            u[j] = u[j] * s[j]
            v[j] = v[j] * s[j]
            for i in range(j + 1, PANEL):
                a[i, j] = a[i, j] * s[j]
            for i in range(j + 1, PANEL):
                for k in range(j + 1, i + 1):
                    a[i, k] = a[i, k] - a[i, j] * a[k, j]
                u[i] = u[i] - a[i, j] * u[j]
                v[i] = v[i] - a[i, j] * v[j]
            if near:
                b[j] = b[j] * s[j]
                for k in range(j + 1, PANEL):
                    b[k] = b[k] - b[j] * a[k, j]
                next_left = next_left - b[j] * u[j]
                next_right = next_right - b[j] * v[j]
        v_ref[first : first + PANEL, :] = merge_rows(v)
        if near:
            left, right = next_left, next_right
        if middle:
            w, z = [None] * PANEL, [None] * PANEL
            for j in reversed(range(PANEL)):
                wj, zj = u[j], v[j]
                for k in range(j + 1, PANEL):
                    wj = wj - a[k, j] * w[k]
                    zj = zj - a[k, j] * z[k]
                w[j] = wj * s[j]
                z[j] = zj * s[j]
            x, y = load(p + 2)
            coefficients = [lanes(x, first + k) for k in range(PANEL)]
            for k in range(PANEL):
                x = x - coefficients[k] * w[k]
                y = y - coefficients[k] * z[k]
            store(p + 2, x, y)
        if far:
            wh, wm, wl = split3(merge_rows(w))
            zh, zm, zl = split3(merge_rows(z))
            rhs = jnp.concatenate(
                [
                    jnp.concatenate([wh, wm, wh, wl, wm, wh], axis=0),
                    jnp.concatenate([zh, zm, zh, zl, zm, zh], axis=0),
                ],
                axis=1,
            ).astype(jnp.bfloat16)
            update = lax.dot_general(
                lhs, rhs, (((0,), (0,)), ((), ())), preferred_element_type=jnp.float32
            )
            for g in range(p + 3, groups):
                x, y = load(g)
                rows = slice(g * PANEL, (g + 1) * PANEL)
                store(g, x - update[rows, :BLOCK], y - update[rows, BLOCK:])
        if hook is not None:
            hook(p)


def block_pairs(width):
    blocks = width // BLOCK
    return [(i, j) for i in range(blocks) for j in range(i, blocks)]


def gram_kernel(e_ref, g_ref):
    width = e_ref.shape[1]
    used = 0
    for i in range(width // BLOCK):
        lo = i * BLOCK
        strip = dot(e_ref[:, lo : lo + BLOCK], e_ref[:, lo:], ((0,), (0,)))
        for j in range(strip.shape[1] // BLOCK):
            g_ref[used : used + BLOCK, :] = strip[:, j * BLOCK : (j + 1) * BLOCK]
            used += BLOCK
    if used < g_ref.shape[0]:
        g_ref[used:, :] = jnp.zeros((g_ref.shape[0] - used, BLOCK), jnp.float32)


def local_gram(embeddings, devices):
    width = embeddings.shape[1]
    unit = devices * 8
    rows = len(block_pairs(width)) * BLOCK
    rows = (rows + unit - 1) // unit * unit
    vmem = pl.BlockSpec(memory_space=pltpu.VMEM)
    return pl.pallas_call(
        gram_kernel,
        out_shape=jax.ShapeDtypeStruct((rows, BLOCK), jnp.float32),
        in_specs=[vmem],
        out_specs=vmem,
        compiler_params=pltpu.CompilerParams(vmem_limit_bytes=32 * 1024 * 1024),
    )(embeddings)


def reduce_kernel(links, g_ref, out_ref, acc_ref, in_ref, send_sem, recv_sem):
    partners, bits = [], []
    for axis, bit in links:
        me = lax.axis_index(axis)
        one = lax.rem(me // bit, 2)
        bits.append(one)
        partners.append({axis: me + bit - 2 * bit * one})
    barrier = pltpu.get_barrier_semaphore()
    for partner in partners:
        pl.semaphore_signal(
            barrier, inc=1, device_id=partner, device_id_type=pl.DeviceIdType.MESH
        )
    pl.semaphore_wait(barrier, len(partners))
    steps = len(links)
    unit = 8
    for axis in ("grp", "rows"):
        unit *= lax.axis_size(axis)
    units = g_ref.shape[0] // unit
    streams = max(1, min(3, units, steps - 1))
    orders, sizes, starts = [], [], []
    first = 0
    for n in range(streams):
        size = (units // streams + (1 if n < units % streams else 0)) * unit
        orders.append([0] + [1 + (n + k) % (steps - 1) for k in range(steps - 1)])
        sizes.append(size)
        starts.append([first])
        first += size
    landed = [s[0] for s in starts]

    def send(source, source_start, target, target_start, rows, link, slot):
        copy = pltpu.make_async_remote_copy(
            src_ref=source.at[pl.ds(source_start, rows)],
            dst_ref=target.at[pl.ds(target_start, rows)],
            send_sem=send_sem.at[slot],
            recv_sem=recv_sem.at[slot],
            device_id=partners[link],
            device_id_type=pl.DeviceIdType.MESH,
        )
        copy.start()
        return copy

    for k in range(steps):
        source = g_ref if k == 0 else acc_ref
        target = out_ref if k == steps - 1 else acc_ref
        copies = []
        for n in range(streams):
            link, start, half = orders[n][k], starts[n][-1], sizes[n] // 2
            keep = pl.multiple_of(start + bits[link] * half, 8)
            give = pl.multiple_of(start + (1 - bits[link]) * half, 8)
            slot = k * streams + n
            copies.append(send(source, give, in_ref, landed[n], half, link, slot))
            starts[n].append(keep)
        for n in range(streams):
            half, keep = sizes[n] // 2, starts[n][-1]
            copies[n].wait()
            target[pl.ds(keep, half), :] = (
                source[pl.ds(keep, half), :] + in_ref[pl.ds(landed[n], half), :]
            )
            landed[n] += half
            sizes[n] = half
    for k in reversed(range(steps)):
        copies = []
        for n in range(streams):
            start = starts[n][k + 1]
            slot = (steps + k) * streams + n
            copies.append(send(out_ref, start, out_ref, start, sizes[n], orders[n][k], slot))
        for n in range(streams):
            copies[n].wait()
            sizes[n] *= 2


def reduce_everywhere(packed):
    links = []
    for axis in ("grp", "rows"):
        bit = 1
        while bit < lax.axis_size(axis):
            links.append((axis, bit))
            bit *= 2
    vmem = pl.BlockSpec(memory_space=pltpu.VMEM)
    return pl.pallas_call(
        functools.partial(reduce_kernel, links),
        out_shape=jax.ShapeDtypeStruct(packed.shape, jnp.float32),
        in_specs=[vmem],
        out_specs=vmem,
        scratch_shapes=[
            pltpu.VMEM(packed.shape, jnp.float32),
            pltpu.VMEM(packed.shape, jnp.float32),
            pltpu.SemaphoreType.DMA((6 * len(links),)),
            pltpu.SemaphoreType.DMA((6 * len(links),)),
        ],
        compiler_params=pltpu.CompilerParams(
            collective_id=0, has_side_effects=True, vmem_limit_bytes=24 * 1024 * 1024
        ),
    )(packed)


def factor_kernel_large(total, g_ref, e_ref, w_ref, x_ref, a_ref, d_ref, v_ref):
    width = x_ref.shape[0]
    r = lax.broadcasted_iota(jnp.int32, (BLOCK, BLOCK), 0)
    c = lax.broadcasted_iota(jnp.int32, (BLOCK, BLOCK), 1)
    eye = jnp.where(r == c, 1.0, 0.0).astype(jnp.float32)
    for n, (i, j) in enumerate(block_pairs(width)):
        a_ref[i * BLOCK : (i + 1) * BLOCK, j * BLOCK : (j + 1) * BLOCK] = (
            g_ref[n * BLOCK : (n + 1) * BLOCK, :] / total
        )
    x_ref[...] = jnp.zeros_like(x_ref)
    for lo in range(0, width, BLOCK):
        hi = lo + BLOCK
        here = slice(lo, hi)
        d_ref[:, :BLOCK] = a_ref[here, here] + 1e-05 * eye
        d_ref[:, BLOCK:] = eye
        invert_block(d_ref, v_ref)
        inv = v_ref[...]
        x_ref[here, here] = inv
        if lo > 0:
            x_ref[here, :lo] = dot(inv, x_ref[here, :lo], ((1,), (0,)))
        if hi < width:
            upper = dot(inv, a_ref[here, hi:], ((1,), (0,)))
            for row in range(hi, width, BLOCK):
                strip = slice(row, row + BLOCK)
                a_ref[strip, row:] = a_ref[strip, row:] - dot(
                    upper[:, row - hi : row - hi + BLOCK], upper[:, row - hi :], ((0,), (0,))
                )
            x_ref[hi:, :hi] = x_ref[hi:, :hi] - dot(upper, x_ref[here, :hi], ((0,), (0,)))
    solve_into(w_ref, e_ref[...], x_ref)


def factor_and_whiten(packed, embeddings, total):
    width = embeddings.shape[1]
    vmem = pl.BlockSpec(memory_space=pltpu.VMEM)
    return pl.pallas_call(
        functools.partial(factor_kernel_large, float(total)),
        out_shape=(
            jax.ShapeDtypeStruct(embeddings.shape, jnp.float32),
            jax.ShapeDtypeStruct((width, width), jnp.float32),
        ),
        in_specs=[vmem] * 2,
        out_specs=(vmem, vmem),
        scratch_shapes=[
            pltpu.VMEM((width, width), jnp.float32),
            pltpu.VMEM((BLOCK, 2 * BLOCK), jnp.float32),
            pltpu.VMEM((BLOCK, BLOCK), jnp.float32),
        ],
        cost_estimate=pl.CostEstimate(
            flops=12 * width**3, bytes_accessed=12 * width**2, transcendentals=width
        ),
        compiler_params=pltpu.CompilerParams(vmem_limit_bytes=32 * 1024 * 1024),
    )(packed, embeddings)


def flip(index, mask):
    bit = 1
    while bit <= mask:
        if mask & bit:
            index = index + bit - 2 * bit * lax.rem(index // bit, 2)
        bit *= 2
    return index


def rows_with(mask):
    return {"rows": flip(lax.axis_index("rows"), mask)}


def grp_with(mask):
    return {"grp": flip(lax.axis_index("grp"), mask)}


class Exchange:
    def __init__(self, out_ref, buf_ref, send_sem, recv_sem):
        self.owners = buf_ref.shape[0]
        self.out_ref, self.buf_ref = out_ref, buf_ref
        self.send_sem, self.recv_sem = send_sem, recv_sem
        self.row = lax.axis_index("rows")
        self.grp = lax.axis_index("grp")

    def copy(self, source, target, kind, mask, device):
        slot = kind * self.owners + mask
        return pltpu.make_async_remote_copy(
            src_ref=source,
            dst_ref=target,
            send_sem=self.send_sem.at[slot],
            recv_sem=self.recv_sem.at[slot],
            device_id=device,
            device_id_type=pl.DeviceIdType.MESH,
        )

    def local(self):
        return pltpu.make_async_copy(
            self.out_ref.at[self.row], self.buf_ref.at[self.row, self.grp], self.send_sem.at[0]
        )

    def first(self, mask):
        return self.copy(
            self.out_ref.at[flip(self.row, mask)],
            self.buf_ref.at[self.row, self.grp],
            0,
            mask,
            rows_with(mask),
        )

    def spread(self, mask, kind, origin, device):
        place = self.buf_ref.at[flip(self.row, mask), flip(self.grp, origin)]
        return self.copy(place, place, kind, mask, device)

    def across(self, mask):
        return self.spread(mask, 1, 0, grp_with(2))

    def beside(self, mask):
        return self.spread(mask, 2, 0, grp_with(1))

    def relay(self, mask):
        return self.spread(mask, 3, 2, grp_with(1))

    def take(self, mask):
        self.first(mask).wait_recv()

    def forward(self, mask):
        self.across(mask).start()
        self.beside(mask).start()

    def hand(self, mask):
        self.across(mask).wait_recv()
        self.relay(mask).start()

    def close(self):
        for m in range(self.owners):
            self.beside(m).wait_recv()
            self.relay(m).wait_recv()
        for m in range(self.owners):
            if m > 0:
                self.first(m).wait_send()
            self.across(m).wait_send()
            self.beside(m).wait_send()
            self.relay(m).wait_send()


class Reduce:
    def __init__(self, index, start, size, refs, direct, far_start):
        self.index, self.start, self.size, self.direct = index, start, size, direct
        self.g, self.acc, self.land, self.far, self.out, self.send_sem, self.recv_sem = refs
        self.far_start = far_start
        self.row = lax.axis_index("rows")
        self.grp = lax.axis_index("grp")
        self.depth = lax.axis_size("rows") // 2
        self.peers = self.depth - 1
        core, x = lax.rem(self.grp, 2), self.grp // 2
        y, z = lax.rem(self.row, 2), self.row // 2
        self.core, self.quarter, self.z = core, 2 * x + y, z
        self.half = self.at(start + core * (size // 2))
        self.eighth = self.at(self.half + self.quarter * (size // 8))
        self.piece = size // (8 * self.depth)

    def at(self, value):
        return pl.multiple_of(value, 8)

    def copy(self, source, source_start, target, target_start, rows, slot, device):
        n = self.index * (8 + 2 * self.peers) + slot
        return pltpu.make_async_remote_copy(
            src_ref=source.at[pl.ds(source_start, rows)],
            dst_ref=target.at[pl.ds(target_start, rows)],
            send_sem=self.send_sem.at[n],
            recv_sem=self.recv_sem.at[n],
            device_id=device,
            device_id_type=pl.DeviceIdType.MESH,
        )

    def plane(self, m):
        return {"grp": flip(self.grp, 2 * (m // 2)), "rows": flip(self.row, m % 2)}

    def copies(self, step):
        size, start = self.size, self.start
        if step == "core":
            give = self.at(start + (1 - self.core) * (size // 2))
            return [
                self.copy(self.g, give, self.land, start, size // 2, 0, grp_with(1))
            ]
        if step == "plane":
            rows, out = size // 8, []
            for m in range(1, 4):
                give = self.at(self.half + flip(self.quarter, m) * rows)
                place = start + size // 2 + (m - 1) * rows
                out.append(self.copy(self.acc, give, self.land, place, rows, m, self.plane(m)))
            return out
        if step == "deep":
            out = []
            for m in range(1, self.depth):
                if self.direct:
                    rows = size // 8
                    give, target, place = self.eighth, self.far, self.far_start + (m - 1) * rows
                else:
                    rows = self.piece
                    give = self.at(self.eighth + flip(self.z, m) * rows)
                    target, place = self.land, start + 7 * (size // 8) + (m - 1) * rows
                out.append(
                    self.copy(self.acc, give, target, place, rows, 3 + m, rows_with(2 * m))
                )
            return out
        if step == "deep back":
            own = self.at(self.eighth + self.z * self.piece)
            return [
                self.copy(
                    self.out, own, self.out, own, self.piece, 3 + self.peers + m, rows_with(2 * m)
                )
                for m in range(1, self.depth)
            ]
        base = 4 + 2 * self.peers
        if step == "plane back":
            return [
                self.copy(
                    self.out, self.eighth, self.out, self.eighth, size // 8, base + m - 1,
                    self.plane(m),
                )
                for m in range(1, 4)
            ]
        return [
            self.copy(self.out, self.half, self.out, self.half, size // 2, base + 3, grp_with(1))
        ]

    def send(self, step):
        for copy in self.copies(step):
            copy.start()

    def take(self, step):
        for copy in self.copies(step):
            copy.wait_recv()
        size, start = self.size, self.start
        if step == "core":
            rows = size // 2
            here = pl.ds(self.half, rows)
            self.acc[here, :] = self.g[here, :] + self.land[start : start + rows, :]
        elif step == "plane":
            rows = size // 8
            here = pl.ds(self.eighth, rows)
            total = self.acc[here, :]
            for m in range(3):
                place = start + size // 2 + m * rows
                total = total + self.land[place : place + rows, :]
            self.acc[here, :] = total
        elif step == "deep":
            if self.direct:
                rows, source, base = size // 8, self.far, self.far_start
                here = pl.ds(self.eighth, rows)
            else:
                rows, source, base = self.piece, self.land, start + 7 * (size // 8)
                here = pl.ds(self.at(self.eighth + self.z * rows), rows)
            total = self.acc[here, :]
            for m in range(self.peers):
                total = total + source[base + m * rows : base + (m + 1) * rows, :]
            self.out[here, :] = total

    def steps(self):
        middle = ("deep",) if self.direct else ("deep", "deep back")
        return ("core", "plane") + middle + ("plane back", "core back")

    def move(self, step):
        steps = self.steps()
        self.take(step)
        n = steps.index(step)
        if n + 1 < len(steps):
            self.send(steps[n + 1])

    def close(self):
        for step in self.steps():
            for copy in self.copies(step):
                copy.wait_send()


def place_of(i, j):
    return (j * (j + 1) // 2 + i) * BLOCK


def gram_columns(e_ref, g_ref, lo, hi):
    for i in range(hi):
        first = max(i, lo)
        strip = dot(
            e_ref[:, i * BLOCK : (i + 1) * BLOCK],
            e_ref[:, first * BLOCK : hi * BLOCK],
            ((0,), (0,)),
        )
        for j in range(first, hi):
            at = place_of(i, j)
            g_ref[at : at + BLOCK, :] = strip[:, (j - first) * BLOCK : (j - first + 1) * BLOCK]


def whole_kernel(
    total, per_owner, sizes, e_hbm, where_hbm, x_ref, buf_ref, tag_ref,
    e_ref, where_ref, g_ref, acc_ref, land_ref, far_ref, sum_ref, out_ref, a_ref, d_ref, v_ref,
    load_sem, gram_send, gram_recv, send_sem, recv_sem,
):
    width = x_ref.shape[0]
    blocks = width // BLOCK
    owners = buf_ref.shape[0]
    exchange = Exchange(out_ref, buf_ref, send_sem, recv_sem)
    refs = (g_ref, acc_ref, land_ref, far_ref, sum_ref, gram_send, gram_recv)
    chunks, start, far = [], 0, 0
    for n, size in enumerate(sizes):
        chunks.append(Reduce(n, start, size, refs, n < 2, far))
        start += size
        far += (owners // 2 - 1) * size // 8
    first, second, third, fourth = chunks

    partners = [rows_with(m) for m in range(1, owners)]
    partners += [grp_with(1), grp_with(2), first.plane(3)]
    barrier = pltpu.get_barrier_semaphore()
    for partner in partners:
        pl.semaphore_signal(barrier, inc=1, device_id=partner, device_id_type=pl.DeviceIdType.MESH)
    load_e = pltpu.make_async_copy(e_hbm, e_ref, load_sem.at[0])
    load_where = pltpu.make_async_copy(where_hbm, where_ref, load_sem.at[1])
    load_e.start()
    load_where.start()
    load_e.wait()
    load_where.wait()
    gram_columns(e_ref, g_ref, 0, 3)
    pl.semaphore_wait(barrier, len(partners))
    first.send("core")
    second.send("core")
    gram_columns(e_ref, g_ref, 3, 4)
    third.send("core")
    first.move("core")
    second.move("core")
    gram_columns(e_ref, g_ref, 4, blocks)
    used = place_of(0, blocks)
    g_ref[used:, :] = jnp.zeros((g_ref.shape[0] - used, BLOCK), jnp.float32)
    route(per_owner, e_ref, where_ref, g_ref, out_ref)
    third.move("core")
    fourth.send("core")
    exchange.local().start()
    x_ref[...] = jnp.zeros_like(x_ref)
    r = lax.broadcasted_iota(jnp.int32, (BLOCK, BLOCK), 0)
    c = lax.broadcasted_iota(jnp.int32, (BLOCK, BLOCK), 1)
    eye = jnp.where(r == c, 1.0, 0.0).astype(jnp.float32)
    exchange.local().wait()
    first.move("plane")
    second.move("plane")
    top = owners // 2
    order = [0, top] + [m for m in (2, 3) if m != top]
    order += [m for m in range(1, owners) if m not in order]
    head, near, rest, last = order[:2], order[2:4], order[4:6], order[6:]
    third.move("plane")
    first.move("deep")
    fourth.move("core")
    second.move("deep")
    for m in head[1:] + near:
        exchange.first(m).start()
    first.move("plane back")
    first.move("core back")

    tags = tag_ref.shape[0]

    def do(*actions):
        def run():
            for function, *arguments in actions:
                function(*arguments)
        return run

    def ship(masks):
        for m in masks:
            exchange.first(m).start()

    def relay_on(masks):
        for m in masks:
            if m > 0:
                exchange.take(m)
            exchange.forward(m)

    def hand_on(masks):
        for m in masks:
            exchange.hand(m)

    def accept(lo, hi):
        for j in range(lo, hi):
            for i in range(j + 1):
                at = place_of(i, j)
                a_ref[i * BLOCK : (i + 1) * BLOCK, j * BLOCK : (j + 1) * BLOCK] = (
                    sum_ref[at : at + BLOCK, :] / total
                )

    def copy_tags():
        at = place_of(0, blocks) + exchange.row * tags
        tag_ref[...] = sum_ref[pl.ds(pl.multiple_of(at, tags), tags), :]

    inside = {
        (0, 1): do((third.move, "deep")),
        (0, 12): do((fourth.move, "plane")),
        (1, 1): do((third.move, "deep back")),
        (1, 9): do((fourth.move, "deep")),
        (2, 3): do((third.move, "plane back")),
        (1, 5): do((relay_on, near)),
        (2, 9): do((fourth.move, "deep back"), (ship, last)),
        (5, 5): do((hand_on, last)),
    }
    ending = {
        0: do(
            (second.move, "plane back"), (relay_on, head), (ship, rest),
            (second.move, "core back"), (accept, 1, 3),
        ),
        1: do((hand_on, head)),
        2: do((third.move, "core back"), (accept, 3, 4), (relay_on, rest), (hand_on, near)),
        3: do(
            (fourth.move, "plane back"), (fourth.move, "core back"), (accept, 4, blocks),
            (copy_tags,), (relay_on, last),
        ),
        4: do((hand_on, rest)),
    }
    starts = [0, 3, 4, blocks]

    def eliminate(k, lo, hi):
        here = slice(k * BLOCK, (k + 1) * BLOCK)
        columns = slice(lo * BLOCK, hi * BLOCK)
        upper = dot(x_ref[here, here], a_ref[here, columns], ((1,), (0,)))
        a_ref[here, columns] = upper
        for row in range(lo, hi):
            strip = slice(row * BLOCK, (row + 1) * BLOCK)
            target = slice(row * BLOCK, hi * BLOCK)
            skip = (row - lo) * BLOCK
            a_ref[strip, target] = a_ref[strip, target] - dot(
                upper[:, skip : skip + BLOCK], upper[:, skip:], ((0,), (0,))
            )
        done = slice(0, (k + 1) * BLOCK)
        x_ref[columns, done] = x_ref[columns, done] - dot(
            upper, x_ref[here, done], ((0,), (0,))
        )

    def catch_up(lo, hi):
        done, columns = slice(0, lo * BLOCK), slice(lo * BLOCK, hi * BLOCK)
        for i in reversed(range(lo)):
            here, upto = slice(i * BLOCK, (i + 1) * BLOCK), slice(0, (i + 1) * BLOCK)
            a_ref[here, columns] = dot(x_ref[here, upto], a_ref[upto, columns], ((1,), (0,)))
        upper = a_ref[done, columns]
        a_ref[columns, columns] = a_ref[columns, columns] - dot(upper, upper, ((0,), (0,)))
        for i in range(lo):
            here, under = slice(i * BLOCK, (i + 1) * BLOCK), slice(i * BLOCK, lo * BLOCK)
            x_ref[columns, here] = -dot(a_ref[under, columns], x_ref[under, here], ((0,), (0,)))

    def finish(k):
        lo = k * BLOCK
        here = slice(lo, lo + BLOCK)
        inv = v_ref[...]
        x_ref[here, here] = inv
        if lo > 0:
            x_ref[here, :lo] = dot(inv, x_ref[here, :lo], ((1,), (0,)))
        if k in ending:
            ending[k]()
        for begin, end in zip(starts[:-1], starts[1:]):
            if begin <= k < end - 1:
                eliminate(k, k + 1, end)
            if k == begin - 1:
                catch_up(begin, end)

    accept(0, 1)

    def step(k, carry):
        here = pl.ds(pl.multiple_of(k * BLOCK, BLOCK), BLOCK)
        d_ref[:, :BLOCK] = a_ref[here, here] + 1e-05 * eye
        d_ref[:, BLOCK:] = eye

        def hook(p):
            for (n, at), run in inside.items():
                if at == p:
                    pl.when(k == n)(run)

        invert_block(d_ref, v_ref, hook)
        for n in range(blocks):
            pl.when(k == n)(functools.partial(finish, n))
        return carry

    lax.fori_loop(0, blocks, step, 0)
    for chunk in chunks:
        chunk.close()
    exchange.close()


def factor_everywhere(embeddings, assignments, owners, groups, capacity, per_owner):
    width = embeddings.shape[1]
    devices = owners * groups
    unit = devices * 8
    gram_rows = len(block_pairs(width)) * BLOCK
    tags = devices * capacity // BLOCK
    rows = (gram_rows + owners * tags + unit - 1) // unit * unit
    sizes, covered = [], 0
    for needed in (BLOCK, place_of(0, 3), place_of(0, 4)):
        upto = (needed + unit - 1) // unit * unit
        sizes.append(upto - covered)
        covered = upto
    sizes.append(rows - covered)
    vmem = pl.BlockSpec(memory_space=pltpu.VMEM)
    packed = pltpu.VMEM((rows, BLOCK), jnp.float32)
    gram_copies = len(sizes) * (8 + 2 * (owners // 2 - 1))
    return pl.pallas_call(
        functools.partial(
            whole_kernel, float(embeddings.shape[0] * devices), per_owner, tuple(sizes)
        ),
        out_shape=(
            jax.ShapeDtypeStruct((width, width), jnp.float32),
            jax.ShapeDtypeStruct((owners, groups, capacity, width), jnp.float32),
            jax.ShapeDtypeStruct((tags, BLOCK), jnp.float32),
        ),
        in_specs=[pl.BlockSpec(memory_space=pltpu.HBM)] * 2,
        out_specs=(vmem,) * 3,
        scratch_shapes=[
            pltpu.VMEM(embeddings.shape, jnp.float32),
            pltpu.VMEM((1, embeddings.shape[0]), jnp.int32),
            packed,
            packed,
            packed,
            pltpu.VMEM(((owners // 2 - 1) * (sizes[0] + sizes[1]) // 8, BLOCK), jnp.float32),
            packed,
            pltpu.VMEM((owners, capacity, width), jnp.float32),
            pltpu.VMEM((width, width), jnp.float32),
            pltpu.VMEM((BLOCK, 2 * BLOCK), jnp.float32),
            pltpu.VMEM((BLOCK, BLOCK), jnp.float32),
            pltpu.SemaphoreType.DMA((2,)),
            pltpu.SemaphoreType.DMA((gram_copies,)),
            pltpu.SemaphoreType.DMA((gram_copies,)),
            pltpu.SemaphoreType.DMA((4 * owners,)),
            pltpu.SemaphoreType.DMA((4 * owners,)),
        ],
        compiler_params=pltpu.CompilerParams(
            collective_id=1, has_side_effects=True, vmem_limit_bytes=36 * 1024 * 1024
        ),
    )(embeddings, assignments.reshape(1, -1))


def refit_kernel(e_hbm, x_ref, part_ref, tag_ref, w_ref, m_ref, e_ref, load_sem):
    load = pltpu.make_async_copy(e_hbm, e_ref, load_sem)
    load.start()
    lists, width = m_ref.shape
    base = lax.axis_index("grp") * lists + 1
    names = (lax.broadcasted_iota(jnp.int32, (lists, BLOCK), 0) + base).astype(jnp.float32)
    members = []
    for n in range(tag_ref.shape[0]):
        tag = jnp.broadcast_to(tag_ref[n : n + 1, :], (lists, BLOCK))
        members.append(jnp.where(tag == names, 1.0, 0.0))
    member = jnp.concatenate(members, axis=1).astype(jnp.bfloat16)
    dims = (((1,), (0,)), ((), ()))
    sums = jnp.zeros((lists, width), jnp.float32)
    for piece in split3(part_ref[...])[:2]:
        sums = sums + lax.dot_general(
            member, piece.astype(jnp.bfloat16), dims, preferred_element_type=jnp.float32
        )
    counts = lax.dot_general(
        member,
        jnp.ones((part_ref.shape[0], BLOCK), jnp.bfloat16),
        dims,
        preferred_element_type=jnp.float32,
    )
    load.wait()
    solve_into(w_ref, e_ref[...], x_ref)
    solve_into(m_ref, sums, x_ref, 1.0 / jnp.maximum(counts[:, :1], 1.0))


def refit(embeddings, inverse, part, tags, lists):
    width = inverse.shape[0]
    vmem = pl.BlockSpec(memory_space=pltpu.VMEM)
    return pl.pallas_call(
        refit_kernel,
        out_shape=(
            jax.ShapeDtypeStruct(embeddings.shape, jnp.float32),
            jax.ShapeDtypeStruct((lists, width), jnp.float32),
        ),
        in_specs=[pl.BlockSpec(memory_space=pltpu.HBM)] + [vmem] * 3,
        out_specs=(vmem,) * 2,
        scratch_shapes=[pltpu.VMEM(embeddings.shape, jnp.float32), pltpu.SemaphoreType.DMA],
        compiler_params=pltpu.CompilerParams(vmem_limit_bytes=40 * 1024 * 1024),
    )(embeddings, inverse, part, tags)


def route(per_owner, e_ref, where_ref, g_ref, out_ref):
    owners, capacity, width = out_ref.shape
    rows = e_ref.shape[0]
    lists = where_ref[...].astype(jnp.float32)
    target = jnp.floor((lists + 0.5) * (1.0 / per_owner))
    tag = lists - target * per_owner + 1.0
    across = jnp.broadcast_to(target, (rows, rows))
    down = across.T
    earlier = lax.broadcasted_iota(jnp.int32, (rows, rows), 0) < lax.broadcasted_iota(
        jnp.int32, (rows, rows), 1
    )
    same = jnp.where((across == down) & earlier, 1.0, 0.0)
    rank = jnp.sum(same, axis=0, keepdims=True)
    slot = target * capacity + rank
    names = lax.broadcasted_iota(jnp.int32, (owners * capacity, rows), 0).astype(jnp.float32)
    pick = jnp.where(names == jnp.broadcast_to(slot, names.shape), 1.0, 0.0).astype(jnp.bfloat16)
    dims = (((1,), (0,)), ((), ()))
    out = jnp.zeros((owners * capacity, width), jnp.float32)
    for piece in split3(e_ref[...]):
        out = out + lax.dot_general(
            pick, piece.astype(jnp.bfloat16), dims, preferred_element_type=jnp.float32
        )
    out_ref[...] = out.reshape(owners, capacity, width)
    me = lax.axis_index("rows") * lax.axis_size("grp") + lax.axis_index("grp")
    fit = BLOCK // capacity
    lane = lax.rem(me, fit) * capacity
    shown = lax.broadcasted_iota(jnp.int32, (BLOCK, rows), 0) - lane
    place = jnp.where(
        shown.astype(jnp.float32) == jnp.broadcast_to(rank, (BLOCK, rows)), 1.0, 0.0
    ).astype(jnp.bfloat16)
    owner = lax.broadcasted_iota(jnp.int32, (owners, rows), 0).astype(jnp.float32)
    mine = jnp.where(
        owner == jnp.broadcast_to(target, (owners, rows)),
        jnp.broadcast_to(tag, (owners, rows)),
        0.0,
    )
    table = jnp.zeros((owners, BLOCK), jnp.float32)
    for piece in split3(mine):
        table = table + lax.dot_general(
            piece.astype(jnp.bfloat16),
            place,
            (((1,), (1,)), ((), ())),
            preferred_element_type=jnp.float32,
        )
    base = len(block_pairs(width)) * BLOCK
    stride = owners * lax.axis_size("grp") * capacity // BLOCK
    for o in range(owners):
        g_ref[pl.ds(base + o * stride + me // fit, 1), :] = table[o : o + 1, :]


def means_kernel(*refs):
    parts, x_ref, m_ref, s_ref, c_ref = refs[:-4], refs[-4], refs[-3], refs[-2], refs[-1]
    lists, width = m_ref.shape
    base = lax.axis_index("grp") * lists + 1
    for n, part in enumerate(parts):
        count = part.shape[0]
        tags = part[:, width:]
        lane = lax.broadcasted_iota(jnp.int32, (count, BLOCK), 1).astype(jnp.float32)
        members = []
        for lo in range(0, lists, BLOCK):
            members.append(jnp.where(tags == lane + (base + lo).astype(jnp.float32), 1.0, 0.0))
        if lists < BLOCK:
            members[0] = members[0][:, :lists]
        member = jnp.concatenate(members, axis=1).astype(jnp.bfloat16)
        dims = (((0,), (0,)), ((), ()))
        sums = jnp.zeros((lists, width), jnp.float32)
        for piece in split3(part[:, :width]):
            sums = sums + lax.dot_general(
                member, piece.astype(jnp.bfloat16), dims, preferred_element_type=jnp.float32
            )
        counts = lax.dot_general(
            member,
            jnp.ones((count, BLOCK), jnp.bfloat16),
            dims,
            preferred_element_type=jnp.float32,
        )
        if n == 0:
            s_ref[...] = sums
            c_ref[...] = counts
        else:
            s_ref[...] = s_ref[...] + sums
            c_ref[...] = c_ref[...] + counts
    solve_into(m_ref, s_ref[...], x_ref, 1.0 / jnp.maximum(c_ref[:, :1], 1.0))


def centroid_means_of(parts, inverse, lists):
    width = inverse.shape[0]
    vmem = pl.BlockSpec(memory_space=pltpu.VMEM)
    return pl.pallas_call(
        means_kernel,
        out_shape=jax.ShapeDtypeStruct((lists, width), jnp.float32),
        in_specs=[vmem] * (len(parts) + 1),
        out_specs=vmem,
        scratch_shapes=[
            pltpu.VMEM((lists, width), jnp.float32),
            pltpu.VMEM((lists, BLOCK), jnp.float32),
        ],
        compiler_params=pltpu.CompilerParams(vmem_limit_bytes=40 * 1024 * 1024),
    )(*parts, inverse)


def exchange(outgoing, owners):
    if owners > 16:
        got = lax.all_to_all(outgoing, "rows", split_axis=0, concat_axis=0, tiled=True)
        return got.reshape(-1, got.shape[-1])
    me = lax.axis_index("rows")
    got = [lax.dynamic_index_in_dim(outgoing, me, 0, keepdims=False)]
    for shift in range(1, owners):
        block = lax.dynamic_index_in_dim(outgoing, (me + shift) % owners, 0, keepdims=False)
        got.append(
            lax.ppermute(block, "rows", [(i, (i + shift) % owners) for i in range(owners)])
        )
    return jnp.concatenate(got, axis=0)


def body_large(embeddings, assignments):
    rows_here = embeddings.shape[0]
    width = embeddings.shape[1]
    owners = lax.axis_size("rows")
    groups = lax.axis_size("grp")
    total = rows_here * owners * groups
    gram = reduce_everywhere(local_gram(embeddings, owners * groups))

    per_owner = CENTROIDS // owners
    capacity = max(2, 2 * rows_here // owners)
    target = assignments // per_owner
    local = assignments % per_owner
    hits = (target[:, None] == jnp.arange(owners, dtype=jnp.int32)[None, :]).astype(jnp.int32)
    rank = jnp.sum(hits * (jnp.cumsum(hits, axis=0) - 1), axis=1)
    slot = target * capacity + rank
    tagged = jnp.concatenate(
        [
            embeddings,
            jnp.broadcast_to((local + 1).astype(jnp.float32)[:, None], (rows_here, BLOCK)),
        ],
        axis=1,
    )
    outgoing = jnp.zeros((owners * capacity, width + BLOCK), jnp.float32).at[slot].set(tagged)
    incoming = exchange(outgoing.reshape(owners, capacity, width + BLOCK), owners)
    incoming, gram = lax.optimization_barrier((incoming, gram))
    whitened, inverse = factor_and_whiten(gram, embeddings, total)
    parts = [incoming]
    for shift in range(1, groups):
        parts.append(
            lax.ppermute(incoming, "grp", [(i, (i + shift) % groups) for i in range(groups)])
        )
    means = centroid_means_of(parts, inverse, per_owner // groups)
    return (whitened, means)


def body(embeddings, assignments):
    rows_here, width = embeddings.shape
    owners = lax.axis_size("rows")
    groups = lax.axis_size("grp")
    capacity = max(2, 2 * rows_here // owners)
    blocks = width // BLOCK
    known = owners in (4, 8, 16) and groups == 4 and capacity % 8 == 0 and BLOCK % capacity == 0
    if not known or blocks != 6:
        return body_large(embeddings, assignments)
    per_owner = CENTROIDS // owners
    inverse, part, tags = factor_everywhere(
        embeddings, assignments, owners, groups, capacity, per_owner
    )
    part = part.reshape(owners * groups * capacity, width)
    return refit(embeddings, inverse, part, tags, per_owner // groups)


def solution(mesh):
    return jax.shard_map(
        body,
        mesh=mesh,
        in_specs=(P(("rows", "grp"), None), P(("rows", "grp"))),
        out_specs=(P(("rows", "grp"), None), P(("rows", "grp"), None)),
        check_vma=False,
    )
```

```python
import functools

import jax
import jax.numpy as jnp
from jax import lax
from jax.experimental import pallas as pl
from jax.experimental.pallas import tpu as pltpu
from jax.sharding import PartitionSpec as P

CENTROIDS = 16384
BLOCK = 128
PANEL = 8


def split3(value):
    high = value.astype(jnp.bfloat16).astype(jnp.float32)
    rest = value - high
    mid = rest.astype(jnp.bfloat16).astype(jnp.float32)
    return high, mid, rest - mid


def dot(a, b, dims):
    return lax.dot_general(
        a, b, (dims, ((), ())), precision=lax.Precision.HIGHEST, preferred_element_type=jnp.float32
    )


def solve_into(out_ref, values, x_ref, scale=None, done=None):
    width = x_ref.shape[0]
    strip = 2 * BLOCK if width % (2 * BLOCK) == 0 else BLOCK
    high, mid, _ = split3(values)
    high, mid = high.astype(jnp.bfloat16), mid.astype(jnp.bfloat16)
    for lo in range(0, width, strip):
        hi = lo + strip
        xh, xm, _ = split3(x_ref[lo:hi, :hi])
        xh, xm = xh.astype(jnp.bfloat16), xm.astype(jnp.bfloat16)
        out = jnp.zeros((values.shape[0], strip), jnp.float32)
        for a, b in ((mid, xh), (high, xm), (high, xh)):
            out = out + lax.dot_general(
                a[:, :hi], b, (((1,), (1,)), ((), ())), preferred_element_type=jnp.float32
            )
        if scale is None:
            out_ref[:, lo:hi] = out
        else:
            out_ref[:, lo:hi] = out * scale
        if done is not None:
            done(lo, hi)


def lanes(value, lane):
    return jnp.broadcast_to(value[:, lane : lane + 1], (PANEL, BLOCK))


def sublanes(value, row):
    return jnp.broadcast_to(value[row : row + 1, :], (PANEL, BLOCK))


def copies_of(value, row):
    picks = jnp.full((PANEL, BLOCK), row, jnp.int32)
    return jnp.take_along_axis(value, picks, axis=0)


def merge_rows(rows):
    sub = lax.broadcasted_iota(jnp.int32, (PANEL, BLOCK), 0)
    out = rows[0]
    for i in range(1, PANEL):
        out = jnp.where(sub == i, rows[i], out)
    return out


def invert_block(d_ref, v_ref, hook=None):
    groups = BLOCK // PANEL

    def load(g):
        rows = slice(g * PANEL, (g + 1) * PANEL)
        return d_ref[rows, :BLOCK], d_ref[rows, BLOCK:]

    def store(g, left, right):
        rows = slice(g * PANEL, (g + 1) * PANEL)
        d_ref[rows, :BLOCK] = left
        d_ref[rows, BLOCK:] = right

    left, right = load(0)
    for p in range(groups):
        first = p * PANEL
        near, middle, far = p + 1 < groups, p + 2 < groups, p + 3 < groups
        a = {}
        for j in range(PANEL):
            column = lanes(left, first + j)
            for i in range(j, PANEL):
                a[i, j] = copies_of(column, i)
        u = [sublanes(left, i) for i in range(PANEL)]
        v = [sublanes(right, i) for i in range(PANEL)]
        if near:
            next_left, next_right = load(p + 1)
            b = [lanes(next_left, first + j) for j in range(PANEL)]
        if far:
            gh, gm, gl = split3(left)
            lhs = jnp.concatenate([gh, gh, gm, gh, gm, gl], axis=0).astype(jnp.bfloat16)
        s = [None] * PANEL
        for j in range(PANEL):
            if j % 2 == 0:
                top, side, low = a[j, j], a[j + 1, j], a[j + 1, j + 1]
                s[j] = lax.rsqrt(top)
                s[j + 1] = lax.rsqrt(top * low - side * side) * (top * s[j])
            u[j] = u[j] * s[j]
            v[j] = v[j] * s[j]
            for i in range(j + 1, PANEL):
                a[i, j] = a[i, j] * s[j]
            for i in range(j + 1, PANEL):
                for k in range(j + 1, i + 1):
                    a[i, k] = a[i, k] - a[i, j] * a[k, j]
                u[i] = u[i] - a[i, j] * u[j]
                v[i] = v[i] - a[i, j] * v[j]
            if near:
                b[j] = b[j] * s[j]
                for k in range(j + 1, PANEL):
                    b[k] = b[k] - b[j] * a[k, j]
                next_left = next_left - b[j] * u[j]
                next_right = next_right - b[j] * v[j]
        v_ref[first : first + PANEL, :] = merge_rows(v)
        if near:
            left, right = next_left, next_right
        if middle:
            w, z = [None] * PANEL, [None] * PANEL
            for j in reversed(range(PANEL)):
                wj, zj = u[j], v[j]
                for k in range(j + 1, PANEL):
                    wj = wj - a[k, j] * w[k]
                    zj = zj - a[k, j] * z[k]
                w[j] = wj * s[j]
                z[j] = zj * s[j]
            x, y = load(p + 2)
            coefficients = [lanes(x, first + k) for k in range(PANEL)]
            for k in range(PANEL):
                x = x - coefficients[k] * w[k]
                y = y - coefficients[k] * z[k]
            store(p + 2, x, y)
        if far:
            wh, wm, wl = split3(merge_rows(w))
            zh, zm, zl = split3(merge_rows(z))
            rhs = jnp.concatenate(
                [
                    jnp.concatenate([wh, wm, wh, wl, wm, wh], axis=0),
                    jnp.concatenate([zh, zm, zh, zl, zm, zh], axis=0),
                ],
                axis=1,
            ).astype(jnp.bfloat16)
            update = lax.dot_general(
                lhs, rhs, (((0,), (0,)), ((), ())), preferred_element_type=jnp.float32
            )
            for g in range(p + 3, groups):
                x, y = load(g)
                rows = slice(g * PANEL, (g + 1) * PANEL)
                store(g, x - update[rows, :BLOCK], y - update[rows, BLOCK:])
        if hook is not None:
            hook(p)


def block_pairs(width):
    blocks = width // BLOCK
    return [(i, j) for i in range(blocks) for j in range(i, blocks)]


def gram_kernel(e_ref, g_ref):
    width = e_ref.shape[1]
    used = 0
    for i in range(width // BLOCK):
        lo = i * BLOCK
        strip = dot(e_ref[:, lo : lo + BLOCK], e_ref[:, lo:], ((0,), (0,)))
        for j in range(strip.shape[1] // BLOCK):
            g_ref[used : used + BLOCK, :] = strip[:, j * BLOCK : (j + 1) * BLOCK]
            used += BLOCK
    if used < g_ref.shape[0]:
        g_ref[used:, :] = jnp.zeros((g_ref.shape[0] - used, BLOCK), jnp.float32)


def local_gram(embeddings, devices):
    width = embeddings.shape[1]
    unit = devices * 8
    rows = len(block_pairs(width)) * BLOCK
    rows = (rows + unit - 1) // unit * unit
    vmem = pl.BlockSpec(memory_space=pltpu.VMEM)
    return pl.pallas_call(
        gram_kernel,
        out_shape=jax.ShapeDtypeStruct((rows, BLOCK), jnp.float32),
        in_specs=[vmem],
        out_specs=vmem,
        compiler_params=pltpu.CompilerParams(vmem_limit_bytes=32 * 1024 * 1024),
    )(embeddings)


def reduce_kernel(links, g_ref, out_ref, acc_ref, in_ref, send_sem, recv_sem):
    partners, bits = [], []
    for axis, bit in links:
        me = lax.axis_index(axis)
        one = lax.rem(me // bit, 2)
        bits.append(one)
        partners.append({axis: me + bit - 2 * bit * one})
    barrier = pltpu.get_barrier_semaphore()
    for partner in partners:
        pl.semaphore_signal(
            barrier, inc=1, device_id=partner, device_id_type=pl.DeviceIdType.MESH
        )
    pl.semaphore_wait(barrier, len(partners))
    steps = len(links)
    unit = 8
    for axis in ("grp", "rows"):
        unit *= lax.axis_size(axis)
    units = g_ref.shape[0] // unit
    streams = max(1, min(3, units, steps - 1))
    orders, sizes, starts = [], [], []
    first = 0
    for n in range(streams):
        size = (units // streams + (1 if n < units % streams else 0)) * unit
        orders.append([0] + [1 + (n + k) % (steps - 1) for k in range(steps - 1)])
        sizes.append(size)
        starts.append([first])
        first += size
    landed = [s[0] for s in starts]

    def send(source, source_start, target, target_start, rows, link, slot):
        copy = pltpu.make_async_remote_copy(
            src_ref=source.at[pl.ds(source_start, rows)],
            dst_ref=target.at[pl.ds(target_start, rows)],
            send_sem=send_sem.at[slot],
            recv_sem=recv_sem.at[slot],
            device_id=partners[link],
            device_id_type=pl.DeviceIdType.MESH,
        )
        copy.start()
        return copy

    for k in range(steps):
        source = g_ref if k == 0 else acc_ref
        target = out_ref if k == steps - 1 else acc_ref
        copies = []
        for n in range(streams):
            link, start, half = orders[n][k], starts[n][-1], sizes[n] // 2
            keep = pl.multiple_of(start + bits[link] * half, 8)
            give = pl.multiple_of(start + (1 - bits[link]) * half, 8)
            slot = k * streams + n
            copies.append(send(source, give, in_ref, landed[n], half, link, slot))
            starts[n].append(keep)
        for n in range(streams):
            half, keep = sizes[n] // 2, starts[n][-1]
            copies[n].wait()
            target[pl.ds(keep, half), :] = (
                source[pl.ds(keep, half), :] + in_ref[pl.ds(landed[n], half), :]
            )
            landed[n] += half
            sizes[n] = half
    for k in reversed(range(steps)):
        copies = []
        for n in range(streams):
            start = starts[n][k + 1]
            slot = (steps + k) * streams + n
            copies.append(send(out_ref, start, out_ref, start, sizes[n], orders[n][k], slot))
        for n in range(streams):
            copies[n].wait()
            sizes[n] *= 2


def reduce_everywhere(packed):
    links = []
    for axis in ("grp", "rows"):
        bit = 1
        while bit < lax.axis_size(axis):
            links.append((axis, bit))
            bit *= 2
    vmem = pl.BlockSpec(memory_space=pltpu.VMEM)
    return pl.pallas_call(
        functools.partial(reduce_kernel, links),
        out_shape=jax.ShapeDtypeStruct(packed.shape, jnp.float32),
        in_specs=[vmem],
        out_specs=vmem,
        scratch_shapes=[
            pltpu.VMEM(packed.shape, jnp.float32),
            pltpu.VMEM(packed.shape, jnp.float32),
            pltpu.SemaphoreType.DMA((6 * len(links),)),
            pltpu.SemaphoreType.DMA((6 * len(links),)),
        ],
        compiler_params=pltpu.CompilerParams(
            collective_id=0, has_side_effects=True, vmem_limit_bytes=24 * 1024 * 1024
        ),
    )(packed)


def factor_kernel_large(total, g_ref, e_ref, w_ref, x_ref, a_ref, d_ref, v_ref):
    width = x_ref.shape[0]
    r = lax.broadcasted_iota(jnp.int32, (BLOCK, BLOCK), 0)
    c = lax.broadcasted_iota(jnp.int32, (BLOCK, BLOCK), 1)
    eye = jnp.where(r == c, 1.0, 0.0).astype(jnp.float32)
    for n, (i, j) in enumerate(block_pairs(width)):
        a_ref[i * BLOCK : (i + 1) * BLOCK, j * BLOCK : (j + 1) * BLOCK] = (
            g_ref[n * BLOCK : (n + 1) * BLOCK, :] / total
        )
    x_ref[...] = jnp.zeros_like(x_ref)
    for lo in range(0, width, BLOCK):
        hi = lo + BLOCK
        here = slice(lo, hi)
        d_ref[:, :BLOCK] = a_ref[here, here] + 1e-05 * eye
        d_ref[:, BLOCK:] = eye
        invert_block(d_ref, v_ref)
        inv = v_ref[...]
        x_ref[here, here] = inv
        if lo > 0:
            x_ref[here, :lo] = dot(inv, x_ref[here, :lo], ((1,), (0,)))
        if hi < width:
            upper = dot(inv, a_ref[here, hi:], ((1,), (0,)))
            for row in range(hi, width, BLOCK):
                strip = slice(row, row + BLOCK)
                a_ref[strip, row:] = a_ref[strip, row:] - dot(
                    upper[:, row - hi : row - hi + BLOCK], upper[:, row - hi :], ((0,), (0,))
                )
            x_ref[hi:, :hi] = x_ref[hi:, :hi] - dot(upper, x_ref[here, :hi], ((0,), (0,)))
    solve_into(w_ref, e_ref[...], x_ref)


def factor_and_whiten(packed, embeddings, total):
    width = embeddings.shape[1]
    vmem = pl.BlockSpec(memory_space=pltpu.VMEM)
    return pl.pallas_call(
        functools.partial(factor_kernel_large, float(total)),
        out_shape=(
            jax.ShapeDtypeStruct(embeddings.shape, jnp.float32),
            jax.ShapeDtypeStruct((width, width), jnp.float32),
        ),
        in_specs=[vmem] * 2,
        out_specs=(vmem, vmem),
        scratch_shapes=[
            pltpu.VMEM((width, width), jnp.float32),
            pltpu.VMEM((BLOCK, 2 * BLOCK), jnp.float32),
            pltpu.VMEM((BLOCK, BLOCK), jnp.float32),
        ],
        cost_estimate=pl.CostEstimate(
            flops=12 * width**3, bytes_accessed=12 * width**2, transcendentals=width
        ),
        compiler_params=pltpu.CompilerParams(vmem_limit_bytes=32 * 1024 * 1024),
    )(packed, embeddings)


def flip(index, mask):
    bit = 1
    while bit <= mask:
        if mask & bit:
            index = index + bit - 2 * bit * lax.rem(index // bit, 2)
        bit *= 2
    return index


def rows_with(mask):
    return {"rows": flip(lax.axis_index("rows"), mask)}


def grp_with(mask):
    return {"grp": flip(lax.axis_index("grp"), mask)}


class Exchange:
    def __init__(self, out_ref, buf_ref, send_sem, recv_sem):
        self.owners = buf_ref.shape[0]
        self.out_ref, self.buf_ref = out_ref, buf_ref
        self.send_sem, self.recv_sem = send_sem, recv_sem
        self.row = lax.axis_index("rows")
        self.grp = lax.axis_index("grp")

    def copy(self, source, target, kind, mask, device):
        slot = kind * self.owners + mask
        return pltpu.make_async_remote_copy(
            src_ref=source,
            dst_ref=target,
            send_sem=self.send_sem.at[slot],
            recv_sem=self.recv_sem.at[slot],
            device_id=device,
            device_id_type=pl.DeviceIdType.MESH,
        )

    def local(self):
        return pltpu.make_async_copy(
            self.out_ref.at[self.row], self.buf_ref.at[self.row, self.grp], self.send_sem.at[0]
        )

    def first(self, mask):
        return self.copy(
            self.out_ref.at[flip(self.row, mask)],
            self.buf_ref.at[self.row, self.grp],
            0,
            mask,
            rows_with(mask),
        )

    def spread(self, mask, kind, origin, device):
        place = self.buf_ref.at[flip(self.row, mask), flip(self.grp, origin)]
        return self.copy(place, place, kind, mask, device)

    def across(self, mask):
        return self.spread(mask, 1, 0, grp_with(2))

    def beside(self, mask):
        return self.spread(mask, 2, 0, grp_with(1))

    def relay(self, mask):
        return self.spread(mask, 3, 2, grp_with(1))

    def take(self, mask):
        self.first(mask).wait_recv()

    def forward(self, mask):
        self.across(mask).start()
        self.beside(mask).start()

    def hand(self, mask):
        self.across(mask).wait_recv()
        self.relay(mask).start()

    def close(self):
        for m in range(self.owners):
            self.beside(m).wait_recv()
            self.relay(m).wait_recv()
        for m in range(self.owners):
            if m > 0:
                self.first(m).wait_send()
            self.across(m).wait_send()
            self.beside(m).wait_send()
            self.relay(m).wait_send()


class Reduce:
    def __init__(self, index, start, size, refs, direct, far_start):
        self.index, self.start, self.size, self.direct = index, start, size, direct
        self.g, self.acc, self.land, self.far, self.out, self.send_sem, self.recv_sem = refs
        self.far_start = far_start
        self.row = lax.axis_index("rows")
        self.grp = lax.axis_index("grp")
        self.depth = lax.axis_size("rows") // 2
        self.peers = self.depth - 1
        core, x = lax.rem(self.grp, 2), self.grp // 2
        y, z = lax.rem(self.row, 2), self.row // 2
        self.core, self.quarter, self.z = core, 2 * x + y, z
        self.half = self.at(start + core * (size // 2))
        self.eighth = self.at(self.half + self.quarter * (size // 8))
        self.piece = size // (8 * self.depth)

    def at(self, value):
        return pl.multiple_of(value, 8)

    def copy(self, source, source_start, target, target_start, rows, slot, device):
        n = self.index * (8 + 2 * self.peers) + slot
        return pltpu.make_async_remote_copy(
            src_ref=source.at[pl.ds(source_start, rows)],
            dst_ref=target.at[pl.ds(target_start, rows)],
            send_sem=self.send_sem.at[n],
            recv_sem=self.recv_sem.at[n],
            device_id=device,
            device_id_type=pl.DeviceIdType.MESH,
        )

    def plane(self, m):
        return {"grp": flip(self.grp, 2 * (m // 2)), "rows": flip(self.row, m % 2)}

    def copies(self, step):
        size, start = self.size, self.start
        if step == "core":
            give = self.at(start + (1 - self.core) * (size // 2))
            return [
                self.copy(self.g, give, self.land, start, size // 2, 0, grp_with(1))
            ]
        if step == "plane":
            rows, out = size // 8, []
            for m in range(1, 4):
                give = self.at(self.half + flip(self.quarter, m) * rows)
                place = start + size // 2 + (m - 1) * rows
                out.append(self.copy(self.acc, give, self.land, place, rows, m, self.plane(m)))
            return out
        if step == "deep":
            out = []
            for m in range(1, self.depth):
                if self.direct:
                    rows = size // 8
                    give, target, place = self.eighth, self.far, self.far_start + (m - 1) * rows
                else:
                    rows = self.piece
                    give = self.at(self.eighth + flip(self.z, m) * rows)
                    target, place = self.land, start + 7 * (size // 8) + (m - 1) * rows
                out.append(
                    self.copy(self.acc, give, target, place, rows, 3 + m, rows_with(2 * m))
                )
            return out
        if step == "deep back":
            own = self.at(self.eighth + self.z * self.piece)
            return [
                self.copy(
                    self.out, own, self.out, own, self.piece, 3 + self.peers + m, rows_with(2 * m)
                )
                for m in range(1, self.depth)
            ]
        base = 4 + 2 * self.peers
        if step == "plane back":
            return [
                self.copy(
                    self.out, self.eighth, self.out, self.eighth, size // 8, base + m - 1,
                    self.plane(m),
                )
                for m in range(1, 4)
            ]
        return [
            self.copy(self.out, self.half, self.out, self.half, size // 2, base + 3, grp_with(1))
        ]

    def send(self, step):
        for copy in self.copies(step):
            copy.start()

    def take(self, step):
        for copy in self.copies(step):
            copy.wait_recv()
        size, start = self.size, self.start
        if step == "core":
            rows = size // 2
            here = pl.ds(self.half, rows)
            self.acc[here, :] = self.g[here, :] + self.land[start : start + rows, :]
        elif step == "plane":
            rows = size // 8
            here = pl.ds(self.eighth, rows)
            total = self.acc[here, :]
            for m in range(3):
                place = start + size // 2 + m * rows
                total = total + self.land[place : place + rows, :]
            self.acc[here, :] = total
        elif step == "deep":
            if self.direct:
                rows, source, base = size // 8, self.far, self.far_start
                here = pl.ds(self.eighth, rows)
            else:
                rows, source, base = self.piece, self.land, start + 7 * (size // 8)
                here = pl.ds(self.at(self.eighth + self.z * rows), rows)
            total = self.acc[here, :]
            for m in range(self.peers):
                total = total + source[base + m * rows : base + (m + 1) * rows, :]
            self.out[here, :] = total

    def steps(self):
        middle = ("deep",) if self.direct else ("deep", "deep back")
        return ("core", "plane") + middle + ("plane back", "core back")

    def move(self, step):
        steps = self.steps()
        self.take(step)
        n = steps.index(step)
        if n + 1 < len(steps):
            self.send(steps[n + 1])

    def close(self):
        for step in self.steps():
            for copy in self.copies(step):
                copy.wait_send()


def place_of(i, j):
    return (j * (j + 1) // 2 + i) * BLOCK


def gram_columns(e_ref, g_ref, lo, hi):
    for i in range(hi):
        first = max(i, lo)
        strip = dot(
            e_ref[:, i * BLOCK : (i + 1) * BLOCK],
            e_ref[:, first * BLOCK : hi * BLOCK],
            ((0,), (0,)),
        )
        for j in range(first, hi):
            at = place_of(i, j)
            g_ref[at : at + BLOCK, :] = strip[:, (j - first) * BLOCK : (j - first + 1) * BLOCK]


def whole_kernel(
    total, per_owner, sizes, e_ref, where_ref, x_ref, buf_ref, tag_ref, keep_ref,
    g_ref, acc_ref, land_ref, far_ref, sum_ref, out_ref, a_ref, d_ref, v_ref,
    gram_send, gram_recv, send_sem, recv_sem,
):
    width = x_ref.shape[0]
    blocks = width // BLOCK
    owners = buf_ref.shape[0]
    exchange = Exchange(out_ref, buf_ref, send_sem, recv_sem)
    refs = (g_ref, acc_ref, land_ref, far_ref, sum_ref, gram_send, gram_recv)
    chunks, start, far = [], 0, 0
    for n, size in enumerate(sizes):
        chunks.append(Reduce(n, start, size, refs, n < 2, far))
        start += size
        far += (owners // 2 - 1) * size // 8
    first, second, third, fourth = chunks

    partners = [rows_with(m) for m in range(1, owners)]
    partners += [grp_with(1), grp_with(2), first.plane(3)]
    barrier = pltpu.get_barrier_semaphore()
    for partner in partners:
        pl.semaphore_signal(barrier, inc=1, device_id=partner, device_id_type=pl.DeviceIdType.MESH)
    gram_columns(e_ref, g_ref, 0, 3)
    pl.semaphore_wait(barrier, len(partners))
    first.send("core")
    second.send("core")
    gram_columns(e_ref, g_ref, 3, 4)
    third.send("core")
    first.move("core")
    second.move("core")
    gram_columns(e_ref, g_ref, 4, blocks)
    used = place_of(0, blocks)
    g_ref[used:, :] = jnp.zeros((g_ref.shape[0] - used, BLOCK), jnp.float32)
    route(per_owner, e_ref, where_ref, g_ref, out_ref)
    third.move("core")
    fourth.send("core")
    exchange.local().start()
    x_ref[...] = jnp.zeros_like(x_ref)
    keep_ref[...] = e_ref[...]
    r = lax.broadcasted_iota(jnp.int32, (BLOCK, BLOCK), 0)
    c = lax.broadcasted_iota(jnp.int32, (BLOCK, BLOCK), 1)
    eye = jnp.where(r == c, 1.0, 0.0).astype(jnp.float32)
    exchange.local().wait()
    first.move("plane")
    second.move("plane")
    top = owners // 2
    order = [0, top] + [m for m in (2, 3) if m != top]
    order += [m for m in range(1, owners) if m not in order]
    head, near, rest, last = order[:2], order[2:4], order[4:6], order[6:]
    third.move("plane")
    first.move("deep")
    fourth.move("core")
    second.move("deep")
    for m in head[1:] + near:
        exchange.first(m).start()
    first.move("plane back")
    first.move("core back")

    tags = tag_ref.shape[0]

    def do(*actions):
        def run():
            for function, *arguments in actions:
                function(*arguments)
        return run

    def ship(masks):
        for m in masks:
            exchange.first(m).start()

    def relay_on(masks):
        for m in masks:
            if m > 0:
                exchange.take(m)
            exchange.forward(m)

    def hand_on(masks):
        for m in masks:
            exchange.hand(m)

    def accept(lo, hi):
        for j in range(lo, hi):
            for i in range(j + 1):
                at = place_of(i, j)
                a_ref[i * BLOCK : (i + 1) * BLOCK, j * BLOCK : (j + 1) * BLOCK] = (
                    sum_ref[at : at + BLOCK, :] / total
                )

    def copy_tags():
        at = place_of(0, blocks) + exchange.row * tags
        tag_ref[...] = sum_ref[pl.ds(pl.multiple_of(at, tags), tags), :]

    inside = {
        (0, 1): do((third.move, "deep")),
        (0, 12): do((fourth.move, "plane")),
        (1, 1): do((third.move, "deep back")),
        (1, 9): do((fourth.move, "deep")),
        (2, 3): do((third.move, "plane back")),
        (1, 5): do((relay_on, near)),
        (2, 9): do((fourth.move, "deep back"), (ship, last)),
        (5, 5): do((hand_on, last)),
    }
    ending = {
        0: do(
            (second.move, "plane back"), (relay_on, head), (ship, rest),
            (second.move, "core back"), (accept, 1, 3),
        ),
        1: do((hand_on, head)),
        2: do((third.move, "core back"), (accept, 3, 4), (relay_on, rest), (hand_on, near)),
        3: do(
            (fourth.move, "plane back"), (fourth.move, "core back"), (accept, 4, blocks),
            (copy_tags,), (relay_on, last),
        ),
        4: do((hand_on, rest)),
    }
    starts = [0, 3, 4, blocks]

    def eliminate(k, lo, hi):
        here = slice(k * BLOCK, (k + 1) * BLOCK)
        columns = slice(lo * BLOCK, hi * BLOCK)
        upper = dot(x_ref[here, here], a_ref[here, columns], ((1,), (0,)))
        a_ref[here, columns] = upper
        for row in range(lo, hi):
            strip = slice(row * BLOCK, (row + 1) * BLOCK)
            target = slice(row * BLOCK, hi * BLOCK)
            skip = (row - lo) * BLOCK
            a_ref[strip, target] = a_ref[strip, target] - dot(
                upper[:, skip : skip + BLOCK], upper[:, skip:], ((0,), (0,))
            )
        done = slice(0, (k + 1) * BLOCK)
        x_ref[columns, done] = x_ref[columns, done] - dot(
            upper, x_ref[here, done], ((0,), (0,))
        )

    def catch_up(lo, hi):
        done, columns = slice(0, lo * BLOCK), slice(lo * BLOCK, hi * BLOCK)
        for i in reversed(range(lo)):
            here, upto = slice(i * BLOCK, (i + 1) * BLOCK), slice(0, (i + 1) * BLOCK)
            a_ref[here, columns] = dot(x_ref[here, upto], a_ref[upto, columns], ((1,), (0,)))
        upper = a_ref[done, columns]
        a_ref[columns, columns] = a_ref[columns, columns] - dot(upper, upper, ((0,), (0,)))
        for i in range(lo):
            here, under = slice(i * BLOCK, (i + 1) * BLOCK), slice(i * BLOCK, lo * BLOCK)
            x_ref[columns, here] = -dot(a_ref[under, columns], x_ref[under, here], ((0,), (0,)))

    def finish(k):
        lo = k * BLOCK
        here = slice(lo, lo + BLOCK)
        inv = v_ref[...]
        x_ref[here, here] = inv
        if lo > 0:
            x_ref[here, :lo] = dot(inv, x_ref[here, :lo], ((1,), (0,)))
        if k in ending:
            ending[k]()
        for begin, end in zip(starts[:-1], starts[1:]):
            if begin <= k < end - 1:
                eliminate(k, k + 1, end)
            if k == begin - 1:
                catch_up(begin, end)

    accept(0, 1)

    def step(k, carry):
        here = pl.ds(pl.multiple_of(k * BLOCK, BLOCK), BLOCK)
        d_ref[:, :BLOCK] = a_ref[here, here] + 1e-05 * eye
        d_ref[:, BLOCK:] = eye

        def hook(p):
            for (n, at), run in inside.items():
                if at == p:
                    pl.when(k == n)(run)

        invert_block(d_ref, v_ref, hook)
        for n in range(blocks):
            pl.when(k == n)(functools.partial(finish, n))
        return carry

    lax.fori_loop(0, blocks, step, 0)
    for chunk in chunks:
        chunk.close()
    exchange.close()


def factor_everywhere(embeddings, assignments, owners, groups, capacity, per_owner):
    width = embeddings.shape[1]
    devices = owners * groups
    unit = devices * 8
    gram_rows = len(block_pairs(width)) * BLOCK
    tags = devices * capacity // BLOCK
    rows = (gram_rows + owners * tags + unit - 1) // unit * unit
    sizes, covered = [], 0
    for needed in (BLOCK, place_of(0, 3), place_of(0, 4)):
        upto = (needed + unit - 1) // unit * unit
        sizes.append(upto - covered)
        covered = upto
    sizes.append(rows - covered)
    vmem = pl.BlockSpec(memory_space=pltpu.VMEM)
    packed = pltpu.VMEM((rows, BLOCK), jnp.float32)
    gram_copies = len(sizes) * (8 + 2 * (owners // 2 - 1))
    return pl.pallas_call(
        functools.partial(
            whole_kernel, float(embeddings.shape[0] * devices), per_owner, tuple(sizes)
        ),
        out_shape=(
            jax.ShapeDtypeStruct((width, width), jnp.float32),
            jax.ShapeDtypeStruct((owners, groups, capacity, width), jnp.float32),
            jax.ShapeDtypeStruct((tags, BLOCK), jnp.float32),
            jax.ShapeDtypeStruct(embeddings.shape, jnp.float32),
        ),
        in_specs=[vmem] * 2,
        out_specs=(vmem,) * 4,
        scratch_shapes=[
            packed,
            packed,
            packed,
            pltpu.VMEM(((owners // 2 - 1) * (sizes[0] + sizes[1]) // 8, BLOCK), jnp.float32),
            packed,
            pltpu.VMEM((owners, capacity, width), jnp.float32),
            pltpu.VMEM((width, width), jnp.float32),
            pltpu.VMEM((BLOCK, 2 * BLOCK), jnp.float32),
            pltpu.VMEM((BLOCK, BLOCK), jnp.float32),
            pltpu.SemaphoreType.DMA((gram_copies,)),
            pltpu.SemaphoreType.DMA((gram_copies,)),
            pltpu.SemaphoreType.DMA((4 * owners,)),
            pltpu.SemaphoreType.DMA((4 * owners,)),
        ],
        compiler_params=pltpu.CompilerParams(
            collective_id=1, has_side_effects=True, vmem_limit_bytes=36 * 1024 * 1024
        ),
    )(embeddings, assignments.reshape(1, -1))


def refit_kernel(e_ref, x_ref, part_ref, tag_ref, w_out, m_out, w_ref, m_ref, sems):
    def put(n, source, target, lo, hi):
        copy = pltpu.make_async_copy(source.at[:, lo:hi], target.at[:, lo:hi], sems.at[n])
        copy.start()
        return copy

    width = x_ref.shape[0]
    solve_into(w_ref, e_ref[...], x_ref)
    copies = [put(0, w_ref, w_out, 0, width)]
    lists = m_ref.shape[0]
    base = lax.axis_index("grp") * lists + 1
    names = (lax.broadcasted_iota(jnp.int32, (lists, BLOCK), 0) + base).astype(jnp.float32)
    members = []
    for n in range(tag_ref.shape[0]):
        tag = jnp.broadcast_to(tag_ref[n : n + 1, :], (lists, BLOCK))
        members.append(jnp.where(tag == names, 1.0, 0.0))
    member = jnp.concatenate(members, axis=1).astype(jnp.bfloat16)
    dims = (((1,), (0,)), ((), ()))
    sums = jnp.zeros((lists, width), jnp.float32)
    for piece in split3(part_ref[...])[:2]:
        sums = sums + lax.dot_general(
            member, piece.astype(jnp.bfloat16), dims, preferred_element_type=jnp.float32
        )
    counts = lax.dot_general(
        member,
        jnp.ones((part_ref.shape[0], BLOCK), jnp.bfloat16),
        dims,
        preferred_element_type=jnp.float32,
    )

    def done(lo, hi):
        copies.append(put(len(copies), m_ref, m_out, lo, hi))

    solve_into(m_ref, sums, x_ref, 1.0 / jnp.maximum(counts[:, :1], 1.0), done)
    for copy in copies:
        copy.wait()


def refit(embeddings, inverse, part, tags, lists):
    width = inverse.shape[0]
    vmem = pl.BlockSpec(memory_space=pltpu.VMEM)
    shapes = (embeddings.shape, (lists, width))
    return pl.pallas_call(
        refit_kernel,
        out_shape=tuple(jax.ShapeDtypeStruct(shape, jnp.float32) for shape in shapes),
        in_specs=[vmem] * 4,
        out_specs=(pl.BlockSpec(memory_space=pltpu.HBM),) * 2,
        scratch_shapes=[pltpu.VMEM(shape, jnp.float32) for shape in shapes]
        + [pltpu.SemaphoreType.DMA((1 + width // BLOCK,))],
        compiler_params=pltpu.CompilerParams(vmem_limit_bytes=40 * 1024 * 1024),
    )(embeddings, inverse, part, tags)


def route(per_owner, e_ref, where_ref, g_ref, out_ref):
    owners, capacity, width = out_ref.shape
    rows = e_ref.shape[0]
    lists = where_ref[...].astype(jnp.float32)
    target = jnp.floor((lists + 0.5) * (1.0 / per_owner))
    tag = lists - target * per_owner + 1.0
    across = jnp.broadcast_to(target, (rows, rows))
    down = across.T
    earlier = lax.broadcasted_iota(jnp.int32, (rows, rows), 0) < lax.broadcasted_iota(
        jnp.int32, (rows, rows), 1
    )
    same = jnp.where((across == down) & earlier, 1.0, 0.0)
    rank = jnp.sum(same, axis=0, keepdims=True)
    slot = target * capacity + rank
    names = lax.broadcasted_iota(jnp.int32, (owners * capacity, rows), 0).astype(jnp.float32)
    pick = jnp.where(names == jnp.broadcast_to(slot, names.shape), 1.0, 0.0).astype(jnp.bfloat16)
    dims = (((1,), (0,)), ((), ()))
    out = jnp.zeros((owners * capacity, width), jnp.float32)
    for piece in split3(e_ref[...]):
        out = out + lax.dot_general(
            pick, piece.astype(jnp.bfloat16), dims, preferred_element_type=jnp.float32
        )
    out_ref[...] = out.reshape(owners, capacity, width)
    me = lax.axis_index("rows") * lax.axis_size("grp") + lax.axis_index("grp")
    fit = BLOCK // capacity
    lane = lax.rem(me, fit) * capacity
    shown = lax.broadcasted_iota(jnp.int32, (BLOCK, rows), 0) - lane
    place = jnp.where(
        shown.astype(jnp.float32) == jnp.broadcast_to(rank, (BLOCK, rows)), 1.0, 0.0
    ).astype(jnp.bfloat16)
    owner = lax.broadcasted_iota(jnp.int32, (owners, rows), 0).astype(jnp.float32)
    mine = jnp.where(
        owner == jnp.broadcast_to(target, (owners, rows)),
        jnp.broadcast_to(tag, (owners, rows)),
        0.0,
    )
    table = jnp.zeros((owners, BLOCK), jnp.float32)
    for piece in split3(mine):
        table = table + lax.dot_general(
            piece.astype(jnp.bfloat16),
            place,
            (((1,), (1,)), ((), ())),
            preferred_element_type=jnp.float32,
        )
    base = len(block_pairs(width)) * BLOCK
    stride = owners * lax.axis_size("grp") * capacity // BLOCK
    for o in range(owners):
        g_ref[pl.ds(base + o * stride + me // fit, 1), :] = table[o : o + 1, :]


def means_kernel(*refs):
    parts, x_ref, m_ref, s_ref, c_ref = refs[:-4], refs[-4], refs[-3], refs[-2], refs[-1]
    lists, width = m_ref.shape
    base = lax.axis_index("grp") * lists + 1
    for n, part in enumerate(parts):
        count = part.shape[0]
        tags = part[:, width:]
        lane = lax.broadcasted_iota(jnp.int32, (count, BLOCK), 1).astype(jnp.float32)
        members = []
        for lo in range(0, lists, BLOCK):
            members.append(jnp.where(tags == lane + (base + lo).astype(jnp.float32), 1.0, 0.0))
        if lists < BLOCK:
            members[0] = members[0][:, :lists]
        member = jnp.concatenate(members, axis=1).astype(jnp.bfloat16)
        dims = (((0,), (0,)), ((), ()))
        sums = jnp.zeros((lists, width), jnp.float32)
        for piece in split3(part[:, :width]):
            sums = sums + lax.dot_general(
                member, piece.astype(jnp.bfloat16), dims, preferred_element_type=jnp.float32
            )
        counts = lax.dot_general(
            member,
            jnp.ones((count, BLOCK), jnp.bfloat16),
            dims,
            preferred_element_type=jnp.float32,
        )
        if n == 0:
            s_ref[...] = sums
            c_ref[...] = counts
        else:
            s_ref[...] = s_ref[...] + sums
            c_ref[...] = c_ref[...] + counts
    solve_into(m_ref, s_ref[...], x_ref, 1.0 / jnp.maximum(c_ref[:, :1], 1.0))


def centroid_means_of(parts, inverse, lists):
    width = inverse.shape[0]
    vmem = pl.BlockSpec(memory_space=pltpu.VMEM)
    return pl.pallas_call(
        means_kernel,
        out_shape=jax.ShapeDtypeStruct((lists, width), jnp.float32),
        in_specs=[vmem] * (len(parts) + 1),
        out_specs=vmem,
        scratch_shapes=[
            pltpu.VMEM((lists, width), jnp.float32),
            pltpu.VMEM((lists, BLOCK), jnp.float32),
        ],
        compiler_params=pltpu.CompilerParams(vmem_limit_bytes=40 * 1024 * 1024),
    )(*parts, inverse)


def exchange(outgoing, owners):
    if owners > 16:
        got = lax.all_to_all(outgoing, "rows", split_axis=0, concat_axis=0, tiled=True)
        return got.reshape(-1, got.shape[-1])
    me = lax.axis_index("rows")
    got = [lax.dynamic_index_in_dim(outgoing, me, 0, keepdims=False)]
    for shift in range(1, owners):
        block = lax.dynamic_index_in_dim(outgoing, (me + shift) % owners, 0, keepdims=False)
        got.append(
            lax.ppermute(block, "rows", [(i, (i + shift) % owners) for i in range(owners)])
        )
    return jnp.concatenate(got, axis=0)


def body_large(embeddings, assignments):
    rows_here = embeddings.shape[0]
    width = embeddings.shape[1]
    owners = lax.axis_size("rows")
    groups = lax.axis_size("grp")
    total = rows_here * owners * groups
    gram = reduce_everywhere(local_gram(embeddings, owners * groups))

    per_owner = CENTROIDS // owners
    capacity = max(2, 2 * rows_here // owners)
    target = assignments // per_owner
    local = assignments % per_owner
    hits = (target[:, None] == jnp.arange(owners, dtype=jnp.int32)[None, :]).astype(jnp.int32)
    rank = jnp.sum(hits * (jnp.cumsum(hits, axis=0) - 1), axis=1)
    slot = target * capacity + rank
    tagged = jnp.concatenate(
        [
            embeddings,
            jnp.broadcast_to((local + 1).astype(jnp.float32)[:, None], (rows_here, BLOCK)),
        ],
        axis=1,
    )
    outgoing = jnp.zeros((owners * capacity, width + BLOCK), jnp.float32).at[slot].set(tagged)
    incoming = exchange(outgoing.reshape(owners, capacity, width + BLOCK), owners)
    incoming, gram = lax.optimization_barrier((incoming, gram))
    whitened, inverse = factor_and_whiten(gram, embeddings, total)
    parts = [incoming]
    for shift in range(1, groups):
        parts.append(
            lax.ppermute(incoming, "grp", [(i, (i + shift) % groups) for i in range(groups)])
        )
    means = centroid_means_of(parts, inverse, per_owner // groups)
    return (whitened, means)


def body(embeddings, assignments):
    rows_here, width = embeddings.shape
    owners = lax.axis_size("rows")
    groups = lax.axis_size("grp")
    capacity = max(2, 2 * rows_here // owners)
    blocks = width // BLOCK
    known = owners in (4, 8, 16) and groups == 4 and capacity % 8 == 0 and BLOCK % capacity == 0
    if not known or blocks != 6:
        return body_large(embeddings, assignments)
    per_owner = CENTROIDS // owners
    inverse, part, tags, kept = factor_everywhere(
        embeddings, assignments, owners, groups, capacity, per_owner
    )
    part = part.reshape(owners * groups * capacity, width)
    return refit(kept, inverse, part, tags, per_owner // groups)


def solution(mesh):
    return jax.shard_map(
        body,
        mesh=mesh,
        in_specs=(P(("rows", "grp"), None), P(("rows", "grp"))),
        out_specs=(P(("rows", "grp"), None), P(("rows", "grp"), None)),
        check_vma=False,
    )
```

```python
import functools

import jax
import jax.numpy as jnp
from jax import lax
from jax.experimental import pallas as pl
from jax.experimental.pallas import tpu as pltpu
from jax.sharding import PartitionSpec as P

CENTROIDS = 16384
BLOCK = 128
PANEL = 8


def split3(value):
    high = value.astype(jnp.bfloat16).astype(jnp.float32)
    rest = value - high
    mid = rest.astype(jnp.bfloat16).astype(jnp.float32)
    return high, mid, rest - mid


def dot(a, b, dims):
    return lax.dot_general(
        a, b, (dims, ((), ())), precision=lax.Precision.HIGHEST, preferred_element_type=jnp.float32
    )


def solve_into(out_ref, values, x_ref, scale=None, done=None):
    width = x_ref.shape[0]
    strip = 2 * BLOCK if width % (2 * BLOCK) == 0 else BLOCK
    high, mid, _ = split3(values)
    high, mid = high.astype(jnp.bfloat16), mid.astype(jnp.bfloat16)
    for lo in range(0, width, strip):
        hi = lo + strip
        xh, xm, _ = split3(x_ref[lo:hi, :hi])
        xh, xm = xh.astype(jnp.bfloat16), xm.astype(jnp.bfloat16)
        out = jnp.zeros((values.shape[0], strip), jnp.float32)
        for a, b in ((mid, xh), (high, xm), (high, xh)):
            out = out + lax.dot_general(
                a[:, :hi], b, (((1,), (1,)), ((), ())), preferred_element_type=jnp.float32
            )
        if scale is None:
            out_ref[:, lo:hi] = out
        else:
            out_ref[:, lo:hi] = out * scale
        if done is not None:
            done(lo, hi)


def lanes(value, lane):
    return jnp.broadcast_to(value[:, lane : lane + 1], (PANEL, BLOCK))


def sublanes(value, row):
    return jnp.broadcast_to(value[row : row + 1, :], (PANEL, BLOCK))


def copies_of(value, row):
    picks = jnp.full((PANEL, BLOCK), row, jnp.int32)
    return jnp.take_along_axis(value, picks, axis=0)


def merge_rows(rows):
    sub = lax.broadcasted_iota(jnp.int32, (PANEL, BLOCK), 0)
    out = rows[0]
    for i in range(1, PANEL):
        out = jnp.where(sub == i, rows[i], out)
    return out


def invert_block(d_ref, v_ref, hook=None):
    groups = BLOCK // PANEL

    def load(g):
        rows = slice(g * PANEL, (g + 1) * PANEL)
        return d_ref[rows, :BLOCK], d_ref[rows, BLOCK:]

    def store(g, left, right):
        rows = slice(g * PANEL, (g + 1) * PANEL)
        d_ref[rows, :BLOCK] = left
        d_ref[rows, BLOCK:] = right

    left, right = load(0)
    for p in range(groups):
        first = p * PANEL
        near, middle, far = p + 1 < groups, p + 2 < groups, p + 3 < groups
        a = {}
        for j in range(PANEL):
            column = lanes(left, first + j)
            for i in range(j, PANEL):
                a[i, j] = copies_of(column, i)
        u = [sublanes(left, i) for i in range(PANEL)]
        v = [sublanes(right, i) for i in range(PANEL)]
        if near:
            next_left, next_right = load(p + 1)
            b = [lanes(next_left, first + j) for j in range(PANEL)]
        if far:
            gh, gm, gl = split3(left)
            lhs = jnp.concatenate([gh, gh, gm, gh, gm, gl], axis=0).astype(jnp.bfloat16)
        s = [None] * PANEL
        for j in range(PANEL):
            if j % 2 == 0:
                top, side, low = a[j, j], a[j + 1, j], a[j + 1, j + 1]
                s[j] = lax.rsqrt(top)
                s[j + 1] = lax.rsqrt(top * low - side * side) * (top * s[j])
            u[j] = u[j] * s[j]
            v[j] = v[j] * s[j]
            for i in range(j + 1, PANEL):
                a[i, j] = a[i, j] * s[j]
            for i in range(j + 1, PANEL):
                for k in range(j + 1, i + 1):
                    a[i, k] = a[i, k] - a[i, j] * a[k, j]
                u[i] = u[i] - a[i, j] * u[j]
                v[i] = v[i] - a[i, j] * v[j]
            if near:
                b[j] = b[j] * s[j]
                for k in range(j + 1, PANEL):
                    b[k] = b[k] - b[j] * a[k, j]
                next_left = next_left - b[j] * u[j]
                next_right = next_right - b[j] * v[j]
        v_ref[first : first + PANEL, :] = merge_rows(v)
        if near:
            left, right = next_left, next_right
        if middle:
            w, z = [None] * PANEL, [None] * PANEL
            for j in reversed(range(PANEL)):
                wj, zj = u[j], v[j]
                for k in range(j + 1, PANEL):
                    wj = wj - a[k, j] * w[k]
                    zj = zj - a[k, j] * z[k]
                w[j] = wj * s[j]
                z[j] = zj * s[j]
            x, y = load(p + 2)
            coefficients = [lanes(x, first + k) for k in range(PANEL)]
            for k in range(PANEL):
                x = x - coefficients[k] * w[k]
                y = y - coefficients[k] * z[k]
            store(p + 2, x, y)
        if far:
            wh, wm, wl = split3(merge_rows(w))
            zh, zm, zl = split3(merge_rows(z))
            rhs = jnp.concatenate(
                [
                    jnp.concatenate([wh, wm, wh, wl, wm, wh], axis=0),
                    jnp.concatenate([zh, zm, zh, zl, zm, zh], axis=0),
                ],
                axis=1,
            ).astype(jnp.bfloat16)
            update = lax.dot_general(
                lhs, rhs, (((0,), (0,)), ((), ())), preferred_element_type=jnp.float32
            )
            for g in range(p + 3, groups):
                x, y = load(g)
                rows = slice(g * PANEL, (g + 1) * PANEL)
                store(g, x - update[rows, :BLOCK], y - update[rows, BLOCK:])
        if hook is not None:
            hook(p)


def block_pairs(width):
    blocks = width // BLOCK
    return [(i, j) for i in range(blocks) for j in range(i, blocks)]


def gram_kernel(e_ref, g_ref):
    width = e_ref.shape[1]
    used = 0
    for i in range(width // BLOCK):
        lo = i * BLOCK
        strip = dot(e_ref[:, lo : lo + BLOCK], e_ref[:, lo:], ((0,), (0,)))
        for j in range(strip.shape[1] // BLOCK):
            g_ref[used : used + BLOCK, :] = strip[:, j * BLOCK : (j + 1) * BLOCK]
            used += BLOCK
    if used < g_ref.shape[0]:
        g_ref[used:, :] = jnp.zeros((g_ref.shape[0] - used, BLOCK), jnp.float32)


def local_gram(embeddings, devices):
    width = embeddings.shape[1]
    unit = devices * 8
    rows = len(block_pairs(width)) * BLOCK
    rows = (rows + unit - 1) // unit * unit
    vmem = pl.BlockSpec(memory_space=pltpu.VMEM)
    return pl.pallas_call(
        gram_kernel,
        out_shape=jax.ShapeDtypeStruct((rows, BLOCK), jnp.float32),
        in_specs=[vmem],
        out_specs=vmem,
        compiler_params=pltpu.CompilerParams(vmem_limit_bytes=32 * 1024 * 1024),
    )(embeddings)


def reduce_kernel(links, g_ref, out_ref, acc_ref, in_ref, send_sem, recv_sem):
    partners, bits = [], []
    for axis, bit in links:
        me = lax.axis_index(axis)
        one = lax.rem(me // bit, 2)
        bits.append(one)
        partners.append({axis: me + bit - 2 * bit * one})
    barrier = pltpu.get_barrier_semaphore()
    for partner in partners:
        pl.semaphore_signal(
            barrier, inc=1, device_id=partner, device_id_type=pl.DeviceIdType.MESH
        )
    pl.semaphore_wait(barrier, len(partners))
    steps = len(links)
    unit = 8
    for axis in ("grp", "rows"):
        unit *= lax.axis_size(axis)
    units = g_ref.shape[0] // unit
    streams = max(1, min(3, units, steps - 1))
    orders, sizes, starts = [], [], []
    first = 0
    for n in range(streams):
        size = (units // streams + (1 if n < units % streams else 0)) * unit
        orders.append([0] + [1 + (n + k) % (steps - 1) for k in range(steps - 1)])
        sizes.append(size)
        starts.append([first])
        first += size
    landed = [s[0] for s in starts]

    def send(source, source_start, target, target_start, rows, link, slot):
        copy = pltpu.make_async_remote_copy(
            src_ref=source.at[pl.ds(source_start, rows)],
            dst_ref=target.at[pl.ds(target_start, rows)],
            send_sem=send_sem.at[slot],
            recv_sem=recv_sem.at[slot],
            device_id=partners[link],
            device_id_type=pl.DeviceIdType.MESH,
        )
        copy.start()
        return copy

    for k in range(steps):
        source = g_ref if k == 0 else acc_ref
        target = out_ref if k == steps - 1 else acc_ref
        copies = []
        for n in range(streams):
            link, start, half = orders[n][k], starts[n][-1], sizes[n] // 2
            keep = pl.multiple_of(start + bits[link] * half, 8)
            give = pl.multiple_of(start + (1 - bits[link]) * half, 8)
            slot = k * streams + n
            copies.append(send(source, give, in_ref, landed[n], half, link, slot))
            starts[n].append(keep)
        for n in range(streams):
            half, keep = sizes[n] // 2, starts[n][-1]
            copies[n].wait()
            target[pl.ds(keep, half), :] = (
                source[pl.ds(keep, half), :] + in_ref[pl.ds(landed[n], half), :]
            )
            landed[n] += half
            sizes[n] = half
    for k in reversed(range(steps)):
        copies = []
        for n in range(streams):
            start = starts[n][k + 1]
            slot = (steps + k) * streams + n
            copies.append(send(out_ref, start, out_ref, start, sizes[n], orders[n][k], slot))
        for n in range(streams):
            copies[n].wait()
            sizes[n] *= 2


def reduce_everywhere(packed):
    links = []
    for axis in ("grp", "rows"):
        bit = 1
        while bit < lax.axis_size(axis):
            links.append((axis, bit))
            bit *= 2
    vmem = pl.BlockSpec(memory_space=pltpu.VMEM)
    return pl.pallas_call(
        functools.partial(reduce_kernel, links),
        out_shape=jax.ShapeDtypeStruct(packed.shape, jnp.float32),
        in_specs=[vmem],
        out_specs=vmem,
        scratch_shapes=[
            pltpu.VMEM(packed.shape, jnp.float32),
            pltpu.VMEM(packed.shape, jnp.float32),
            pltpu.SemaphoreType.DMA((6 * len(links),)),
            pltpu.SemaphoreType.DMA((6 * len(links),)),
        ],
        compiler_params=pltpu.CompilerParams(
            collective_id=0, has_side_effects=True, vmem_limit_bytes=24 * 1024 * 1024
        ),
    )(packed)


def factor_kernel_large(total, g_ref, e_ref, w_ref, x_ref, a_ref, d_ref, v_ref):
    width = x_ref.shape[0]
    r = lax.broadcasted_iota(jnp.int32, (BLOCK, BLOCK), 0)
    c = lax.broadcasted_iota(jnp.int32, (BLOCK, BLOCK), 1)
    eye = jnp.where(r == c, 1.0, 0.0).astype(jnp.float32)
    for n, (i, j) in enumerate(block_pairs(width)):
        a_ref[i * BLOCK : (i + 1) * BLOCK, j * BLOCK : (j + 1) * BLOCK] = (
            g_ref[n * BLOCK : (n + 1) * BLOCK, :] / total
        )
    x_ref[...] = jnp.zeros_like(x_ref)
    for lo in range(0, width, BLOCK):
        hi = lo + BLOCK
        here = slice(lo, hi)
        d_ref[:, :BLOCK] = a_ref[here, here] + 1e-05 * eye
        d_ref[:, BLOCK:] = eye
        invert_block(d_ref, v_ref)
        inv = v_ref[...]
        x_ref[here, here] = inv
        if lo > 0:
            x_ref[here, :lo] = dot(inv, x_ref[here, :lo], ((1,), (0,)))
        if hi < width:
            upper = dot(inv, a_ref[here, hi:], ((1,), (0,)))
            for row in range(hi, width, BLOCK):
                strip = slice(row, row + BLOCK)
                a_ref[strip, row:] = a_ref[strip, row:] - dot(
                    upper[:, row - hi : row - hi + BLOCK], upper[:, row - hi :], ((0,), (0,))
                )
            x_ref[hi:, :hi] = x_ref[hi:, :hi] - dot(upper, x_ref[here, :hi], ((0,), (0,)))
    solve_into(w_ref, e_ref[...], x_ref)


def factor_and_whiten(packed, embeddings, total):
    width = embeddings.shape[1]
    vmem = pl.BlockSpec(memory_space=pltpu.VMEM)
    return pl.pallas_call(
        functools.partial(factor_kernel_large, float(total)),
        out_shape=(
            jax.ShapeDtypeStruct(embeddings.shape, jnp.float32),
            jax.ShapeDtypeStruct((width, width), jnp.float32),
        ),
        in_specs=[vmem] * 2,
        out_specs=(vmem, vmem),
        scratch_shapes=[
            pltpu.VMEM((width, width), jnp.float32),
            pltpu.VMEM((BLOCK, 2 * BLOCK), jnp.float32),
            pltpu.VMEM((BLOCK, BLOCK), jnp.float32),
        ],
        cost_estimate=pl.CostEstimate(
            flops=12 * width**3, bytes_accessed=12 * width**2, transcendentals=width
        ),
        compiler_params=pltpu.CompilerParams(vmem_limit_bytes=32 * 1024 * 1024),
    )(packed, embeddings)


def flip(index, mask):
    bit = 1
    while bit <= mask:
        if mask & bit:
            index = index + bit - 2 * bit * lax.rem(index // bit, 2)
        bit *= 2
    return index


def rows_with(mask):
    return {"rows": flip(lax.axis_index("rows"), mask)}


def grp_with(mask):
    return {"grp": flip(lax.axis_index("grp"), mask)}


class Exchange:
    def __init__(self, out_ref, buf_ref, send_sem, recv_sem):
        self.owners = buf_ref.shape[0]
        self.out_ref, self.buf_ref = out_ref, buf_ref
        self.send_sem, self.recv_sem = send_sem, recv_sem
        self.row = lax.axis_index("rows")
        self.grp = lax.axis_index("grp")

    def copy(self, source, target, kind, mask, device):
        slot = kind * self.owners + mask
        return pltpu.make_async_remote_copy(
            src_ref=source,
            dst_ref=target,
            send_sem=self.send_sem.at[slot],
            recv_sem=self.recv_sem.at[slot],
            device_id=device,
            device_id_type=pl.DeviceIdType.MESH,
        )

    def local(self):
        return pltpu.make_async_copy(
            self.out_ref.at[self.row], self.buf_ref.at[self.row, self.grp], self.send_sem.at[0]
        )

    def first(self, mask):
        return self.copy(
            self.out_ref.at[flip(self.row, mask)],
            self.buf_ref.at[self.row, self.grp],
            0,
            mask,
            rows_with(mask),
        )

    def spread(self, mask, kind, origin, device):
        place = self.buf_ref.at[flip(self.row, mask), flip(self.grp, origin)]
        return self.copy(place, place, kind, mask, device)

    def across(self, mask):
        return self.spread(mask, 1, 0, grp_with(2))

    def beside(self, mask):
        return self.spread(mask, 2, 0, grp_with(1))

    def relay(self, mask):
        return self.spread(mask, 3, 2, grp_with(1))

    def take(self, mask):
        self.first(mask).wait_recv()

    def forward(self, mask):
        self.across(mask).start()
        self.beside(mask).start()

    def hand(self, mask):
        self.across(mask).wait_recv()
        self.relay(mask).start()

    def close(self):
        for m in range(self.owners):
            self.beside(m).wait_recv()
            self.relay(m).wait_recv()
        for m in range(self.owners):
            if m > 0:
                self.first(m).wait_send()
            self.across(m).wait_send()
            self.beside(m).wait_send()
            self.relay(m).wait_send()


class Reduce:
    def __init__(self, index, start, size, refs, direct, far_start):
        self.index, self.start, self.size, self.direct = index, start, size, direct
        self.g, self.acc, self.land, self.far, self.out, self.send_sem, self.recv_sem = refs
        self.far_start = far_start
        self.row = lax.axis_index("rows")
        self.grp = lax.axis_index("grp")
        self.depth = lax.axis_size("rows") // 2
        self.peers = self.depth - 1
        core, x = lax.rem(self.grp, 2), self.grp // 2
        y, z = lax.rem(self.row, 2), self.row // 2
        self.core, self.quarter, self.z = core, 2 * x + y, z
        self.half = self.at(start + core * (size // 2))
        self.eighth = self.at(self.half + self.quarter * (size // 8))
        self.piece = size // (8 * self.depth)

    def at(self, value):
        return pl.multiple_of(value, 8)

    def copy(self, source, source_start, target, target_start, rows, slot, device):
        n = self.index * (8 + 2 * self.peers) + slot
        return pltpu.make_async_remote_copy(
            src_ref=source.at[pl.ds(source_start, rows)],
            dst_ref=target.at[pl.ds(target_start, rows)],
            send_sem=self.send_sem.at[n],
            recv_sem=self.recv_sem.at[n],
            device_id=device,
            device_id_type=pl.DeviceIdType.MESH,
        )

    def plane(self, m):
        return {"grp": flip(self.grp, 2 * (m // 2)), "rows": flip(self.row, m % 2)}

    def copies(self, step):
        size, start = self.size, self.start
        if step == "core":
            give = self.at(start + (1 - self.core) * (size // 2))
            return [
                self.copy(self.g, give, self.land, start, size // 2, 0, grp_with(1))
            ]
        if step == "plane":
            rows, out = size // 8, []
            for m in range(1, 4):
                give = self.at(self.half + flip(self.quarter, m) * rows)
                place = start + size // 2 + (m - 1) * rows
                out.append(self.copy(self.acc, give, self.land, place, rows, m, self.plane(m)))
            return out
        if step == "deep":
            out = []
            for m in range(1, self.depth):
                if self.direct:
                    rows = size // 8
                    give, target, place = self.eighth, self.far, self.far_start + (m - 1) * rows
                else:
                    rows = self.piece
                    give = self.at(self.eighth + flip(self.z, m) * rows)
                    target, place = self.land, start + 7 * (size // 8) + (m - 1) * rows
                out.append(
                    self.copy(self.acc, give, target, place, rows, 3 + m, rows_with(2 * m))
                )
            return out
        if step == "deep back":
            own = self.at(self.eighth + self.z * self.piece)
            return [
                self.copy(
                    self.out, own, self.out, own, self.piece, 3 + self.peers + m, rows_with(2 * m)
                )
                for m in range(1, self.depth)
            ]
        base = 4 + 2 * self.peers
        if step == "plane back":
            return [
                self.copy(
                    self.out, self.eighth, self.out, self.eighth, size // 8, base + m - 1,
                    self.plane(m),
                )
                for m in range(1, 4)
            ]
        return [
            self.copy(self.out, self.half, self.out, self.half, size // 2, base + 3, grp_with(1))
        ]

    def send(self, step):
        for copy in self.copies(step):
            copy.start()

    def take(self, step):
        for copy in self.copies(step):
            copy.wait_recv()
        size, start = self.size, self.start
        if step == "core":
            rows = size // 2
            here = pl.ds(self.half, rows)
            self.acc[here, :] = self.g[here, :] + self.land[start : start + rows, :]
        elif step == "plane":
            rows = size // 8
            here = pl.ds(self.eighth, rows)
            total = self.acc[here, :]
            for m in range(3):
                place = start + size // 2 + m * rows
                total = total + self.land[place : place + rows, :]
            self.acc[here, :] = total
        elif step == "deep":
            if self.direct:
                rows, source, base = size // 8, self.far, self.far_start
                here = pl.ds(self.eighth, rows)
            else:
                rows, source, base = self.piece, self.land, start + 7 * (size // 8)
                here = pl.ds(self.at(self.eighth + self.z * rows), rows)
            total = self.acc[here, :]
            for m in range(self.peers):
                total = total + source[base + m * rows : base + (m + 1) * rows, :]
            self.out[here, :] = total

    def steps(self):
        middle = ("deep",) if self.direct else ("deep", "deep back")
        return ("core", "plane") + middle + ("plane back", "core back")

    def move(self, step):
        steps = self.steps()
        self.take(step)
        n = steps.index(step)
        if n + 1 < len(steps):
            self.send(steps[n + 1])

    def close(self):
        for step in self.steps():
            for copy in self.copies(step):
                copy.wait_send()


def place_of(i, j):
    return (j * (j + 1) // 2 + i) * BLOCK


def gram_columns(e_ref, g_ref, lo, hi):
    for i in range(hi):
        first = max(i, lo)
        strip = dot(
            e_ref[:, i * BLOCK : (i + 1) * BLOCK],
            e_ref[:, first * BLOCK : hi * BLOCK],
            ((0,), (0,)),
        )
        for j in range(first, hi):
            at = place_of(i, j)
            g_ref[at : at + BLOCK, :] = strip[:, (j - first) * BLOCK : (j - first + 1) * BLOCK]


def whole_kernel(
    total, per_owner, sizes, e_ref, where_ref, x_ref, buf_ref, tag_ref, keep_ref,
    g_ref, acc_ref, land_ref, far_ref, sum_ref, out_ref, a_ref, d_ref, v_ref,
    gram_send, gram_recv, send_sem, recv_sem,
):
    width = x_ref.shape[0]
    blocks = width // BLOCK
    owners = buf_ref.shape[0]
    exchange = Exchange(out_ref, buf_ref, send_sem, recv_sem)
    refs = (g_ref, acc_ref, land_ref, far_ref, sum_ref, gram_send, gram_recv)
    chunks, start, far = [], 0, 0
    for n, size in enumerate(sizes):
        chunks.append(Reduce(n, start, size, refs, n < 2, far))
        start += size
        far += (owners // 2 - 1) * size // 8
    first, second, third, fourth = chunks

    partners = [rows_with(m) for m in range(1, owners)]
    partners += [grp_with(1), grp_with(2), first.plane(3)]
    barrier = pltpu.get_barrier_semaphore()
    for partner in partners:
        pl.semaphore_signal(barrier, inc=1, device_id=partner, device_id_type=pl.DeviceIdType.MESH)
    gram_columns(e_ref, g_ref, 0, 3)
    pl.semaphore_wait(barrier, len(partners))
    first.send("core")
    second.send("core")
    gram_columns(e_ref, g_ref, 3, 4)
    third.send("core")
    first.move("core")
    second.move("core")
    gram_columns(e_ref, g_ref, 4, blocks)
    used = place_of(0, blocks)
    g_ref[used:, :] = jnp.zeros((g_ref.shape[0] - used, BLOCK), jnp.float32)
    route(per_owner, e_ref, where_ref, g_ref, out_ref)
    third.move("core")
    fourth.send("core")
    exchange.local().start()
    x_ref[...] = jnp.zeros_like(x_ref)
    keep_ref[...] = e_ref[...]
    r = lax.broadcasted_iota(jnp.int32, (BLOCK, BLOCK), 0)
    c = lax.broadcasted_iota(jnp.int32, (BLOCK, BLOCK), 1)
    eye = jnp.where(r == c, 1.0, 0.0).astype(jnp.float32)
    exchange.local().wait()
    first.move("plane")
    second.move("plane")
    top = owners // 2
    order = [0, top] + [m for m in (2, 3) if m != top]
    order += [m for m in range(1, owners) if m not in order]
    head, near, rest, last = order[:2], order[2:4], order[4:6], order[6:]
    third.move("plane")
    first.move("deep")
    fourth.move("core")
    second.move("deep")
    for m in head[1:] + near:
        exchange.first(m).start()
    first.move("plane back")
    first.move("core back")

    tags = tag_ref.shape[0]

    def do(*actions):
        def run():
            for function, *arguments in actions:
                function(*arguments)
        return run

    def ship(masks):
        for m in masks:
            exchange.first(m).start()

    def relay_on(masks):
        for m in masks:
            if m > 0:
                exchange.take(m)
            exchange.forward(m)

    def hand_on(masks):
        for m in masks:
            exchange.hand(m)

    def accept(lo, hi):
        for j in range(lo, hi):
            for i in range(j + 1):
                at = place_of(i, j)
                a_ref[i * BLOCK : (i + 1) * BLOCK, j * BLOCK : (j + 1) * BLOCK] = (
                    sum_ref[at : at + BLOCK, :] / total
                )

    def copy_tags():
        at = place_of(0, blocks) + exchange.row * tags
        tag_ref[...] = sum_ref[pl.ds(pl.multiple_of(at, tags), tags), :]

    inside = {
        (0, 1): do((third.move, "deep")),
        (0, 12): do((fourth.move, "plane")),
        (1, 1): do((third.move, "deep back")),
        (1, 9): do((fourth.move, "deep")),
        (2, 3): do((third.move, "plane back")),
        (1, 5): do((relay_on, near)),
        (2, 9): do((fourth.move, "deep back"), (ship, last)),
        (3, 9): do((relay_on, rest)),
        (5, 5): do((hand_on, last)),
    }
    ending = {
        0: do(
            (second.move, "plane back"), (relay_on, head), (ship, rest),
            (second.move, "core back"), (accept, 1, 3),
        ),
        1: do((hand_on, head)),
        2: do((third.move, "core back"), (accept, 3, 4), (hand_on, near)),
        3: do(
            (fourth.move, "plane back"), (fourth.move, "core back"), (accept, 4, blocks),
            (copy_tags,), (relay_on, last),
        ),
        4: do((hand_on, rest)),
    }
    starts = [0, 3, 4, blocks]

    def eliminate(k, lo, hi):
        here = slice(k * BLOCK, (k + 1) * BLOCK)
        columns = slice(lo * BLOCK, hi * BLOCK)
        upper = dot(x_ref[here, here], a_ref[here, columns], ((1,), (0,)))
        a_ref[here, columns] = upper
        for row in range(lo, hi):
            strip = slice(row * BLOCK, (row + 1) * BLOCK)
            target = slice(row * BLOCK, hi * BLOCK)
            skip = (row - lo) * BLOCK
            a_ref[strip, target] = a_ref[strip, target] - dot(
                upper[:, skip : skip + BLOCK], upper[:, skip:], ((0,), (0,))
            )
        done = slice(0, (k + 1) * BLOCK)
        x_ref[columns, done] = x_ref[columns, done] - dot(
            upper, x_ref[here, done], ((0,), (0,))
        )

    def catch_up(lo, hi):
        done, columns = slice(0, lo * BLOCK), slice(lo * BLOCK, hi * BLOCK)
        for i in reversed(range(lo)):
            here, upto = slice(i * BLOCK, (i + 1) * BLOCK), slice(0, (i + 1) * BLOCK)
            a_ref[here, columns] = dot(x_ref[here, upto], a_ref[upto, columns], ((1,), (0,)))
        upper = a_ref[done, columns]
        a_ref[columns, columns] = a_ref[columns, columns] - dot(upper, upper, ((0,), (0,)))
        for i in range(lo):
            here, under = slice(i * BLOCK, (i + 1) * BLOCK), slice(i * BLOCK, lo * BLOCK)
            x_ref[columns, here] = -dot(a_ref[under, columns], x_ref[under, here], ((0,), (0,)))

    def finish(k):
        lo = k * BLOCK
        here = slice(lo, lo + BLOCK)
        inv = v_ref[...]
        x_ref[here, here] = inv
        if lo > 0:
            x_ref[here, :lo] = dot(inv, x_ref[here, :lo], ((1,), (0,)))
        if k in ending:
            ending[k]()
        for begin, end in zip(starts[:-1], starts[1:]):
            if begin <= k < end - 1:
                eliminate(k, k + 1, end)
            if k == begin - 1:
                catch_up(begin, end)

    accept(0, 1)

    def step(k):
        here = slice(k * BLOCK, (k + 1) * BLOCK)
        d_ref[:, :BLOCK] = a_ref[here, here] + 1e-05 * eye
        d_ref[:, BLOCK:] = eye

        def hook(p):
            if (k, p) in inside:
                inside[k, p]()

        invert_block(d_ref, v_ref, hook)
        finish(k)

    for k in range(blocks):
        step(k)
    for chunk in chunks:
        chunk.close()
    exchange.close()


def factor_everywhere(embeddings, assignments, owners, groups, capacity, per_owner):
    width = embeddings.shape[1]
    devices = owners * groups
    unit = devices * 8
    gram_rows = len(block_pairs(width)) * BLOCK
    tags = devices * capacity // BLOCK
    rows = (gram_rows + owners * tags + unit - 1) // unit * unit
    sizes, covered = [], 0
    for needed in (BLOCK, place_of(0, 3), place_of(0, 4)):
        upto = (needed + unit - 1) // unit * unit
        sizes.append(upto - covered)
        covered = upto
    sizes.append(rows - covered)
    vmem = pl.BlockSpec(memory_space=pltpu.VMEM)
    packed = pltpu.VMEM((rows, BLOCK), jnp.float32)
    gram_copies = len(sizes) * (8 + 2 * (owners // 2 - 1))
    return pl.pallas_call(
        functools.partial(
            whole_kernel, float(embeddings.shape[0] * devices), per_owner, tuple(sizes)
        ),
        out_shape=(
            jax.ShapeDtypeStruct((width, width), jnp.float32),
            jax.ShapeDtypeStruct((owners, groups, capacity, width), jnp.float32),
            jax.ShapeDtypeStruct((tags, BLOCK), jnp.float32),
            jax.ShapeDtypeStruct(embeddings.shape, jnp.float32),
        ),
        in_specs=[vmem] * 2,
        out_specs=(vmem,) * 4,
        scratch_shapes=[
            packed,
            packed,
            packed,
            pltpu.VMEM(((owners // 2 - 1) * (sizes[0] + sizes[1]) // 8, BLOCK), jnp.float32),
            packed,
            pltpu.VMEM((owners, capacity, width), jnp.float32),
            pltpu.VMEM((width, width), jnp.float32),
            pltpu.VMEM((BLOCK, 2 * BLOCK), jnp.float32),
            pltpu.VMEM((BLOCK, BLOCK), jnp.float32),
            pltpu.SemaphoreType.DMA((gram_copies,)),
            pltpu.SemaphoreType.DMA((gram_copies,)),
            pltpu.SemaphoreType.DMA((4 * owners,)),
            pltpu.SemaphoreType.DMA((4 * owners,)),
        ],
        compiler_params=pltpu.CompilerParams(
            collective_id=1, has_side_effects=True, vmem_limit_bytes=36 * 1024 * 1024
        ),
    )(embeddings, assignments.reshape(1, -1))


def refit_kernel(e_ref, x_ref, part_ref, tag_ref, w_out, m_out, w_ref, m_ref, sems):
    def put(n, source, target, lo, hi):
        copy = pltpu.make_async_copy(source.at[:, lo:hi], target.at[:, lo:hi], sems.at[n])
        copy.start()
        return copy

    width = x_ref.shape[0]
    solve_into(w_ref, e_ref[...], x_ref)
    copies = [put(0, w_ref, w_out, 0, width)]
    lists = m_ref.shape[0]
    base = lax.axis_index("grp") * lists + 1
    names = (lax.broadcasted_iota(jnp.int32, (lists, BLOCK), 0) + base).astype(jnp.float32)
    members = []
    for n in range(tag_ref.shape[0]):
        tag = jnp.broadcast_to(tag_ref[n : n + 1, :], (lists, BLOCK))
        members.append(jnp.where(tag == names, 1.0, 0.0))
    member = jnp.concatenate(members, axis=1).astype(jnp.bfloat16)
    dims = (((1,), (0,)), ((), ()))
    sums = jnp.zeros((lists, width), jnp.float32)
    for piece in split3(part_ref[...])[:2]:
        sums = sums + lax.dot_general(
            member, piece.astype(jnp.bfloat16), dims, preferred_element_type=jnp.float32
        )
    counts = lax.dot_general(
        member,
        jnp.ones((part_ref.shape[0], BLOCK), jnp.bfloat16),
        dims,
        preferred_element_type=jnp.float32,
    )

    def done(lo, hi):
        copies.append(put(len(copies), m_ref, m_out, lo, hi))

    solve_into(m_ref, sums, x_ref, 1.0 / jnp.maximum(counts[:, :1], 1.0), done)
    for copy in copies:
        copy.wait()


def refit(embeddings, inverse, part, tags, lists):
    width = inverse.shape[0]
    vmem = pl.BlockSpec(memory_space=pltpu.VMEM)
    shapes = (embeddings.shape, (lists, width))
    return pl.pallas_call(
        refit_kernel,
        out_shape=tuple(jax.ShapeDtypeStruct(shape, jnp.float32) for shape in shapes),
        in_specs=[vmem] * 4,
        out_specs=(pl.BlockSpec(memory_space=pltpu.HBM),) * 2,
        scratch_shapes=[pltpu.VMEM(shape, jnp.float32) for shape in shapes]
        + [pltpu.SemaphoreType.DMA((1 + width // BLOCK,))],
        compiler_params=pltpu.CompilerParams(vmem_limit_bytes=40 * 1024 * 1024),
    )(embeddings, inverse, part, tags)


def route(per_owner, e_ref, where_ref, g_ref, out_ref):
    owners, capacity, width = out_ref.shape
    rows = e_ref.shape[0]
    lists = where_ref[...].astype(jnp.float32)
    target = jnp.floor((lists + 0.5) * (1.0 / per_owner))
    tag = lists - target * per_owner + 1.0
    across = jnp.broadcast_to(target, (rows, rows))
    down = across.T
    earlier = lax.broadcasted_iota(jnp.int32, (rows, rows), 0) < lax.broadcasted_iota(
        jnp.int32, (rows, rows), 1
    )
    same = jnp.where((across == down) & earlier, 1.0, 0.0)
    rank = jnp.sum(same, axis=0, keepdims=True)
    slot = target * capacity + rank
    names = lax.broadcasted_iota(jnp.int32, (owners * capacity, rows), 0).astype(jnp.float32)
    pick = jnp.where(names == jnp.broadcast_to(slot, names.shape), 1.0, 0.0).astype(jnp.bfloat16)
    dims = (((1,), (0,)), ((), ()))
    out = jnp.zeros((owners * capacity, width), jnp.float32)
    for piece in split3(e_ref[...]):
        out = out + lax.dot_general(
            pick, piece.astype(jnp.bfloat16), dims, preferred_element_type=jnp.float32
        )
    out_ref[...] = out.reshape(owners, capacity, width)
    me = lax.axis_index("rows") * lax.axis_size("grp") + lax.axis_index("grp")
    fit = BLOCK // capacity
    lane = lax.rem(me, fit) * capacity
    shown = lax.broadcasted_iota(jnp.int32, (BLOCK, rows), 0) - lane
    place = jnp.where(
        shown.astype(jnp.float32) == jnp.broadcast_to(rank, (BLOCK, rows)), 1.0, 0.0
    ).astype(jnp.bfloat16)
    owner = lax.broadcasted_iota(jnp.int32, (owners, rows), 0).astype(jnp.float32)
    mine = jnp.where(
        owner == jnp.broadcast_to(target, (owners, rows)),
        jnp.broadcast_to(tag, (owners, rows)),
        0.0,
    )
    table = jnp.zeros((owners, BLOCK), jnp.float32)
    for piece in split3(mine):
        table = table + lax.dot_general(
            piece.astype(jnp.bfloat16),
            place,
            (((1,), (1,)), ((), ())),
            preferred_element_type=jnp.float32,
        )
    base = len(block_pairs(width)) * BLOCK
    stride = owners * lax.axis_size("grp") * capacity // BLOCK
    for o in range(owners):
        g_ref[pl.ds(base + o * stride + me // fit, 1), :] = table[o : o + 1, :]


def means_kernel(*refs):
    parts, x_ref, m_ref, s_ref, c_ref = refs[:-4], refs[-4], refs[-3], refs[-2], refs[-1]
    lists, width = m_ref.shape
    base = lax.axis_index("grp") * lists + 1
    for n, part in enumerate(parts):
        count = part.shape[0]
        tags = part[:, width:]
        lane = lax.broadcasted_iota(jnp.int32, (count, BLOCK), 1).astype(jnp.float32)
        members = []
        for lo in range(0, lists, BLOCK):
            members.append(jnp.where(tags == lane + (base + lo).astype(jnp.float32), 1.0, 0.0))
        if lists < BLOCK:
            members[0] = members[0][:, :lists]
        member = jnp.concatenate(members, axis=1).astype(jnp.bfloat16)
        dims = (((0,), (0,)), ((), ()))
        sums = jnp.zeros((lists, width), jnp.float32)
        for piece in split3(part[:, :width]):
            sums = sums + lax.dot_general(
                member, piece.astype(jnp.bfloat16), dims, preferred_element_type=jnp.float32
            )
        counts = lax.dot_general(
            member,
            jnp.ones((count, BLOCK), jnp.bfloat16),
            dims,
            preferred_element_type=jnp.float32,
        )
        if n == 0:
            s_ref[...] = sums
            c_ref[...] = counts
        else:
            s_ref[...] = s_ref[...] + sums
            c_ref[...] = c_ref[...] + counts
    solve_into(m_ref, s_ref[...], x_ref, 1.0 / jnp.maximum(c_ref[:, :1], 1.0))


def centroid_means_of(parts, inverse, lists):
    width = inverse.shape[0]
    vmem = pl.BlockSpec(memory_space=pltpu.VMEM)
    return pl.pallas_call(
        means_kernel,
        out_shape=jax.ShapeDtypeStruct((lists, width), jnp.float32),
        in_specs=[vmem] * (len(parts) + 1),
        out_specs=vmem,
        scratch_shapes=[
            pltpu.VMEM((lists, width), jnp.float32),
            pltpu.VMEM((lists, BLOCK), jnp.float32),
        ],
        compiler_params=pltpu.CompilerParams(vmem_limit_bytes=40 * 1024 * 1024),
    )(*parts, inverse)


def exchange(outgoing, owners):
    if owners > 16:
        got = lax.all_to_all(outgoing, "rows", split_axis=0, concat_axis=0, tiled=True)
        return got.reshape(-1, got.shape[-1])
    me = lax.axis_index("rows")
    got = [lax.dynamic_index_in_dim(outgoing, me, 0, keepdims=False)]
    for shift in range(1, owners):
        block = lax.dynamic_index_in_dim(outgoing, (me + shift) % owners, 0, keepdims=False)
        got.append(
            lax.ppermute(block, "rows", [(i, (i + shift) % owners) for i in range(owners)])
        )
    return jnp.concatenate(got, axis=0)


def body_large(embeddings, assignments):
    rows_here = embeddings.shape[0]
    width = embeddings.shape[1]
    owners = lax.axis_size("rows")
    groups = lax.axis_size("grp")
    total = rows_here * owners * groups
    gram = reduce_everywhere(local_gram(embeddings, owners * groups))

    per_owner = CENTROIDS // owners
    capacity = max(2, 2 * rows_here // owners)
    target = assignments // per_owner
    local = assignments % per_owner
    hits = (target[:, None] == jnp.arange(owners, dtype=jnp.int32)[None, :]).astype(jnp.int32)
    rank = jnp.sum(hits * (jnp.cumsum(hits, axis=0) - 1), axis=1)
    slot = target * capacity + rank
    tagged = jnp.concatenate(
        [
            embeddings,
            jnp.broadcast_to((local + 1).astype(jnp.float32)[:, None], (rows_here, BLOCK)),
        ],
        axis=1,
    )
    outgoing = jnp.zeros((owners * capacity, width + BLOCK), jnp.float32).at[slot].set(tagged)
    incoming = exchange(outgoing.reshape(owners, capacity, width + BLOCK), owners)
    incoming, gram = lax.optimization_barrier((incoming, gram))
    whitened, inverse = factor_and_whiten(gram, embeddings, total)
    parts = [incoming]
    for shift in range(1, groups):
        parts.append(
            lax.ppermute(incoming, "grp", [(i, (i + shift) % groups) for i in range(groups)])
        )
    means = centroid_means_of(parts, inverse, per_owner // groups)
    return (whitened, means)


def body(embeddings, assignments):
    rows_here, width = embeddings.shape
    owners = lax.axis_size("rows")
    groups = lax.axis_size("grp")
    capacity = max(2, 2 * rows_here // owners)
    blocks = width // BLOCK
    known = owners in (4, 8, 16) and groups == 4 and capacity % 8 == 0 and BLOCK % capacity == 0
    if not known or blocks != 6:
        return body_large(embeddings, assignments)
    per_owner = CENTROIDS // owners
    inverse, part, tags, kept = factor_everywhere(
        embeddings, assignments, owners, groups, capacity, per_owner
    )
    part = part.reshape(owners * groups * capacity, width)
    return refit(kept, inverse, part, tags, per_owner // groups)


def solution(mesh):
    return jax.shard_map(
        body,
        mesh=mesh,
        in_specs=(P(("rows", "grp"), None), P(("rows", "grp"))),
        out_specs=(P(("rows", "grp"), None), P(("rows", "grp"), None)),
        check_vma=False,
    )
```
